128 devices in a mesh: train: 8 (over z, x_hi), serve: 16 (over x_lo, y, core).
Axes of the slice: x: 4 (x_hi: 2, x_lo: 2; x = x_hi * 2 + x_lo), y: 4, z: 4, core: 2. Of those that a mesh axis runs over, the one named last changes fastest.
Arguments:
- train_weights: bfloat16 [16, 7680, 2112], P(None, 'train', 'serve'), may hold values from -6 to 6
- row_offset: int32 [16, 9], replicated, may hold values from 0 to 7168, as said below
- block_group: int32 [16, 224, 1], P(None, 'train'), may hold values from 0 to 15; in each aligned block of 28 rows (0 to 27, 28 to 55, ..., all dimensions but the last counted through in order) at most 3 rows name the same one
Outputs:
- quant_codes: bfloat16 [16, 16, 8, 3, 32, 2112], P(None, 'serve', 'train')
- block_scales: float32 [16, 16, 8, 3, 2112], P(None, 'serve', 'train')
The draws below stay inside these ranges and needn't reach their ends.
Inputs may be any that keep to these rules, and one draw needn't show every extreme that they name: For every layer l: row_offset[l, 0] = 0 and row_offset[l, 8] = 7168; every other row_offset[l, t] lies 1 to 32 rows above or below t * 896, never on it; in every layer one entry lies exactly 32 rows above and another exactly 32 rows below; layer 1 has the opposite sign of layer 0 at every such entry. `block_group`: within each aligned block of 28 entries (one training device's blocks of one layer), no group is named more than 3 times; some group reaches 3 in some of them.
All inputs are finite; a program needn't handle non-finite values.
Results may differ from the reference program's by a relative error of at most 0.001.
Values may be sent and summed in bfloat16 or wider, within the bound.
A program may use at most 128 MiB of HBM per device.

```python
import math
import jax
import jax.numpy as jnp
import numpy as np
from jax import lax

MODEL_DIM = 7168
LAYERS = 16
BLOCK = 32
SHIFT = 32
FEAT = 2112
ROWS_DEV = 896
SLOT = 960
BLOCKS = 224
BLOCKS_DEV = 28
SLOTS = 3
N_TRAIN = 8
N_SERVE = 16


def draw_train_weights(key, part):
    base_key = jax.random.fold_in(key, 23)
    value_key, quiet_key, scale_key = jax.random.split(base_key, 3)
    full_shape = (LAYERS, N_TRAIN * SLOT, FEAT)
    values = jnp.clip(jax.random.normal(value_key, full_shape, jnp.float32), -6.0, 6.0)
    quiet_mask = jax.random.randint(quiet_key, (LAYERS, MODEL_DIM // BLOCK, FEAT), 0, 8, dtype=jnp.int32) == 0
    buffer_row = jnp.arange(N_TRAIN * SLOT, dtype=jnp.int32)
    owner_dev = buffer_row // SLOT
    global_row = jnp.clip(owner_dev * ROWS_DEV + buffer_row % SLOT - SHIFT, 0, MODEL_DIM - 1).astype(jnp.int32)
    block_of_row = (global_row // BLOCK).astype(jnp.int32)
    quiet_rows = jnp.take(quiet_mask, block_of_row, axis=1)
    damping = jnp.where(quiet_rows, 0.02, 1.0).astype(jnp.float32)
    return (values * damping).astype(jnp.bfloat16)


def draw_row_offset(key, part):
    base_key = jax.random.fold_in(key, 11)
    size_key, sign_key, pick_key = jax.random.split(base_key, 3)
    magnitude = jax.random.randint(size_key, (LAYERS, N_TRAIN - 1), 1, SHIFT + 1, dtype=jnp.int32)
    signs = jax.random.randint(sign_key, (LAYERS, N_TRAIN - 1), 0, 2, dtype=jnp.int32) * 2 - 1
    inner = (magnitude * signs).astype(jnp.int32)
    pick_keys = jax.random.split(pick_key, LAYERS)
    picked = jax.vmap(lambda one_key: jax.random.permutation(one_key, N_TRAIN - 1))(pick_keys)
    column_ids = jnp.arange(N_TRAIN - 1, dtype=jnp.int32)[None, :]
    inner = jnp.where(column_ids == picked[:, 0:1], SHIFT, inner)
    inner = jnp.where(column_ids == picked[:, 1:2], -SHIFT, inner)
    layer_ids = jnp.arange(LAYERS, dtype=jnp.int32)[:, None]
    inner = jnp.where(layer_ids == 1, -inner[0:1], inner).astype(jnp.int32)
    middle = jnp.arange(1, N_TRAIN, dtype=jnp.int32)[None, :] * ROWS_DEV + inner
    start = jnp.zeros((LAYERS, 1), jnp.int32)
    finish = jnp.full((LAYERS, 1), N_TRAIN * ROWS_DEV, jnp.int32)
    return jnp.concatenate([start, middle, finish], axis=1).astype(jnp.int32)


def routed_block(key, own, number, rows, number_of, top, most, slope):
    order = jax.random.permutation(key, number_of)
    crowded, ordinary = shares(number_of, rows * top, most, slope, True), shares(number_of, rows * top, most, slope, False)
    places = jnp.arange(number_of)

    def named(lengths, rotation):
        used = int((lengths > 0).sum())
        fixed = max(1, used // 4)
        moved = fixed + (places - fixed + rotation * (used - fixed)) % max(1, number_of - fixed)
        return jnp.zeros((number_of,), jnp.int32).at[order[jnp.where(places < fixed, places, moved)]].set(jnp.asarray(lengths, jnp.int32))

    lengths = jnp.where(number % 4 == 0, named(crowded, number // 4), named(ordinary, number - number // 4 - 1))
    mixed = jax.random.permutation(jax.random.fold_in(own, 3), number_of)
    donor, sink = mixed[0:number_of // 2 * 2:2], mixed[1:number_of // 2 * 2:2]
    slack = jnp.minimum(lengths[donor] - 1, most - lengths[sink]) // 2
    slack = jnp.where((donor == order[0]) | (sink == order[0]) | (lengths[sink] == 0), 0, jnp.maximum(slack, 0))
    moved = jax.random.randint(jax.random.fold_in(own, 4), (number_of // 2,), 0, 1 << 20) % (slack + 1)
    lengths = lengths.at[donor].add(-moved).at[sink].add(moved)
    labels = jnp.searchsorted(jnp.cumsum(lengths), jnp.arange(rows * top), side="right").astype(jnp.int32)
    listing = labels.reshape(top, rows).T
    listing = listing[jax.random.permutation(jax.random.fold_in(own, 1), rows)]
    rotation = jax.random.randint(jax.random.fold_in(own, 2), (rows, 1), 0, top)
    return jnp.take_along_axis(listing, (jnp.arange(top)[None, :] + rotation) % top, axis=1)


def shares(number_of, total, bound, skew, full):
    portions = [(1 << 20) // math.isqrt(grade ** skew) + 1 for grade in range(1, number_of + 1)]
    largest = bound if full else min(bound, max(-(-total // number_of), total * portions[0] // sum(portions)))
    least = 1 if total - largest >= number_of - 1 else 0
    given, rest = [largest] + [least] * (number_of - 1), total - largest - least * (number_of - 1)
    while rest > 0:
        movable = [i for i in range(1, number_of) if given[i] < largest] or [i for i in range(1, number_of) if given[i] < bound]
        pool, budget = sum([portions[i] for i in movable]), rest
        for i in movable:
            extra = min(bound - given[i], max(1, budget * portions[i] // pool), rest)
            given[i] = given[i] + extra
            rest = rest - extra
    return np.array(given)


def setup_inputs(seed: int = 0) -> dict:
    splits = jax.random.split(jax.random.key(seed), 4)
    train_weights = draw_train_weights(jax.random.fold_in(splits[3], 71), 0)
    row_offset = draw_row_offset(jax.random.fold_in(splits[3], 71), 0)
    block_group_keys = jax.random.split(jax.random.fold_in(splits[2], 1), LAYERS * BLOCKS // BLOCKS_DEV)
    block_group_turns = jax.random.permutation(jax.random.fold_in(splits[2], 3), LAYERS * BLOCKS // BLOCKS_DEV)
    block_group = jax.vmap(lambda own, number: routed_block(jax.random.fold_in(splits[2], 2), own, number, BLOCKS_DEV, N_SERVE, 1, SLOTS, 0))(block_group_keys, block_group_turns).reshape((LAYERS, BLOCKS, 1))
    return {"train_weights": train_weights, "row_offset": row_offset, "block_group": block_group}


def reference(train_weights, row_offset, block_group):
    row_ids = jnp.arange(MODEL_DIM, dtype=jnp.int32)
    block_owner = (jnp.arange(BLOCKS, dtype=jnp.int32) // BLOCKS_DEV).astype(jnp.int32)
    position = jnp.arange(BLOCKS_DEV, dtype=jnp.int32)
    earlier = position[None, :] < position[:, None]

    def one_layer(inputs):
        weights, groups, offsets = inputs
        owner_dev = jnp.sum((row_ids[:, None] >= offsets[None, 1:N_TRAIN]).astype(jnp.int32), axis=1).astype(jnp.int32)
        source = (owner_dev * SLOT + row_ids - owner_dev * ROWS_DEV + SHIFT).astype(jnp.int32)
        gathered = jnp.take(weights, source, axis=0)
        blocks = gathered.reshape(BLOCKS, BLOCK, FEAT).astype(jnp.float32)
        absmax = jnp.max(jnp.abs(blocks), axis=1)
        divisor = jnp.maximum(absmax, 0.25)
        coded = (blocks / divisor[:, None, :]).astype(jnp.bfloat16)
        group_ids = groups[:, 0].astype(jnp.int32)
        per_dev = group_ids.reshape(N_TRAIN, BLOCKS_DEV)
        same_group = per_dev[:, :, None] == per_dev[:, None, :]
        order_in = jnp.sum((same_group & earlier[None]).astype(jnp.int32), axis=2).reshape(BLOCKS).astype(jnp.int32)
        flat_slot = ((group_ids * N_TRAIN + block_owner) * SLOTS + order_in).astype(jnp.int32)
        out_codes = jnp.zeros((N_SERVE * N_TRAIN * SLOTS, BLOCK, FEAT), jnp.bfloat16).at[flat_slot].set(coded)
        out_scales = jnp.zeros((N_SERVE * N_TRAIN * SLOTS, FEAT), jnp.float32).at[flat_slot].set(divisor)
        return (out_codes.reshape(N_SERVE, N_TRAIN, SLOTS, BLOCK, FEAT),
                out_scales.reshape(N_SERVE, N_TRAIN, SLOTS, FEAT))

    quant_codes, block_scales = lax.map(one_layer, (train_weights, block_group, row_offset))
    return quant_codes, block_scales
```

```python
import functools

import jax
import jax.numpy as jnp
from jax import lax
from jax.experimental import pallas as pl
from jax.experimental.pallas import tpu as pltpu
from jax.sharding import PartitionSpec as P

MESH = pl.DeviceIdType.MESH
BF = jnp.bfloat16
F32 = jnp.float32
LAYERS = 16
BLOCK = 32
BLOCKS_DEV = 28
ROWS_DEV = 896
COLS = 132
SERVE_N = 16
TRAIN_N = 8
SLOTS = 3
FEAT = SERVE_N * COLS
TILES = -(-FEAT // 128)
PARTS = (2, 4, 4, 4, 2)
FIRST = (0, 2, 6, 10, 14)
SIZES = tuple(n * SLOTS * BLOCK + 16 for n in PARTS)
BASES = tuple(sum(SIZES[:i]) for i in range(len(PARTS)))
TOTAL = sum(SIZES)
HALO = 16 + LAYERS * BLOCK
HALO_ENDS = tuple(16 + (f + n) * BLOCK for f, n in zip(FIRST, PARTS))
HALO_BASES = (0,) + HALO_ENDS[:-1]


def exchange(
    blocks_at, held, offsets, weights, out, scales,
    raw, edge, rot, lanes, tails, turned, rest, hsend, hrecv, send, recv, patch,
    raw_sem, edge_sem, hs_sem, hr_sem, s_sem, r_sem,
):
    t = lax.axis_index("train")
    me = lax.axis_index("serve")
    mx, my, mc = me // 8, lax.rem(me // 2, 4), lax.rem(me, 2)
    right, left = lax.rem(t + 1, TRAIN_N), lax.rem(t + TRAIN_N - 1, TRAIN_N)

    def peer(v):
        return (
            lax.rem(mx + v // 8, 2) * 8
            + lax.rem(my + lax.rem(v // 2, 4), 4) * 2
            + lax.rem(mc + lax.rem(v, 2), 2)
        )

    barrier = pltpu.get_barrier_semaphore()
    for v in range(1, SERVE_N):
        pl.semaphore_signal(barrier, inc=1, device_id={"serve": peer(v)}, device_id_type=MESH)
    for other in (left, right):
        pl.semaphore_signal(barrier, inc=1, device_id={"train": other}, device_id_type=MESH)

    edges = [
        pltpu.make_async_copy(weights.at[:, b], edge.at[side], edge_sem.at[side])
        for side, b in enumerate((BLOCKS_DEV + 1, 0))
    ]
    loads = [
        pltpu.make_async_copy(weights.at[pl.ds(f, n)], raw.at[pl.ds(f, n)], raw_sem.at[i])
        for i, (f, n) in enumerate(zip(FIRST, PARTS))
    ]
    for copy in edges + loads:
        copy.start()

    row = lax.broadcasted_iota(jnp.int32, (COLS, 256), 0)
    col = lax.broadcasted_iota(jnp.int32, (COLS, 256), 1)
    turn = (row < 128) & (col < 128) & (col == ((row + 4 * me) & 127))
    spread = (row >= 128) & (col >= 128) & ((col & 3) == row - 128)
    rot[...] = jnp.where(turn | spread, 1.0, 0.0).astype(BF)
    lane16 = lax.broadcasted_iota(jnp.int32, (16, 128), 1)
    for m in range(32):
        lanes[m] = jnp.where((lane16 >> 2) == m, 1.0, 0.0).astype(BF)
    rrow = lax.broadcasted_iota(jnp.int32, (128, 128), 0)
    rcol = lax.broadcasted_iota(jnp.int32, (128, 128), 1)
    patch[...] = jnp.where((rrow & 3) == (rcol & 3), 1.0, 0.0).astype(BF)

    for copy in edges:
        copy.wait()
    for side in range(2):
        def edge_step(i, total, side=side):
            x = edge[side, pl.ds(i * 4, 4)].reshape(4 * BLOCK, COLS)
            y = jnp.dot(x, rot[...], preferred_element_type=F32).astype(BF)
            hsend[side, pl.ds(pl.multiple_of(16 + i * 128, 16), 128)] = y[:, :128]
            for q in range(8):
                total = total + y[q * 16 : q * 16 + 16, 128:] * lanes[lax.rem(i * 8 + q + me, 32)]
            return total

        hsend[side, 0:16] = lax.fori_loop(0, LAYERS // 4, edge_step, jnp.zeros((16, 128), BF))

    pl.semaphore_wait(barrier, SERVE_N + 1)

    halos = []
    for i in range(len(PARTS)):
        window = pl.ds(HALO_BASES[i], HALO_ENDS[i] - HALO_BASES[i])
        for side, target in enumerate((right, left)):
            copy = pltpu.make_async_remote_copy(
                src_ref=hsend.at[side, window],
                dst_ref=hrecv.at[side, window],
                send_sem=hs_sem.at[side, i],
                recv_sem=hr_sem.at[side, i],
                device_id={"train": target},
                device_id_type=MESH,
            )
            copy.start()
            halos.append(copy)

    def block_copy(i, v):
        window = pl.ds(BASES[i], SIZES[i])
        return pltpu.make_async_remote_copy(
            src_ref=send.at[v, window],
            dst_ref=recv.at[me, window],
            send_sem=s_sem.at[i, v],
            recv_sem=r_sem.at[i, v],
            device_id={"serve": peer(v)},
            device_id_type=MESH,
        )

    block_row = lax.broadcasted_iota(jnp.int32, (BLOCK, 128), 0)

    for i, (f, n) in enumerate(zip(FIRST, PARTS)):
        loads[i].wait()

        def turn_step(j, carry, f=f):
            l, b = j // 7, lax.rem(j, 7) * 4
            x = raw[f + l, pl.ds(b + 1, 4)].reshape(4 * BLOCK, COLS)
            y = jnp.dot(x, rot[...], preferred_element_type=F32).astype(BF)
            turned[l, pl.ds(b, 4)] = y[:, :128].reshape(4, BLOCK, 128)
            rest[l, pl.ds(b, 4)] = y[:, 128:].reshape(4, BLOCK, 128)
            return carry

        lax.fori_loop(0, n * 7, turn_step, 0)
        halos[2 * i].wait_recv()
        halos[2 * i + 1].wait_recv()

        def patch_step(l, carry, f=f):
            layer = f + l
            first = offsets[layer, t] - t * ROWS_DEV
            last = offsets[layer, t + 1] - t * ROWS_DEV - (ROWS_DEV - BLOCK)
            for side, (b, take) in enumerate(
                ((0, block_row < first), (BLOCKS_DEV - 1, block_row >= last))
            ):
                main = hrecv[side, pl.ds(pl.multiple_of(16 + layer * BLOCK, 16), BLOCK)]
                packed = hrecv[side, 0:16]
                both = jnp.concatenate(
                    [packed * lanes[lax.rem(2 * layer + h + me, 32)] for h in range(2)], axis=0
                )
                tail = jnp.dot(both, patch[...], preferred_element_type=F32)
                turned[l, b] = jnp.where(take, main.astype(F32), turned[l, b].astype(F32)).astype(BF)
                rest[l, b] = jnp.where(take, tail, rest[l, b].astype(F32)).astype(BF)
            return carry

        lax.fori_loop(0, n, patch_step, 0)

        def fill(dest, index, group, i=i, f=f, n=n):
            total = jnp.zeros((16, 128), BF)
            for l in range(n):
                for k in range(SLOTS):
                    slot = l * SLOTS + k
                    b = blocks_at[f + l, group * SLOTS + k]
                    dest[index, pl.ds(BASES[i] + slot * BLOCK, BLOCK)] = turned[l, b]
                    pair = rest[l, b]
                    for h in range(2):
                        total = total + pair[h * 16 : h * 16 + 16] * lanes[
                            lax.rem(2 * slot + h + me, 32)
                        ]
            dest[index, pl.ds(BASES[i] + n * SLOTS * BLOCK, 16)] = total

        def send_step(j, carry, i=i, fill=fill):
            v = SERVE_N - 1 - j
            fill(send, v, peer(v))
            block_copy(i, v).start()
            return carry

        lax.fori_loop(0, SERVE_N - 1, send_step, 0)
        fill(recv, me, me)

    lane = lax.broadcasted_iota(jnp.int32, (BLOCK, 128), 1)
    for i, (f, n) in enumerate(zip(FIRST, PARTS)):
        def arrive(j, carry, i=i):
            block_copy(i, j + 1).wait_recv()
            return carry

        lax.fori_loop(0, SERVE_N - 1, arrive, 0)

        def tail_step(q, carry, i=i, n=n):
            total = jnp.zeros((16, 128), BF)
            for s in range(SERVE_N):
                total = total + recv[s, pl.ds(BASES[i] + n * SLOTS * BLOCK, 16)] * lanes[
                    lax.rem(q + s, 32)
                ]
            tails[q // 2, pl.ds(pl.multiple_of(lax.rem(q, 2) * 16, 16), 16)] = pltpu.roll(
                total.astype(F32), 128 - 4 * q, axis=1
            )
            return carry

        lax.fori_loop(0, 2 * n * SLOTS, tail_step, 0)

        def block_step(slot, carry, i=i, f=f):
            layer, k = f + slot // SLOTS, lax.rem(slot, SLOTS)
            there = held[layer, me * SLOTS + k].astype(F32)
            at = f * SLOTS + slot
            tail = tails[slot]
            before = None
            for j in range(TILES):
                if j < SERVE_N:
                    now = recv[j, pl.ds(pl.multiple_of(BASES[i] + slot * BLOCK, 16), BLOCK)].astype(F32)
                else:
                    now = tail
                if j == 0:
                    value = now
                else:
                    value = jnp.where(
                        lane < 4 * j - 4, before, jnp.where(lane < 4 * j, tail, now)
                    )
                before = now
                top = jnp.maximum(jnp.max(jnp.abs(value), axis=0, keepdims=True), 0.25)
                codes = (value * (there / top)).astype(BF)
                width = min(128, FEAT - j * 128)
                out[at, :, j * 128 : j * 128 + width] = codes[:, :width]
                scales[at, :, j * 128 : j * 128 + width] = (top * there)[:, :width]
            return carry

        lax.fori_loop(0, n * SLOTS, block_step, 0)

    for copy in halos:
        copy.wait_send()
    for i in range(len(PARTS)):
        def leave(j, carry, i=i):
            block_copy(i, j + 1).wait_send()
            return carry

        lax.fori_loop(0, SERVE_N - 1, leave, 0)


def shards(train_weights, row_offset, block_group):
    groups = block_group[:, :, 0]
    position = jnp.arange(BLOCKS_DEV, dtype=jnp.int32)
    earlier = position[None, :] < position[:, None]
    same = groups[:, :, None] == groups[:, None, :]
    order = jnp.sum((same & earlier[None]).astype(jnp.int32), axis=2)
    slot_id = groups * SLOTS + order
    onehot = slot_id[:, None, :] == jnp.arange(SERVE_N * SLOTS, dtype=jnp.int32)[None, :, None]
    blocks_at = jnp.sum(jnp.where(onehot, position[None, None, :], 0), axis=2)
    held = jnp.sum(onehot.astype(jnp.int32), axis=2)
    weights = train_weights.reshape(LAYERS, BLOCKS_DEV + 2, BLOCK, COLS)
    parts = len(PARTS)
    smem = pl.BlockSpec(memory_space=pltpu.SMEM)
    vmem = pl.BlockSpec(memory_space=pltpu.VMEM)
    codes, scales = pl.pallas_call(
        exchange,
        out_shape=(
            pltpu.VMEM((LAYERS * SLOTS, BLOCK, FEAT), BF),
            pltpu.VMEM((LAYERS * SLOTS, 1, FEAT), F32),
        ),
        in_specs=[smem, smem, smem, pl.BlockSpec(memory_space=pl.ANY)],
        out_specs=(vmem, vmem),
        scratch_shapes=[
            pltpu.VMEM((LAYERS, BLOCKS_DEV + 2, BLOCK, COLS), BF),
            pltpu.VMEM((2, LAYERS, BLOCK, COLS), BF),
            pltpu.VMEM((COLS, 256), BF),
            pltpu.VMEM((32, 16, 128), BF),
            pltpu.VMEM((max(PARTS) * SLOTS, BLOCK, 128), F32),
            pltpu.VMEM((max(PARTS), BLOCKS_DEV, BLOCK, 128), BF),
            pltpu.VMEM((max(PARTS), BLOCKS_DEV, BLOCK, 128), BF),
            pltpu.VMEM((2, HALO, 128), BF),
            pltpu.VMEM((2, HALO, 128), BF),
            pltpu.VMEM((SERVE_N, TOTAL, 128), BF),
            pltpu.VMEM((SERVE_N, TOTAL, 128), BF),
            pltpu.VMEM((128, 128), BF),
            pltpu.SemaphoreType.DMA((parts,)),
            pltpu.SemaphoreType.DMA((2,)),
            pltpu.SemaphoreType.DMA((2, parts)),
            pltpu.SemaphoreType.DMA((2, parts)),
            pltpu.SemaphoreType.DMA((parts, SERVE_N)),
            pltpu.SemaphoreType.DMA((parts, SERVE_N)),
        ],
        compiler_params=pltpu.CompilerParams(
            collective_id=1, has_side_effects=True, vmem_limit_bytes=44 * 2**20
        ),
    )(blocks_at, held, row_offset, weights)
    return (
        codes.reshape(LAYERS, 1, 1, SLOTS, BLOCK, FEAT),
        scales.reshape(LAYERS, 1, 1, SLOTS, FEAT),
    )


def solution(mesh):
    return jax.shard_map(
        shards,
        mesh=mesh,
        in_specs=(P(None, "train", "serve"), P(), P(None, "train", None)),
        out_specs=(P(None, "serve", "train", None, None, None), P(None, "serve", "train", None, None)),
        check_vma=False,
    )
```

```python
import functools

import jax
import jax.numpy as jnp
from jax import lax
from jax.experimental import pallas as pl
from jax.experimental.pallas import tpu as pltpu
from jax.sharding import PartitionSpec as P

MESH = pl.DeviceIdType.MESH
BF = jnp.bfloat16
F32 = jnp.float32
I32 = jnp.int32
LAYERS = 16
BLOCK = 32
BLOCKS_DEV = 28
HELD = BLOCKS_DEV + 2
ROWS_DEV = 896
BUFFER = HELD * BLOCK
COLS = 132
SERVE_N = 16
TRAIN_N = 8
SLOTS = 3
FEAT = SERVE_N * COLS
TILES = -(-FEAT // 128)

PARTS = (2, 4, 4, 4, 2)
FIRST = (0, 2, 6, 10, 14)
SIZES = tuple(n * SLOTS * BLOCK + 16 for n in PARTS)
BASES = tuple(sum(SIZES[:i]) for i in range(len(PARTS)))
TOTAL = sum(SIZES)
HALO = 16 + LAYERS * BLOCK
HALO_ENDS = tuple(16 + (f + n) * BLOCK for f, n in zip(FIRST, PARTS))
HALO_BASES = (0,) + HALO_ENDS[:-1]

BASE = 2
EXTRA = 8
MESSAGES = ((0, 2, 0), (2, 8, 0), (10, 4, EXTRA), (14, 2, 0))
LENGTHS = tuple((n * BASE + e) * BLOCK + 16 for _, n, e in MESSAGES)
PAIRS = LAYERS // 2
EARLY = 5
EDGE = BLOCK + LAYERS * BLOCK


def full_exchange(
    blocks_at, held, offsets, weights, out, scales,
    raw, edge, rot, lanes, tails, turned, rest, hsend, hrecv, send, recv, patch,
    raw_sem, edge_sem, hs_sem, hr_sem, s_sem, r_sem,
):
    t = lax.axis_index("train")
    me = lax.axis_index("serve")
    mx, my, mc = me // 8, lax.rem(me // 2, 4), lax.rem(me, 2)
    right, left = lax.rem(t + 1, TRAIN_N), lax.rem(t + TRAIN_N - 1, TRAIN_N)

    def peer(v):
        return (
            lax.rem(mx + v // 8, 2) * 8
            + lax.rem(my + lax.rem(v // 2, 4), 4) * 2
            + lax.rem(mc + lax.rem(v, 2), 2)
        )

    barrier = pltpu.get_barrier_semaphore()
    for v in range(1, SERVE_N):
        pl.semaphore_signal(barrier, inc=1, device_id={"serve": peer(v)}, device_id_type=MESH)
    for other in (left, right):
        pl.semaphore_signal(barrier, inc=1, device_id={"train": other}, device_id_type=MESH)

    edges = [
        pltpu.make_async_copy(weights.at[:, b], edge.at[side], edge_sem.at[side])
        for side, b in enumerate((BLOCKS_DEV + 1, 0))
    ]
    loads = [
        pltpu.make_async_copy(weights.at[pl.ds(f, n)], raw.at[pl.ds(f, n)], raw_sem.at[i])
        for i, (f, n) in enumerate(zip(FIRST, PARTS))
    ]
    for copy in edges + loads:
        copy.start()

    row = lax.broadcasted_iota(jnp.int32, (COLS, 256), 0)
    col = lax.broadcasted_iota(jnp.int32, (COLS, 256), 1)
    turn = (row < 128) & (col < 128) & (col == ((row + 4 * me) & 127))
    spread = (row >= 128) & (col >= 128) & ((col & 3) == row - 128)
    rot[...] = jnp.where(turn | spread, 1.0, 0.0).astype(BF)
    lane16 = lax.broadcasted_iota(jnp.int32, (16, 128), 1)
    for m in range(32):
        lanes[m] = jnp.where((lane16 >> 2) == m, 1.0, 0.0).astype(BF)
    rrow = lax.broadcasted_iota(jnp.int32, (128, 128), 0)
    rcol = lax.broadcasted_iota(jnp.int32, (128, 128), 1)
    patch[...] = jnp.where((rrow & 3) == (rcol & 3), 1.0, 0.0).astype(BF)

    for copy in edges:
        copy.wait()
    for side in range(2):
        def edge_step(i, total, side=side):
            x = edge[side, pl.ds(i * 4, 4)].reshape(4 * BLOCK, COLS)
            y = jnp.dot(x, rot[...], preferred_element_type=F32).astype(BF)
            hsend[side, pl.ds(pl.multiple_of(16 + i * 128, 16), 128)] = y[:, :128]
            for q in range(8):
                total = total + y[q * 16 : q * 16 + 16, 128:] * lanes[lax.rem(i * 8 + q + me, 32)]
            return total

        hsend[side, 0:16] = lax.fori_loop(0, LAYERS // 4, edge_step, jnp.zeros((16, 128), BF))

    pl.semaphore_wait(barrier, SERVE_N + 1)

    halos = []
    for i in range(len(PARTS)):
        window = pl.ds(HALO_BASES[i], HALO_ENDS[i] - HALO_BASES[i])
        for side, target in enumerate((right, left)):
            copy = pltpu.make_async_remote_copy(
                src_ref=hsend.at[side, window],
                dst_ref=hrecv.at[side, window],
                send_sem=hs_sem.at[side, i],
                recv_sem=hr_sem.at[side, i],
                device_id={"train": target},
                device_id_type=MESH,
            )
            copy.start()
            halos.append(copy)

    def block_copy(i, v):
        window = pl.ds(BASES[i], SIZES[i])
        return pltpu.make_async_remote_copy(
            src_ref=send.at[v, window],
            dst_ref=recv.at[me, window],
            send_sem=s_sem.at[i, v],
            recv_sem=r_sem.at[i, v],
            device_id={"serve": peer(v)},
            device_id_type=MESH,
        )

    block_row = lax.broadcasted_iota(jnp.int32, (BLOCK, 128), 0)

    for i, (f, n) in enumerate(zip(FIRST, PARTS)):
        loads[i].wait()

        def turn_step(j, carry, f=f):
            l, b = j // 7, lax.rem(j, 7) * 4
            x = raw[f + l, pl.ds(b + 1, 4)].reshape(4 * BLOCK, COLS)
            y = jnp.dot(x, rot[...], preferred_element_type=F32).astype(BF)
            turned[l, pl.ds(b, 4)] = y[:, :128].reshape(4, BLOCK, 128)
            rest[l, pl.ds(b, 4)] = y[:, 128:].reshape(4, BLOCK, 128)
            return carry

        lax.fori_loop(0, n * 7, turn_step, 0)
        halos[2 * i].wait_recv()
        halos[2 * i + 1].wait_recv()

        def patch_step(l, carry, f=f):
            layer = f + l
            first = offsets[layer, t] - t * ROWS_DEV
            last = offsets[layer, t + 1] - t * ROWS_DEV - (ROWS_DEV - BLOCK)
            for side, (b, take) in enumerate(
                ((0, block_row < first), (BLOCKS_DEV - 1, block_row >= last))
            ):
                main = hrecv[side, pl.ds(pl.multiple_of(16 + layer * BLOCK, 16), BLOCK)]
                packed = hrecv[side, 0:16]
                both = jnp.concatenate(
                    [packed * lanes[lax.rem(2 * layer + h + me, 32)] for h in range(2)], axis=0
                )
                tail = jnp.dot(both, patch[...], preferred_element_type=F32)
                turned[l, b] = jnp.where(take, main.astype(F32), turned[l, b].astype(F32)).astype(BF)
                rest[l, b] = jnp.where(take, tail, rest[l, b].astype(F32)).astype(BF)
            return carry

        lax.fori_loop(0, n, patch_step, 0)

        def fill(dest, index, group, i=i, f=f, n=n):
            total = jnp.zeros((16, 128), BF)
            for l in range(n):
                for k in range(SLOTS):
                    slot = l * SLOTS + k
                    b = blocks_at[f + l, group * SLOTS + k]
                    dest[index, pl.ds(BASES[i] + slot * BLOCK, BLOCK)] = turned[l, b]
                    pair = rest[l, b]
                    for h in range(2):
                        total = total + pair[h * 16 : h * 16 + 16] * lanes[
                            lax.rem(2 * slot + h + me, 32)
                        ]
            dest[index, pl.ds(BASES[i] + n * SLOTS * BLOCK, 16)] = total

        def send_step(j, carry, i=i, fill=fill):
            v = SERVE_N - 1 - j
            fill(send, v, peer(v))
            block_copy(i, v).start()
            return carry

        lax.fori_loop(0, SERVE_N - 1, send_step, 0)
        fill(recv, me, me)

    lane = lax.broadcasted_iota(jnp.int32, (BLOCK, 128), 1)
    for i, (f, n) in enumerate(zip(FIRST, PARTS)):
        def arrive(j, carry, i=i):
            block_copy(i, j + 1).wait_recv()
            return carry

        lax.fori_loop(0, SERVE_N - 1, arrive, 0)

        def tail_step(q, carry, i=i, n=n):
            total = jnp.zeros((16, 128), BF)
            for s in range(SERVE_N):
                total = total + recv[s, pl.ds(BASES[i] + n * SLOTS * BLOCK, 16)] * lanes[
                    lax.rem(q + s, 32)
                ]
            tails[q // 2, pl.ds(pl.multiple_of(lax.rem(q, 2) * 16, 16), 16)] = pltpu.roll(
                total.astype(F32), 128 - 4 * q, axis=1
            )
            return carry

        lax.fori_loop(0, 2 * n * SLOTS, tail_step, 0)

        def block_step(slot, carry, i=i, f=f):
            layer, k = f + slot // SLOTS, lax.rem(slot, SLOTS)
            there = held[layer, me * SLOTS + k].astype(F32)
            at = f * SLOTS + slot
            tail = tails[slot]
            before = None
            for j in range(TILES):
                if j < SERVE_N:
                    now = recv[j, pl.ds(pl.multiple_of(BASES[i] + slot * BLOCK, 16), BLOCK)].astype(F32)
                else:
                    now = tail
                if j == 0:
                    value = now
                else:
                    value = jnp.where(
                        lane < 4 * j - 4, before, jnp.where(lane < 4 * j, tail, now)
                    )
                before = now
                top = jnp.maximum(jnp.max(jnp.abs(value), axis=0, keepdims=True), 0.25)
                codes = (value * (there / top)).astype(BF)
                width = min(128, FEAT - j * 128)
                out[at, :, j * 128 : j * 128 + width] = codes[:, :width]
                scales[at, :, j * 128 : j * 128 + width] = (top * there)[:, :width]
            return carry

        lax.fori_loop(0, n * SLOTS, block_step, 0)

    for copy in halos:
        copy.wait_send()
    for i in range(len(PARTS)):
        def leave(j, carry, i=i):
            block_copy(i, j + 1).wait_send()
            return carry

        lax.fori_loop(0, SERVE_N - 1, leave, 0)


def route(
    blocks_at, extra_at, counts, extra_pos, over, offsets, weights, out, scales, flag,
    raw, eye, mixed, mixed_tail, pick, pick_pair, lanes, rows16, turned, rest,
    hsend, hrecv, tails, extra_codes, extra_scales, fsend, frecv,
    send0, send1, send2, send3, recv0, recv1, recv2, recv3,
    raw_sem, hs_sem, hr_sem, s_sem, r_sem, fs_sem, fr_sem,
):
    sends, recvs = (send0, send1, send2, send3), (recv0, recv1, recv2, recv3)
    t = lax.axis_index("train")
    me = lax.axis_index("serve")
    mx, my, mc = me // 8, lax.rem(me // 2, 4), lax.rem(me, 2)
    right, left = lax.rem(t + 1, TRAIN_N), lax.rem(t + TRAIN_N - 1, TRAIN_N)

    def peer(v):
        return (
            lax.rem(mx + v // 8, 2) * 8
            + lax.rem(my + lax.rem(v // 2, 4), 4) * 2
            + lax.rem(mc + lax.rem(v, 2), 2)
        )

    barrier = pltpu.get_barrier_semaphore()
    for v in range(1, SERVE_N):
        pl.semaphore_signal(barrier, inc=1, device_id={"serve": peer(v)}, device_id_type=MESH)
    for step in range(1, TRAIN_N):
        pl.semaphore_signal(
            barrier, inc=1, device_id={"train": lax.rem(t + step, TRAIN_N)}, device_id_type=MESH
        )

    def load(m, rows=16):
        window = pl.ds(16 * m, rows)
        return pltpu.make_async_copy(weights.at[window], raw.at[window], raw_sem.at[m])

    for m in range(8):
        load(m).start()
    load(8, 4).start()

    def index(shape, dim):
        return lax.broadcasted_iota(I32, shape, dim)

    def ones(cond):
        return jnp.where(cond, 1.0, 0.0).astype(BF)

    eye[...] = ones(index((256, 256), 0) == index((256, 256), 1))
    lane16, row16 = index((16, 128), 1), index((16, 128), 0)
    for m in range(32):
        lanes[m] = ones((lane16 >> 2) == m)
    for m in range(LAYERS):
        rows16[m] = ones(row16 == m)
    fsend[...] = jnp.full((8, 128), over[0, 0], F32)
    frecv[t] = fsend[...]

    NT = (((1,), (1,)), ((), ()))

    def mix_step(m, carry):
        load(m).wait()
        for r in range(0, BUFFER, 256):
            w = min(256, BUFFER - r)
            x = raw[pl.ds(16 * m, 16), :, r : r + w].reshape(256, w)
            y = lax.dot_general(eye[:w, :w], x, NT, preferred_element_type=F32)
            mixed[r : r + w, pl.ds(pl.multiple_of(256 * m, 256), 256)] = y.astype(BF)
        return carry

    lax.fori_loop(0, 8, mix_step, 0)
    load(8, 4).wait()
    for r in range(0, BUFFER, 256):
        w = min(256, BUFFER - r)
        x = raw[128:132, :, r : r + w].reshape(64, w)
        y = lax.dot_general(eye[:w, :w], x, NT, preferred_element_type=F32)
        mixed_tail[r : r + w] = y.astype(BF)

    def pick_step(m, carry):
        column = index((256, 128), 0) >> 4
        lane = index((256, 128), 1)
        pick[pl.ds(pl.multiple_of(256 * m, 256), 256)] = ones(
            ((lane - 4 * me - 16 * m) & 127) == column
        )
        return carry

    lax.fori_loop(0, 8, pick_step, 0)

    def tail_pick(p):
        k, q = index((64, 256), 0), index((64, 256), 1)
        return ones(((k & 15) == 2 * p + (q >> 7)) & ((k >> 4) == (q & 3)))

    hsend[0, 0:BLOCK, 0:64] = mixed_tail[BUFFER - BLOCK : BUFFER]
    hsend[1, 0:BLOCK, 0:64] = mixed_tail[0:BLOCK]
    hsend[0, 0:BLOCK, 64:128] = jnp.zeros((BLOCK, 64), BF)
    hsend[1, 0:BLOCK, 64:128] = jnp.zeros((BLOCK, 64), BF)

    def prepare(p):
        def pair_step(c, carry):
            window = pl.ds(pl.multiple_of(16 * c, 16), 16)
            for h in range(2):
                pick_pair[window, 128 * h : 128 * h + 128] = pick[window] * rows16[2 * p + h]
            return carry

        lax.fori_loop(0, 128, pair_step, 0, unroll=8)
        tail_of = tail_pick(p)

        def turn_step(i, carry):
            window = pl.ds(pl.multiple_of(192 * i, 64), 192)
            y = jnp.dot(mixed[window], pick_pair[...], preferred_element_type=F32).astype(BF)
            z = jnp.dot(mixed_tail[window], tail_of, preferred_element_type=F32).astype(BF)
            for h in range(2):
                at = pl.ds((2 * p + h) * HELD + 6 * i, 6)
                turned[at] = y[:, 128 * h : 128 * h + 128].reshape(6, BLOCK, 128)
                rest[at] = z[:, 128 * h : 128 * h + 128].reshape(6, BLOCK, 128)
            return carry

        lax.fori_loop(0, BUFFER // 192, turn_step, 0)
        for h in range(2):
            layer = 2 * p + h
            window = pl.ds(pl.multiple_of(BLOCK + layer * BLOCK, BLOCK), BLOCK)
            hsend[0, window] = turned[layer * HELD + HELD - 1]
            hsend[1, window] = turned[layer * HELD]

    def halo(side, p):
        if isinstance(p, int) and p == 0:
            window = pl.ds(0, 3 * BLOCK)
        else:
            window = pl.ds(pl.multiple_of(BLOCK + 2 * BLOCK * p, BLOCK), 2 * BLOCK)
        return pltpu.make_async_remote_copy(
            src_ref=hsend.at[side, window],
            dst_ref=hrecv.at[side, window],
            send_sem=hs_sem.at[side, p],
            recv_sem=hr_sem.at[side, p],
            device_id={"train": (right, left)[side]},
            device_id_type=MESH,
        )

    def prepare_step(p, carry):
        prepare(p)
        for side in range(2):
            halo(side, p).start()
        return carry

    block_row = index((BLOCK, 128), 0)

    def patch(p):
        tail_of = tail_pick(p)
        for side, (b, last) in enumerate(((1, False), (HELD - 2, True))):
            tail = jnp.dot(hrecv[side, 0:BLOCK, 0:64], tail_of, preferred_element_type=F32)
            for h in range(2):
                layer = 2 * p + h
                if last:
                    take = block_row >= offsets[layer, t + 1] - t * ROWS_DEV - (ROWS_DEV - BLOCK)
                else:
                    take = block_row < offsets[layer, t] - t * ROWS_DEV
                at = layer * HELD + b
                window = pl.ds(pl.multiple_of(BLOCK + layer * BLOCK, BLOCK), BLOCK)
                main = hrecv[side, window].astype(F32)
                turned[at] = jnp.where(take, main, turned[at].astype(F32)).astype(BF)
                rest[at] = jnp.where(
                    take, tail[:, 128 * h : 128 * h + 128], rest[at].astype(F32)
                ).astype(BF)

    def patch_step(p, carry):
        for side in range(2):
            halo(side, p).wait_recv()
        patch(p)
        return carry

    def message(i, v):
        return pltpu.make_async_remote_copy(
            src_ref=sends[i].at[v],
            dst_ref=recvs[i].at[me],
            send_sem=s_sem.at[i, v],
            recv_sem=r_sem.at[i, v],
            device_id={"serve": peer(v)},
            device_id_type=MESH,
        )

    def dispatch(i):
        f, n, e = MESSAGES[i]

        def fill(dest, place, group):
            total = jnp.zeros((16, 128), BF)
            for slot in range(n * BASE + e):
                if slot < n * BASE:
                    layer, k = f + slot // BASE, slot % BASE
                    at = layer * HELD + 1 + blocks_at[layer, group * SLOTS + k]
                else:
                    at = extra_at[group, slot - n * BASE]
                dest[place, slot * BLOCK : slot * BLOCK + BLOCK] = turned[at]
                pair = rest[at]
                for h in range(2):
                    mask = lanes[lax.rem(2 * slot + h + me, 32)]
                    total = total + pair[h * 16 : h * 16 + 16] * mask
            dest[place, LENGTHS[i] - 16 : LENGTHS[i]] = total

        def send_step(j, carry):
            v = SERVE_N - 1 - j
            fill(sends[i], v, peer(v))
            message(i, v).start()
            return carry

        lax.fori_loop(0, SERVE_N - 1, send_step, 0)
        fill(recvs[i], me, me)

    lane = index((BLOCK, 128), 1)

    def finish(i):
        f, n, e = MESSAGES[i]
        recv = recvs[i]

        def arrive(j, carry):
            message(i, j + 1).wait_recv()
            return carry

        lax.fori_loop(0, SERVE_N - 1, arrive, 0)

        def tail_step(q, carry):
            total = jnp.zeros((16, 128), BF)
            for s in range(SERVE_N):
                total = total + recv[s, LENGTHS[i] - 16 : LENGTHS[i]] * lanes[lax.rem(q + s, 32)]
            tails[q // 2, pl.ds(pl.multiple_of(lax.rem(q, 2) * 16, 16), 16)] = pltpu.roll(
                total.astype(F32), 128 - 4 * q, axis=1
            )
            return carry

        lax.fori_loop(0, 2 * (n * BASE + e), tail_step, 0)

        def scale_block(slot, at, there, codes_out, scales_out):
            tail = tails[slot]
            before = None
            for j in range(TILES):
                if j < SERVE_N:
                    now = recv[j, pl.ds(pl.multiple_of(slot * BLOCK, BLOCK), BLOCK)].astype(F32)
                else:
                    now = tail
                if j == 0:
                    value = now
                else:
                    value = jnp.where(
                        lane < 4 * j - 4, before, jnp.where(lane < 4 * j, tail, now)
                    )
                before = now
                top = jnp.maximum(jnp.max(jnp.abs(value), axis=0, keepdims=True), 0.25)
                codes = (value * (there / top)).astype(BF)
                width = min(128, FEAT - j * 128)
                codes_out[at, :, j * 128 : j * 128 + width] = codes[:, :width]
                scales_out[at, :, j * 128 : j * 128 + width] = (top * there)[:, :width]

        def present(layer, k):
            return jnp.minimum(jnp.maximum(counts[layer, me] - k, 0), 1).astype(F32)

        def base_step(slot, carry):
            layer, k = f + slot // BASE, lax.rem(slot, BASE)
            scale_block(slot, layer * SLOTS + k, present(layer, k), out, scales)
            return carry

        lax.fori_loop(0, n * BASE, base_step, 0)
        if e:
            def extra_step(entry, carry):
                scale_block(n * BASE + entry, entry, 1.0, extra_codes, extra_scales)
                return carry

            lax.fori_loop(0, e, extra_step, 0)

            def place_step(layer, carry):
                entry, there = extra_pos[layer, me], present(layer, BASE)
                at = layer * SLOTS + BASE
                out[at] = (extra_codes[entry].astype(F32) * there).astype(BF)
                scales[at] = extra_scales[entry] * there
                return carry

            lax.fori_loop(0, LAYERS, place_step, 0)

    def tell(step):
        return pltpu.make_async_remote_copy(
            src_ref=fsend,
            dst_ref=frecv.at[t],
            send_sem=fs_sem.at[step],
            recv_sem=fr_sem.at[step],
            device_id={"train": lax.rem(t + step, TRAIN_N)},
            device_id_type=MESH,
        )

    pl.semaphore_wait(barrier, SERVE_N + TRAIN_N - 2)
    prepare(0)
    for side in range(2):
        halo(side, 0).start()
    lax.fori_loop(1, EARLY, prepare_step, 0)
    for side in range(2):
        halo(side, 0).wait_recv()
    patch(0)
    dispatch(0)
    lax.fori_loop(EARLY, PAIRS, prepare_step, 0)
    lax.fori_loop(1, EARLY, patch_step, 0)
    dispatch(1)
    lax.fori_loop(EARLY, PAIRS, patch_step, 0)
    dispatch(2)
    dispatch(3)
    for step in range(1, TRAIN_N):
        tell(step).start()
    finish(0)
    finish(1)
    finish(2)
    finish(3)
    for step in range(1, TRAIN_N):
        tell(step).wait()
    flag[...] = jnp.max(frecv[...], axis=0)

    for side in range(2):
        halo(side, 0).wait_send()

        def halo_left(p, carry, side=side):
            halo(side, p).wait_send()
            return carry

        lax.fori_loop(1, PAIRS, halo_left, 0)
    for i in range(len(MESSAGES)):
        def leave(j, carry, i=i):
            message(i, j + 1).wait_send()
            return carry

        lax.fori_loop(0, SERVE_N - 1, leave, 0)


def everything(train_weights, row_offset, blocks_at, counts):
    held = (counts[:, :, None] > jnp.arange(SLOTS, dtype=I32)).astype(I32)
    held = held.reshape(LAYERS, SERVE_N * SLOTS)
    weights = train_weights.reshape(LAYERS, HELD, BLOCK, COLS)
    parts = len(PARTS)
    smem = pl.BlockSpec(memory_space=pltpu.SMEM)
    vmem = pl.BlockSpec(memory_space=pltpu.VMEM)
    return pl.pallas_call(
        full_exchange,
        out_shape=(
            pltpu.VMEM((LAYERS * SLOTS, BLOCK, FEAT), BF),
            pltpu.VMEM((LAYERS * SLOTS, 1, FEAT), F32),
        ),
        in_specs=[smem, smem, smem, pl.BlockSpec(memory_space=pl.ANY)],
        out_specs=(vmem, vmem),
        scratch_shapes=[
            pltpu.VMEM((LAYERS, HELD, BLOCK, COLS), BF),
            pltpu.VMEM((2, LAYERS, BLOCK, COLS), BF),
            pltpu.VMEM((COLS, 256), BF),
            pltpu.VMEM((32, 16, 128), BF),
            pltpu.VMEM((max(PARTS) * SLOTS, BLOCK, 128), F32),
            pltpu.VMEM((max(PARTS), BLOCKS_DEV, BLOCK, 128), BF),
            pltpu.VMEM((max(PARTS), BLOCKS_DEV, BLOCK, 128), BF),
            pltpu.VMEM((2, HALO, 128), BF),
            pltpu.VMEM((2, HALO, 128), BF),
            pltpu.VMEM((SERVE_N, TOTAL, 128), BF),
            pltpu.VMEM((SERVE_N, TOTAL, 128), BF),
            pltpu.VMEM((128, 128), BF),
            pltpu.SemaphoreType.DMA((parts,)),
            pltpu.SemaphoreType.DMA((2,)),
            pltpu.SemaphoreType.DMA((2, parts)),
            pltpu.SemaphoreType.DMA((2, parts)),
            pltpu.SemaphoreType.DMA((parts, SERVE_N)),
            pltpu.SemaphoreType.DMA((parts, SERVE_N)),
        ],
        compiler_params=pltpu.CompilerParams(
            collective_id=1, has_side_effects=True, vmem_limit_bytes=44 * 2**20
        ),
    )(blocks_at, held, row_offset, weights)


def shards(train_weights, row_offset, block_group):
    groups = block_group[:, :, 0]
    position = jnp.arange(BLOCKS_DEV, dtype=I32)
    earlier = position[None, :] < position[:, None]
    same = groups[:, :, None] == groups[:, None, :]
    order = jnp.sum((same & earlier[None]).astype(I32), axis=2)
    slot_id = groups * SLOTS + order
    onehot = slot_id[:, None, :] == jnp.arange(SERVE_N * SLOTS, dtype=I32)[None, :, None]
    blocks_at = jnp.sum(jnp.where(onehot, position[None, None, :], 0), axis=2)
    group_ids = jnp.arange(SERVE_N, dtype=I32)
    counts = jnp.sum((groups[:, None, :] == group_ids[None, :, None]).astype(I32), axis=2)
    third = counts > BASE
    layer_ids = jnp.arange(LAYERS, dtype=I32)
    before = jnp.sum(
        (third[None] & (layer_ids[None, :] < layer_ids[:, None])[:, :, None]).astype(I32), axis=1
    )
    over = jnp.max(jnp.sum(third.astype(F32), axis=0)) > EXTRA
    third_at = layer_ids[:, None] * HELD + 1 + blocks_at[:, BASE::SLOTS]
    chosen = third[:, :, None] & (before[:, :, None] == jnp.arange(EXTRA, dtype=I32))
    extra_at = jnp.sum(jnp.where(chosen, third_at[:, :, None], 0), axis=0)
    extra_pos = jnp.minimum(before, EXTRA - 1)
    smem = pl.BlockSpec(memory_space=pltpu.SMEM)
    vmem = pl.BlockSpec(memory_space=pltpu.VMEM)
    parts = len(MESSAGES)
    codes, scales, flag = pl.pallas_call(
        route,
        out_shape=(
            pltpu.VMEM((LAYERS * SLOTS, BLOCK, FEAT), BF),
            pltpu.VMEM((LAYERS * SLOTS, 1, FEAT), F32),
            jax.ShapeDtypeStruct((8, 128), F32),
        ),
        in_specs=[smem] * 6 + [pl.BlockSpec(memory_space=pl.ANY)],
        out_specs=(vmem, vmem, vmem),
        scratch_shapes=[
            pltpu.VMEM((COLS, LAYERS, BUFFER), BF),
            pltpu.VMEM((256, 256), BF),
            pltpu.VMEM((BUFFER, 128 * LAYERS), BF),
            pltpu.VMEM((BUFFER, 64), BF),
            pltpu.VMEM((128 * LAYERS, 128), BF),
            pltpu.VMEM((128 * LAYERS, 256), BF),
            pltpu.VMEM((32, 16, 128), BF),
            pltpu.VMEM((LAYERS, 16, 128), BF),
            pltpu.VMEM((LAYERS * HELD, BLOCK, 128), BF),
            pltpu.VMEM((LAYERS * HELD, BLOCK, 128), BF),
            pltpu.VMEM((2, EDGE, 128), BF),
            pltpu.VMEM((2, EDGE, 128), BF),
            pltpu.VMEM((16, BLOCK, 128), F32),
            pltpu.VMEM((EXTRA, BLOCK, FEAT), BF),
            pltpu.VMEM((EXTRA, 1, FEAT), F32),
            pltpu.VMEM((8, 128), F32),
            pltpu.VMEM((TRAIN_N, 8, 128), F32),
            *[pltpu.VMEM((SERVE_N, length, 128), BF) for length in LENGTHS * 2],
            pltpu.SemaphoreType.DMA((9,)),
            pltpu.SemaphoreType.DMA((2, PAIRS)),
            pltpu.SemaphoreType.DMA((2, PAIRS)),
            pltpu.SemaphoreType.DMA((parts, SERVE_N)),
            pltpu.SemaphoreType.DMA((parts, SERVE_N)),
            pltpu.SemaphoreType.DMA((TRAIN_N,)),
            pltpu.SemaphoreType.DMA((TRAIN_N,)),
        ],
        compiler_params=pltpu.CompilerParams(
            collective_id=2, has_side_effects=True, vmem_limit_bytes=46 * 2**20
        ),
    )(
        blocks_at, extra_at, counts, extra_pos, over.astype(F32).reshape(1, 1), row_offset,
        jnp.transpose(train_weights, (2, 0, 1)),
    )
    codes, scales = lax.cond(
        flag[0, 0] > 0.0,
        lambda: tuple(everything(train_weights, row_offset, blocks_at, counts)),
        lambda: (codes, scales),
    )
    return (
        codes.reshape(LAYERS, 1, 1, SLOTS, BLOCK, FEAT),
        scales.reshape(LAYERS, 1, 1, SLOTS, FEAT),
    )


def solution(mesh):
    return jax.shard_map(
        shards,
        mesh=mesh,
        in_specs=(P(None, "train", "serve"), P(), P(None, "train", None)),
        out_specs=(P(None, "serve", "train", None, None, None), P(None, "serve", "train", None, None)),
        check_vma=False,
    )
```

```python
import functools

import jax
import jax.numpy as jnp
from jax import lax
from jax.experimental import pallas as pl
from jax.experimental.pallas import tpu as pltpu
from jax.sharding import PartitionSpec as P

MESH = pl.DeviceIdType.MESH
BF = jnp.bfloat16
F32 = jnp.float32
I32 = jnp.int32
LAYERS = 16
BLOCK = 32
BLOCKS_DEV = 28
HELD = BLOCKS_DEV + 2
ROWS_DEV = 896
BUFFER = HELD * BLOCK
COLS = 132
SERVE_N = 16
TRAIN_N = 8
SLOTS = 3
FEAT = SERVE_N * COLS
TILES = -(-FEAT // 128)

PARTS = (2, 4, 4, 4, 2)
FIRST = (0, 2, 6, 10, 14)
SIZES = tuple(n * SLOTS * BLOCK + 16 for n in PARTS)
BASES = tuple(sum(SIZES[:i]) for i in range(len(PARTS)))
TOTAL = sum(SIZES)
HALO = 16 + LAYERS * BLOCK
HALO_ENDS = tuple(16 + (f + n) * BLOCK for f, n in zip(FIRST, PARTS))
HALO_BASES = (0,) + HALO_ENDS[:-1]

BASE = 2
EXTRA = 8
MESSAGES = ((0, 2, 0), (2, 8, 0), (10, 4, EXTRA), (14, 2, 0))
LENGTHS = tuple((n * BASE + e) * BLOCK + 16 for _, n, e in MESSAGES)
PAIRS = LAYERS // 2
EARLY = 5
EDGE = BLOCK + LAYERS * BLOCK
HALO_STARTS = (0, 3 * BLOCK, (1 + 2 * EARLY) * BLOCK, EDGE)


def full_exchange(
    blocks_at, held, offsets, weights, out, scales,
    raw, edge, rot, lanes, tails, turned, rest, hsend, hrecv, send, recv, patch,
    raw_sem, edge_sem, hs_sem, hr_sem, s_sem, r_sem,
):
    t = lax.axis_index("train")
    me = lax.axis_index("serve")
    mx, my, mc = me // 8, lax.rem(me // 2, 4), lax.rem(me, 2)
    right, left = lax.rem(t + 1, TRAIN_N), lax.rem(t + TRAIN_N - 1, TRAIN_N)

    def peer(v):
        return (
            lax.rem(mx + v // 8, 2) * 8
            + lax.rem(my + lax.rem(v // 2, 4), 4) * 2
            + lax.rem(mc + lax.rem(v, 2), 2)
        )

    barrier = pltpu.get_barrier_semaphore()
    for v in range(1, SERVE_N):
        pl.semaphore_signal(barrier, inc=1, device_id={"serve": peer(v)}, device_id_type=MESH)
    for other in (left, right):
        pl.semaphore_signal(barrier, inc=1, device_id={"train": other}, device_id_type=MESH)

    edges = [
        pltpu.make_async_copy(weights.at[:, b], edge.at[side], edge_sem.at[side])
        for side, b in enumerate((BLOCKS_DEV + 1, 0))
    ]
    loads = [
        pltpu.make_async_copy(weights.at[pl.ds(f, n)], raw.at[pl.ds(f, n)], raw_sem.at[i])
        for i, (f, n) in enumerate(zip(FIRST, PARTS))
    ]
    for copy in edges + loads:
        copy.start()

    row = lax.broadcasted_iota(jnp.int32, (COLS, 256), 0)
    col = lax.broadcasted_iota(jnp.int32, (COLS, 256), 1)
    turn = (row < 128) & (col < 128) & (col == ((row + 4 * me) & 127))
    spread = (row >= 128) & (col >= 128) & ((col & 3) == row - 128)
    rot[...] = jnp.where(turn | spread, 1.0, 0.0).astype(BF)
    lane16 = lax.broadcasted_iota(jnp.int32, (16, 128), 1)
    for m in range(32):
        lanes[m] = jnp.where((lane16 >> 2) == m, 1.0, 0.0).astype(BF)
    rrow = lax.broadcasted_iota(jnp.int32, (128, 128), 0)
    rcol = lax.broadcasted_iota(jnp.int32, (128, 128), 1)
    patch[...] = jnp.where((rrow & 3) == (rcol & 3), 1.0, 0.0).astype(BF)

    for copy in edges:
        copy.wait()
    for side in range(2):
        def edge_step(i, total, side=side):
            x = edge[side, pl.ds(i * 4, 4)].reshape(4 * BLOCK, COLS)
            y = jnp.dot(x, rot[...], preferred_element_type=F32).astype(BF)
            hsend[side, pl.ds(pl.multiple_of(16 + i * 128, 16), 128)] = y[:, :128]
            for q in range(8):
                total = total + y[q * 16 : q * 16 + 16, 128:] * lanes[lax.rem(i * 8 + q + me, 32)]
            return total

        hsend[side, 0:16] = lax.fori_loop(0, LAYERS // 4, edge_step, jnp.zeros((16, 128), BF))

    pl.semaphore_wait(barrier, SERVE_N + 1)

    halos = []
    for i in range(len(PARTS)):
        window = pl.ds(HALO_BASES[i], HALO_ENDS[i] - HALO_BASES[i])
        for side, target in enumerate((right, left)):
            copy = pltpu.make_async_remote_copy(
                src_ref=hsend.at[side, window],
                dst_ref=hrecv.at[side, window],
                send_sem=hs_sem.at[side, i],
                recv_sem=hr_sem.at[side, i],
                device_id={"train": target},
                device_id_type=MESH,
            )
            copy.start()
            halos.append(copy)

    def block_copy(i, v):
        window = pl.ds(BASES[i], SIZES[i])
        return pltpu.make_async_remote_copy(
            src_ref=send.at[v, window],
            dst_ref=recv.at[me, window],
            send_sem=s_sem.at[i, v],
            recv_sem=r_sem.at[i, v],
            device_id={"serve": peer(v)},
            device_id_type=MESH,
        )

    block_row = lax.broadcasted_iota(jnp.int32, (BLOCK, 128), 0)

    for i, (f, n) in enumerate(zip(FIRST, PARTS)):
        loads[i].wait()

        def turn_step(j, carry, f=f):
            l, b = j // 7, lax.rem(j, 7) * 4
            x = raw[f + l, pl.ds(b + 1, 4)].reshape(4 * BLOCK, COLS)
            y = jnp.dot(x, rot[...], preferred_element_type=F32).astype(BF)
            turned[l, pl.ds(b, 4)] = y[:, :128].reshape(4, BLOCK, 128)
            rest[l, pl.ds(b, 4)] = y[:, 128:].reshape(4, BLOCK, 128)
            return carry

        lax.fori_loop(0, n * 7, turn_step, 0)
        halos[2 * i].wait_recv()
        halos[2 * i + 1].wait_recv()

        def patch_step(l, carry, f=f):
            layer = f + l
            first = offsets[layer, t] - t * ROWS_DEV
            last = offsets[layer, t + 1] - t * ROWS_DEV - (ROWS_DEV - BLOCK)
            for side, (b, take) in enumerate(
                ((0, block_row < first), (BLOCKS_DEV - 1, block_row >= last))
            ):
                main = hrecv[side, pl.ds(pl.multiple_of(16 + layer * BLOCK, 16), BLOCK)]
                packed = hrecv[side, 0:16]
                both = jnp.concatenate(
                    [packed * lanes[lax.rem(2 * layer + h + me, 32)] for h in range(2)], axis=0
                )
                tail = jnp.dot(both, patch[...], preferred_element_type=F32)
                turned[l, b] = jnp.where(take, main.astype(F32), turned[l, b].astype(F32)).astype(BF)
                rest[l, b] = jnp.where(take, tail, rest[l, b].astype(F32)).astype(BF)
            return carry

        lax.fori_loop(0, n, patch_step, 0)

        def fill(dest, index, group, i=i, f=f, n=n):
            total = jnp.zeros((16, 128), BF)
            for l in range(n):
                for k in range(SLOTS):
                    slot = l * SLOTS + k
                    b = blocks_at[f + l, group * SLOTS + k]
                    dest[index, pl.ds(BASES[i] + slot * BLOCK, BLOCK)] = turned[l, b]
                    pair = rest[l, b]
                    for h in range(2):
                        total = total + pair[h * 16 : h * 16 + 16] * lanes[
                            lax.rem(2 * slot + h + me, 32)
                        ]
            dest[index, pl.ds(BASES[i] + n * SLOTS * BLOCK, 16)] = total

        def send_step(j, carry, i=i, fill=fill):
            v = SERVE_N - 1 - j
            fill(send, v, peer(v))
            block_copy(i, v).start()
            return carry

        lax.fori_loop(0, SERVE_N - 1, send_step, 0)
        fill(recv, me, me)

    lane = lax.broadcasted_iota(jnp.int32, (BLOCK, 128), 1)
    for i, (f, n) in enumerate(zip(FIRST, PARTS)):
        def arrive(j, carry, i=i):
            block_copy(i, j + 1).wait_recv()
            return carry

        lax.fori_loop(0, SERVE_N - 1, arrive, 0)

        def tail_step(q, carry, i=i, n=n):
            total = jnp.zeros((16, 128), BF)
            for s in range(SERVE_N):
                total = total + recv[s, pl.ds(BASES[i] + n * SLOTS * BLOCK, 16)] * lanes[
                    lax.rem(q + s, 32)
                ]
            tails[q // 2, pl.ds(pl.multiple_of(lax.rem(q, 2) * 16, 16), 16)] = pltpu.roll(
                total.astype(F32), 128 - 4 * q, axis=1
            )
            return carry

        lax.fori_loop(0, 2 * n * SLOTS, tail_step, 0)

        def block_step(slot, carry, i=i, f=f):
            layer, k = f + slot // SLOTS, lax.rem(slot, SLOTS)
            there = held[layer, me * SLOTS + k].astype(F32)
            at = f * SLOTS + slot
            tail = tails[slot]
            before = None
            for j in range(TILES):
                if j < SERVE_N:
                    now = recv[j, pl.ds(pl.multiple_of(BASES[i] + slot * BLOCK, 16), BLOCK)].astype(F32)
                else:
                    now = tail
                if j == 0:
                    value = now
                else:
                    value = jnp.where(
                        lane < 4 * j - 4, before, jnp.where(lane < 4 * j, tail, now)
                    )
                before = now
                top = jnp.maximum(jnp.max(jnp.abs(value), axis=0, keepdims=True), 0.25)
                codes = (value * (there / top)).astype(BF)
                width = min(128, FEAT - j * 128)
                out[at, :, j * 128 : j * 128 + width] = codes[:, :width]
                scales[at, :, j * 128 : j * 128 + width] = (top * there)[:, :width]
            return carry

        lax.fori_loop(0, n * SLOTS, block_step, 0)

    for copy in halos:
        copy.wait_send()
    for i in range(len(PARTS)):
        def leave(j, carry, i=i):
            block_copy(i, j + 1).wait_send()
            return carry

        lax.fori_loop(0, SERVE_N - 1, leave, 0)


def route(
    groups, offsets, weights, out, scales, flag,
    named, found, table, raw, eye, spread, turning, mixed_tail, lanes, turned, rest,
    hsend, hrecv, tails, extra_codes, extra_scales, fsend, frecv,
    send0, send1, send2, send3, recv0, recv1, recv2, recv3,
    table_sem, raw_sem, hs_sem, hr_sem, s_sem, r_sem, fs_sem, fr_sem,
):
    sends, recvs = (send0, send1, send2, send3), (recv0, recv1, recv2, recv3)
    t = lax.axis_index("train")
    me = lax.axis_index("serve")
    mx, my, mc = me // 8, lax.rem(me // 2, 4), lax.rem(me, 2)
    right, left = lax.rem(t + 1, TRAIN_N), lax.rem(t + TRAIN_N - 1, TRAIN_N)

    def peer(v):
        return (
            lax.rem(mx + v // 8, 2) * 8
            + lax.rem(my + lax.rem(v // 2, 4), 4) * 2
            + lax.rem(mc + lax.rem(v, 2), 2)
        )

    barrier = pltpu.get_barrier_semaphore()
    for v in range(1, SERVE_N):
        pl.semaphore_signal(barrier, inc=1, device_id={"serve": peer(v)}, device_id_type=MESH)
    for step in range(1, TRAIN_N):
        pl.semaphore_signal(
            barrier, inc=1, device_id={"train": lax.rem(t + step, TRAIN_N)}, device_id_type=MESH
        )

    def load(m, rows=16):
        return pltpu.make_async_copy(
            weights.at[pl.ds(16 * m, rows)], raw.at[pl.ds(16 + 16 * m, rows)], raw_sem.at[m]
        )

    wrapped = pltpu.make_async_copy(weights.at[112:128], raw.at[0:16], raw_sem.at[9])
    wrapped.start()
    for m in range(8):
        load(m).start()
    load(8, 4).start()

    def index(shape, dim):
        return lax.broadcasted_iota(I32, shape, dim)

    def ones(cond):
        return jnp.where(cond, 1.0, 0.0).astype(BF)

    lane16, row16 = index((16, 128), 1), index((16, 128), 0)
    named[...] = jnp.full((16, 128), -1, I32)
    named[:, 0:BLOCKS_DEV] = groups[...]
    group = named[...]
    order = jnp.zeros((16, 128), I32)
    for d in range(1, BLOCKS_DEV):
        same = (pltpu.roll(group, d, axis=1) == group) & (lane16 >= d)
        order = order + jnp.where(same, 1, 0)
    slot_of = group * SLOTS + order
    blocks_at = jnp.zeros((16, 128), I32)
    third_at = jnp.zeros((16, 128), I32)
    counted = jnp.zeros((16, 128), I32)
    for b in range(BLOCKS_DEV):
        slot_b = slot_of[:, b : b + 1]
        blocks_at = jnp.where(slot_b == lane16, b, blocks_at)
        third_at = jnp.where(slot_b == lane16 * SLOTS + BASE, b, third_at)
        counted = counted + jnp.where(group[:, b : b + 1] == lane16, 1, 0)
    third = jnp.where(counted > BASE, 1, 0)
    before = jnp.zeros((16, 128), I32)
    for d in range(1, LAYERS):
        before = before + jnp.where(row16 >= d, pltpu.roll(third, d, axis=0), 0)
    found[0:16] = blocks_at
    found[16:32] = counted
    found[32:48] = jnp.minimum(before, EXTRA - 1)
    where_third = row16 * HELD + 1 + third_at
    for e in range(EXTRA):
        mine = (third > 0) & (before == e)
        found[48 + e : 49 + e] = jnp.sum(jnp.where(mine, where_third, 0), axis=0, keepdims=True)
    known = pltpu.make_async_copy(found, table, table_sem)
    known.start()
    long = jnp.where(jnp.sum(third, axis=0, keepdims=True) > EXTRA, 1.0, 0.0)
    fsend[...] = jnp.broadcast_to(long, (8, 128))
    frecv[t] = fsend[...]

    eye[...] = ones(index((256, 256), 0) == index((256, 256), 1))
    a, b = index((256, 256), 0), index((256, 256), 1)
    spread[...] = ones(((b >> 4) == (a & 15)) & ((b & 15) == (a >> 4)))
    for m in range(32):
        lanes[m] = ones((lane16 >> 2) == m)

    NT = (((1,), (1,)), ((), ()))

    def gather_columns(m, tiles):
        start = 16 * (m + 1) - 4 * lax.rem(me, 4)
        place = 16 * lax.rem(m + me // 4, 8)
        for r, w in tiles:
            x = raw[pl.ds(start, 16), :, r : r + w].reshape(256, w)
            y = jnp.dot(spread[...], x, preferred_element_type=F32).astype(BF)
            for layer in range(LAYERS):
                window = pl.ds(pl.multiple_of(128 * layer + place, 16), 16)
                turning[window, r : r + w] = y[16 * layer : 16 * layer + 16]

    ends, middle = ((0, 128), (896, 64)), ((128, 256), (384, 256), (640, 256))
    wrapped.wait()

    def ends_step(m, carry):
        load(m).wait()
        gather_columns(m, ends)
        return carry

    lax.fori_loop(0, 8, ends_step, 0)
    load(8, 4).wait()

    def turn_tail(tiles):
        for r, w in tiles:
            x = raw[144:148, :, r : r + w].reshape(64, w)
            y = lax.dot_general(eye[:w, :w], x, NT, preferred_element_type=F32)
            mixed_tail[r : r + w] = y.astype(BF)

    turn_tail(ends)
    hsend[0, 0:BLOCK, 0:64] = mixed_tail[BUFFER - BLOCK : BUFFER]
    hsend[1, 0:BLOCK, 0:64] = mixed_tail[0:BLOCK]
    hsend[0, 0:BLOCK, 64:128] = jnp.zeros((BLOCK, 64), BF)
    hsend[1, 0:BLOCK, 64:128] = jnp.zeros((BLOCK, 64), BF)

    def edge_step(p, carry):
        rows = pl.ds(pl.multiple_of(256 * p, 256), 256)
        low = lax.dot_general(eye[0:32, 0:128], turning[rows, 0:128], NT, preferred_element_type=F32)
        high = lax.dot_general(
            eye[32:64, 0:64], turning[rows, 896:960], NT, preferred_element_type=F32
        )
        for h in range(2):
            window = pl.ds(pl.multiple_of(BLOCK + (2 * p + h) * BLOCK, BLOCK), BLOCK)
            hsend[0, window] = high[:, 128 * h : 128 * h + 128].astype(BF)
            hsend[1, window] = low[:, 128 * h : 128 * h + 128].astype(BF)
        return carry

    lax.fori_loop(0, PAIRS, edge_step, 0, unroll=2)

    def middle_step(m, carry):
        gather_columns(m, middle)
        return carry

    def tail_pick(p):
        k, q = index((64, 256), 0), index((64, 256), 1)
        return ones(((k & 15) == 2 * p + (q >> 7)) & ((k >> 4) == (q & 3)))

    def prepare_step(p, carry):
        rows = pl.ds(pl.multiple_of(256 * p, 256), 256)
        tail_of = tail_pick(p)
        for r, w in ((0, 128), (128, 256), (384, 256), (640, 256), (896, 64)):
            y = lax.dot_general(
                eye[:w, :w], turning[rows, r : r + w], NT, preferred_element_type=F32
            ).astype(BF)
            z = jnp.dot(mixed_tail[r : r + w], tail_of, preferred_element_type=F32).astype(BF)
            for h in range(2):
                at = pl.ds((2 * p + h) * HELD + r // BLOCK, w // BLOCK)
                turned[at] = y[:, 128 * h : 128 * h + 128].reshape(w // BLOCK, BLOCK, 128)
                rest[at] = z[:, 128 * h : 128 * h + 128].reshape(w // BLOCK, BLOCK, 128)
        return carry

    def halo(side, i):
        window = pl.ds(HALO_STARTS[i], HALO_STARTS[i + 1] - HALO_STARTS[i])
        return pltpu.make_async_remote_copy(
            src_ref=hsend.at[side, window],
            dst_ref=hrecv.at[side, window],
            send_sem=hs_sem.at[side, i],
            recv_sem=hr_sem.at[side, i],
            device_id={"train": (right, left)[side]},
            device_id_type=MESH,
        )

    block_row = index((BLOCK, 128), 0)

    def patch(p):
        tail_of = tail_pick(p)
        for side, (b, last) in enumerate(((1, False), (HELD - 2, True))):
            tail = jnp.dot(hrecv[side, 0:BLOCK, 0:64], tail_of, preferred_element_type=F32)
            for h in range(2):
                layer = 2 * p + h
                if last:
                    take = block_row >= offsets[layer, t + 1] - t * ROWS_DEV - (ROWS_DEV - BLOCK)
                else:
                    take = block_row < offsets[layer, t] - t * ROWS_DEV
                at = layer * HELD + b
                window = pl.ds(pl.multiple_of(BLOCK + layer * BLOCK, BLOCK), BLOCK)
                main = hrecv[side, window].astype(F32)
                turned[at] = jnp.where(take, main, turned[at].astype(F32)).astype(BF)
                rest[at] = jnp.where(
                    take, tail[:, 128 * h : 128 * h + 128], rest[at].astype(F32)
                ).astype(BF)

    def patch_step(p, carry):
        patch(p)
        return carry

    def message(i, v):
        return pltpu.make_async_remote_copy(
            src_ref=sends[i].at[v],
            dst_ref=recvs[i].at[me],
            send_sem=s_sem.at[i, v],
            recv_sem=r_sem.at[i, v],
            device_id={"serve": peer(v)},
            device_id_type=MESH,
        )

    def dispatch(i):
        f, n, e = MESSAGES[i]

        def fill(dest, place, group):
            total = jnp.zeros((16, 128), BF)
            for slot in range(n * BASE + e):
                if slot < n * BASE:
                    layer, k = f + slot // BASE, slot % BASE
                    at = layer * HELD + 1 + table[layer, group * SLOTS + k]
                else:
                    at = table[48 + slot - n * BASE, group]
                dest[place, slot * BLOCK : slot * BLOCK + BLOCK] = turned[at]
                pair = rest[at]
                for h in range(2):
                    mask = lanes[lax.rem(2 * slot + h + me, 32)]
                    total = total + pair[h * 16 : h * 16 + 16] * mask
            dest[place, LENGTHS[i] - 16 : LENGTHS[i]] = total

        def send_step(j, carry):
            v = SERVE_N - 1 - j
            fill(sends[i], v, peer(v))
            message(i, v).start()
            return carry

        lax.fori_loop(0, SERVE_N - 1, send_step, 0)
        fill(recvs[i], me, me)

    lane = index((BLOCK, 128), 1)

    def finish(i):
        f, n, e = MESSAGES[i]
        recv = recvs[i]

        def arrive(j, carry):
            message(i, j + 1).wait_recv()
            return carry

        lax.fori_loop(0, SERVE_N - 1, arrive, 0)

        def tail_step(q, carry):
            total = jnp.zeros((16, 128), BF)
            for s in range(SERVE_N):
                total = total + recv[s, LENGTHS[i] - 16 : LENGTHS[i]] * lanes[lax.rem(q + s, 32)]
            tails[q // 2, pl.ds(pl.multiple_of(lax.rem(q, 2) * 16, 16), 16)] = pltpu.roll(
                total.astype(F32), 128 - 4 * q, axis=1
            )
            return carry

        lax.fori_loop(0, 2 * (n * BASE + e), tail_step, 0)

        def scale_block(slot, at, there, codes_out, scales_out):
            tail = tails[slot]
            before = None
            for j in range(TILES):
                if j < SERVE_N:
                    now = recv[j, pl.ds(pl.multiple_of(slot * BLOCK, BLOCK), BLOCK)].astype(F32)
                else:
                    now = tail
                if j == 0:
                    value = now
                else:
                    value = jnp.where(
                        lane < 4 * j - 4, before, jnp.where(lane < 4 * j, tail, now)
                    )
                before = now
                top = jnp.maximum(jnp.max(jnp.abs(value), axis=0, keepdims=True), 0.25)
                codes = (value * (there / top)).astype(BF)
                width = min(128, FEAT - j * 128)
                codes_out[at, :, j * 128 : j * 128 + width] = codes[:, :width]
                scales_out[at, :, j * 128 : j * 128 + width] = (top * there)[:, :width]

        def present(layer, k):
            return jnp.minimum(jnp.maximum(table[16 + layer, me] - k, 0), 1).astype(F32)

        def base_step(slot, carry):
            layer, k = f + slot // BASE, lax.rem(slot, BASE)
            scale_block(slot, layer * SLOTS + k, present(layer, k), out, scales)
            return carry

        lax.fori_loop(0, n * BASE, base_step, 0)
        if e:
            def extra_step(entry, carry):
                scale_block(n * BASE + entry, entry, 1.0, extra_codes, extra_scales)
                return carry

            lax.fori_loop(0, e, extra_step, 0)

            def place_step(layer, carry):
                entry, there = table[32 + layer, me], present(layer, BASE)
                at = layer * SLOTS + BASE
                out[at] = (extra_codes[entry].astype(F32) * there).astype(BF)
                scales[at] = extra_scales[entry] * there
                return carry

            lax.fori_loop(0, LAYERS, place_step, 0)

    def tell(step):
        return pltpu.make_async_remote_copy(
            src_ref=fsend,
            dst_ref=frecv.at[t],
            send_sem=fs_sem.at[step],
            recv_sem=fr_sem.at[step],
            device_id={"train": lax.rem(t + step, TRAIN_N)},
            device_id_type=MESH,
        )

    pl.semaphore_wait(barrier, SERVE_N + TRAIN_N - 2)
    for i in range(3):
        for side in range(2):
            halo(side, i).start()
    for step in range(1, TRAIN_N):
        tell(step).start()
    lax.fori_loop(0, 8, middle_step, 0)
    turn_tail(middle)
    lax.fori_loop(0, 1, prepare_step, 0)
    known.wait()
    for side in range(2):
        halo(side, 0).wait_recv()
    patch(0)
    dispatch(0)
    lax.fori_loop(1, EARLY, prepare_step, 0)
    for side in range(2):
        halo(side, 1).wait_recv()
    lax.fori_loop(1, EARLY, patch_step, 0)
    dispatch(1)
    lax.fori_loop(EARLY, PAIRS, prepare_step, 0)
    for side in range(2):
        halo(side, 2).wait_recv()
    lax.fori_loop(EARLY, PAIRS, patch_step, 0)
    dispatch(2)
    dispatch(3)
    finish(0)
    finish(1)
    finish(2)
    finish(3)
    for step in range(1, TRAIN_N):
        tell(step).wait()
    flag[...] = jnp.broadcast_to(jnp.max(frecv[...]).reshape(1, 1), (8, 128))

    for side in range(2):
        halo(side, 0).wait_send()
        halo(side, 1).wait_send()
        halo(side, 2).wait_send()
    for i in range(len(MESSAGES)):
        def leave(j, carry, i=i):
            message(i, j + 1).wait_send()
            return carry

        lax.fori_loop(0, SERVE_N - 1, leave, 0)


def everything(train_weights, row_offset, groups):
    position = jnp.arange(BLOCKS_DEV, dtype=I32)
    earlier = position[None, :] < position[:, None]
    same = groups[:, :, None] == groups[:, None, :]
    order = jnp.sum((same & earlier[None]).astype(I32), axis=2)
    slot_id = groups * SLOTS + order
    onehot = slot_id[:, None, :] == jnp.arange(SERVE_N * SLOTS, dtype=I32)[None, :, None]
    blocks_at = jnp.sum(jnp.where(onehot, position[None, None, :], 0), axis=2)
    group_ids = jnp.arange(SERVE_N, dtype=I32)
    counts = jnp.sum((groups[:, None, :] == group_ids[None, :, None]).astype(I32), axis=2)
    held = (counts[:, :, None] > jnp.arange(SLOTS, dtype=I32)).astype(I32)
    held = held.reshape(LAYERS, SERVE_N * SLOTS)
    weights = train_weights.reshape(LAYERS, HELD, BLOCK, COLS)
    parts = len(PARTS)
    smem = pl.BlockSpec(memory_space=pltpu.SMEM)
    vmem = pl.BlockSpec(memory_space=pltpu.VMEM)
    return pl.pallas_call(
        full_exchange,
        out_shape=(
            pltpu.VMEM((LAYERS * SLOTS, BLOCK, FEAT), BF),
            pltpu.VMEM((LAYERS * SLOTS, 1, FEAT), F32),
        ),
        in_specs=[smem, smem, smem, pl.BlockSpec(memory_space=pl.ANY)],
        out_specs=(vmem, vmem),
        scratch_shapes=[
            pltpu.VMEM((LAYERS, HELD, BLOCK, COLS), BF),
            pltpu.VMEM((2, LAYERS, BLOCK, COLS), BF),
            pltpu.VMEM((COLS, 256), BF),
            pltpu.VMEM((32, 16, 128), BF),
            pltpu.VMEM((max(PARTS) * SLOTS, BLOCK, 128), F32),
            pltpu.VMEM((max(PARTS), BLOCKS_DEV, BLOCK, 128), BF),
            pltpu.VMEM((max(PARTS), BLOCKS_DEV, BLOCK, 128), BF),
            pltpu.VMEM((2, HALO, 128), BF),
            pltpu.VMEM((2, HALO, 128), BF),
            pltpu.VMEM((SERVE_N, TOTAL, 128), BF),
            pltpu.VMEM((SERVE_N, TOTAL, 128), BF),
            pltpu.VMEM((128, 128), BF),
            pltpu.SemaphoreType.DMA((parts,)),
            pltpu.SemaphoreType.DMA((2,)),
            pltpu.SemaphoreType.DMA((2, parts)),
            pltpu.SemaphoreType.DMA((2, parts)),
            pltpu.SemaphoreType.DMA((parts, SERVE_N)),
            pltpu.SemaphoreType.DMA((parts, SERVE_N)),
        ],
        compiler_params=pltpu.CompilerParams(
            collective_id=1, has_side_effects=True, vmem_limit_bytes=44 * 2**20
        ),
    )(blocks_at, held, row_offset, weights)


def shards(train_weights, row_offset, block_group):
    groups = block_group[:, :, 0]
    smem = pl.BlockSpec(memory_space=pltpu.SMEM)
    vmem = pl.BlockSpec(memory_space=pltpu.VMEM)
    parts = len(MESSAGES)
    codes, scales, flag = pl.pallas_call(
        route,
        out_shape=(
            pltpu.VMEM((LAYERS * SLOTS, BLOCK, FEAT), BF),
            pltpu.VMEM((LAYERS * SLOTS, 1, FEAT), F32),
            jax.ShapeDtypeStruct((8, 128), F32),
        ),
        in_specs=[vmem, smem, pl.BlockSpec(memory_space=pl.ANY)],
        out_specs=(vmem, vmem, vmem),
        scratch_shapes=[
            pltpu.VMEM((LAYERS, 128), I32),
            pltpu.VMEM((56, 128), I32),
            pltpu.SMEM((56, 128), I32),
            pltpu.VMEM((COLS + 16, LAYERS, BUFFER), BF),
            pltpu.VMEM((256, 256), BF),
            pltpu.VMEM((256, 256), BF),
            pltpu.VMEM((128 * LAYERS, BUFFER), BF),
            pltpu.VMEM((BUFFER, 64), BF),
            pltpu.VMEM((32, 16, 128), BF),
            pltpu.VMEM((LAYERS * HELD, BLOCK, 128), BF),
            pltpu.VMEM((LAYERS * HELD, BLOCK, 128), BF),
            pltpu.VMEM((2, EDGE, 128), BF),
            pltpu.VMEM((2, EDGE, 128), BF),
            pltpu.VMEM((16, BLOCK, 128), F32),
            pltpu.VMEM((EXTRA, BLOCK, FEAT), BF),
            pltpu.VMEM((EXTRA, 1, FEAT), F32),
            pltpu.VMEM((8, 128), F32),
            pltpu.VMEM((TRAIN_N, 8, 128), F32),
            *[pltpu.VMEM((SERVE_N, length, 128), BF) for length in LENGTHS * 2],
            pltpu.SemaphoreType.DMA,
            pltpu.SemaphoreType.DMA((10,)),
            pltpu.SemaphoreType.DMA((2, 3)),
            pltpu.SemaphoreType.DMA((2, 3)),
            pltpu.SemaphoreType.DMA((parts, SERVE_N)),
            pltpu.SemaphoreType.DMA((parts, SERVE_N)),
            pltpu.SemaphoreType.DMA((TRAIN_N,)),
            pltpu.SemaphoreType.DMA((TRAIN_N,)),
        ],
        compiler_params=pltpu.CompilerParams(
            collective_id=2, has_side_effects=True, vmem_limit_bytes=46 * 2**20
        ),
    )(
        groups, row_offset, jnp.transpose(train_weights, (2, 0, 1)),
    )
    codes, scales = lax.cond(
        flag[0, 0] > 0.0,
        lambda: tuple(everything(train_weights, row_offset, groups)),
        lambda: (codes, scales),
    )
    return (
        codes.reshape(LAYERS, 1, 1, SLOTS, BLOCK, FEAT),
        scales.reshape(LAYERS, 1, 1, SLOTS, FEAT),
    )


def solution(mesh):
    return jax.shard_map(
        shards,
        mesh=mesh,
        in_specs=(P(None, "train", "serve"), P(), P(None, "train", None)),
        out_specs=(P(None, "serve", "train", None, None, None), P(None, "serve", "train", None, None)),
        check_vma=False,
    )
```

```python
import functools

import jax
import jax.numpy as jnp
from jax import lax
from jax.experimental import pallas as pl
from jax.experimental.pallas import tpu as pltpu
from jax.sharding import PartitionSpec as P

MESH = pl.DeviceIdType.MESH
BF = jnp.bfloat16
F32 = jnp.float32
I32 = jnp.int32
LAYERS = 16
BLOCK = 32
BLOCKS_DEV = 28
HELD = BLOCKS_DEV + 2
ROWS_DEV = 896
BUFFER = HELD * BLOCK
COLS = 132
SERVE_N = 16
TRAIN_N = 8
SLOTS = 3
FEAT = SERVE_N * COLS
TILES = -(-FEAT // 128)

PARTS = (2, 4, 4, 4, 2)
FIRST = (0, 2, 6, 10, 14)
SIZES = tuple(n * SLOTS * BLOCK + 16 for n in PARTS)
BASES = tuple(sum(SIZES[:i]) for i in range(len(PARTS)))
TOTAL = sum(SIZES)
HALO = 16 + LAYERS * BLOCK
HALO_ENDS = tuple(16 + (f + n) * BLOCK for f, n in zip(FIRST, PARTS))
HALO_BASES = (0,) + HALO_ENDS[:-1]

BASE = 2
EXTRA = 8
MESSAGES = ((0, 2, 2), (2, 8, 8), (10, 4, 6), (14, 2, 0))
LENGTHS = tuple(n * BASE * BLOCK + (16 if m else 0) for _, n, m in MESSAGES)
LIST = EXTRA * BLOCK + 16
PAIRS = LAYERS // 2
EARLY = 5
EDGE = BLOCK + LAYERS * BLOCK
HALO_STARTS = (0, 3 * BLOCK, (1 + 2 * EARLY) * BLOCK, EDGE)


def full_exchange(
    blocks_at, held, offsets, weights, out, scales,
    raw, edge, rot, lanes, tails, turned, rest, hsend, hrecv, send, recv, patch,
    raw_sem, edge_sem, hs_sem, hr_sem, s_sem, r_sem,
):
    t = lax.axis_index("train")
    me = lax.axis_index("serve")
    mx, my, mc = me // 8, lax.rem(me // 2, 4), lax.rem(me, 2)
    right, left = lax.rem(t + 1, TRAIN_N), lax.rem(t + TRAIN_N - 1, TRAIN_N)

    def peer(v):
        return (
            lax.rem(mx + v // 8, 2) * 8
            + lax.rem(my + lax.rem(v // 2, 4), 4) * 2
            + lax.rem(mc + lax.rem(v, 2), 2)
        )

    barrier = pltpu.get_barrier_semaphore()
    for v in range(1, SERVE_N):
        pl.semaphore_signal(barrier, inc=1, device_id={"serve": peer(v)}, device_id_type=MESH)
    for other in (left, right):
        pl.semaphore_signal(barrier, inc=1, device_id={"train": other}, device_id_type=MESH)

    edges = [
        pltpu.make_async_copy(weights.at[:, b], edge.at[side], edge_sem.at[side])
        for side, b in enumerate((BLOCKS_DEV + 1, 0))
    ]
    loads = [
        pltpu.make_async_copy(weights.at[pl.ds(f, n)], raw.at[pl.ds(f, n)], raw_sem.at[i])
        for i, (f, n) in enumerate(zip(FIRST, PARTS))
    ]
    for copy in edges + loads:
        copy.start()

    row = lax.broadcasted_iota(jnp.int32, (COLS, 256), 0)
    col = lax.broadcasted_iota(jnp.int32, (COLS, 256), 1)
    turn = (row < 128) & (col < 128) & (col == ((row + 4 * me) & 127))
    spread = (row >= 128) & (col >= 128) & ((col & 3) == row - 128)
    rot[...] = jnp.where(turn | spread, 1.0, 0.0).astype(BF)
    lane16 = lax.broadcasted_iota(jnp.int32, (16, 128), 1)
    for m in range(32):
        lanes[m] = jnp.where((lane16 >> 2) == m, 1.0, 0.0).astype(BF)
    rrow = lax.broadcasted_iota(jnp.int32, (128, 128), 0)
    rcol = lax.broadcasted_iota(jnp.int32, (128, 128), 1)
    patch[...] = jnp.where((rrow & 3) == (rcol & 3), 1.0, 0.0).astype(BF)

    for copy in edges:
        copy.wait()
    for side in range(2):
        def edge_step(i, total, side=side):
            x = edge[side, pl.ds(i * 4, 4)].reshape(4 * BLOCK, COLS)
            y = jnp.dot(x, rot[...], preferred_element_type=F32).astype(BF)
            hsend[side, pl.ds(pl.multiple_of(16 + i * 128, 16), 128)] = y[:, :128]
            for q in range(8):
                total = total + y[q * 16 : q * 16 + 16, 128:] * lanes[lax.rem(i * 8 + q + me, 32)]
            return total

        hsend[side, 0:16] = lax.fori_loop(0, LAYERS // 4, edge_step, jnp.zeros((16, 128), BF))

    pl.semaphore_wait(barrier, SERVE_N + 1)

    halos = []
    for i in range(len(PARTS)):
        window = pl.ds(HALO_BASES[i], HALO_ENDS[i] - HALO_BASES[i])
        for side, target in enumerate((right, left)):
            copy = pltpu.make_async_remote_copy(
                src_ref=hsend.at[side, window],
                dst_ref=hrecv.at[side, window],
                send_sem=hs_sem.at[side, i],
                recv_sem=hr_sem.at[side, i],
                device_id={"train": target},
                device_id_type=MESH,
            )
            copy.start()
            halos.append(copy)

    def block_copy(i, v):
        window = pl.ds(BASES[i], SIZES[i])
        return pltpu.make_async_remote_copy(
            src_ref=send.at[v, window],
            dst_ref=recv.at[me, window],
            send_sem=s_sem.at[i, v],
            recv_sem=r_sem.at[i, v],
            device_id={"serve": peer(v)},
            device_id_type=MESH,
        )

    block_row = lax.broadcasted_iota(jnp.int32, (BLOCK, 128), 0)

    for i, (f, n) in enumerate(zip(FIRST, PARTS)):
        loads[i].wait()

        def turn_step(j, carry, f=f):
            l, b = j // 7, lax.rem(j, 7) * 4
            x = raw[f + l, pl.ds(b + 1, 4)].reshape(4 * BLOCK, COLS)
            y = jnp.dot(x, rot[...], preferred_element_type=F32).astype(BF)
            turned[l, pl.ds(b, 4)] = y[:, :128].reshape(4, BLOCK, 128)
            rest[l, pl.ds(b, 4)] = y[:, 128:].reshape(4, BLOCK, 128)
            return carry

        lax.fori_loop(0, n * 7, turn_step, 0)
        halos[2 * i].wait_recv()
        halos[2 * i + 1].wait_recv()

        def patch_step(l, carry, f=f):
            layer = f + l
            first = offsets[layer, t] - t * ROWS_DEV
            last = offsets[layer, t + 1] - t * ROWS_DEV - (ROWS_DEV - BLOCK)
            for side, (b, take) in enumerate(
                ((0, block_row < first), (BLOCKS_DEV - 1, block_row >= last))
            ):
                main = hrecv[side, pl.ds(pl.multiple_of(16 + layer * BLOCK, 16), BLOCK)]
                packed = hrecv[side, 0:16]
                both = jnp.concatenate(
                    [packed * lanes[lax.rem(2 * layer + h + me, 32)] for h in range(2)], axis=0
                )
                tail = jnp.dot(both, patch[...], preferred_element_type=F32)
                turned[l, b] = jnp.where(take, main.astype(F32), turned[l, b].astype(F32)).astype(BF)
                rest[l, b] = jnp.where(take, tail, rest[l, b].astype(F32)).astype(BF)
            return carry

        lax.fori_loop(0, n, patch_step, 0)

        def fill(dest, index, group, i=i, f=f, n=n):
            total = jnp.zeros((16, 128), BF)
            for l in range(n):
                for k in range(SLOTS):
                    slot = l * SLOTS + k
                    b = blocks_at[f + l, group * SLOTS + k]
                    dest[index, pl.ds(BASES[i] + slot * BLOCK, BLOCK)] = turned[l, b]
                    pair = rest[l, b]
                    for h in range(2):
                        total = total + pair[h * 16 : h * 16 + 16] * lanes[
                            lax.rem(2 * slot + h + me, 32)
                        ]
            dest[index, pl.ds(BASES[i] + n * SLOTS * BLOCK, 16)] = total

        def send_step(j, carry, i=i, fill=fill):
            v = SERVE_N - 1 - j
            fill(send, v, peer(v))
            block_copy(i, v).start()
            return carry

        lax.fori_loop(0, SERVE_N - 1, send_step, 0)
        fill(recv, me, me)

    lane = lax.broadcasted_iota(jnp.int32, (BLOCK, 128), 1)
    for i, (f, n) in enumerate(zip(FIRST, PARTS)):
        def arrive(j, carry, i=i):
            block_copy(i, j + 1).wait_recv()
            return carry

        lax.fori_loop(0, SERVE_N - 1, arrive, 0)

        def tail_step(q, carry, i=i, n=n):
            total = jnp.zeros((16, 128), BF)
            for s in range(SERVE_N):
                total = total + recv[s, pl.ds(BASES[i] + n * SLOTS * BLOCK, 16)] * lanes[
                    lax.rem(q + s, 32)
                ]
            tails[q // 2, pl.ds(pl.multiple_of(lax.rem(q, 2) * 16, 16), 16)] = pltpu.roll(
                total.astype(F32), 128 - 4 * q, axis=1
            )
            return carry

        lax.fori_loop(0, 2 * n * SLOTS, tail_step, 0)

        def block_step(slot, carry, i=i, f=f):
            layer, k = f + slot // SLOTS, lax.rem(slot, SLOTS)
            there = held[layer, me * SLOTS + k].astype(F32)
            at = f * SLOTS + slot
            tail = tails[slot]
            before = None
            for j in range(TILES):
                if j < SERVE_N:
                    now = recv[j, pl.ds(pl.multiple_of(BASES[i] + slot * BLOCK, 16), BLOCK)].astype(F32)
                else:
                    now = tail
                if j == 0:
                    value = now
                else:
                    value = jnp.where(
                        lane < 4 * j - 4, before, jnp.where(lane < 4 * j, tail, now)
                    )
                before = now
                top = jnp.maximum(jnp.max(jnp.abs(value), axis=0, keepdims=True), 0.25)
                codes = (value * (there / top)).astype(BF)
                width = min(128, FEAT - j * 128)
                out[at, :, j * 128 : j * 128 + width] = codes[:, :width]
                scales[at, :, j * 128 : j * 128 + width] = (top * there)[:, :width]
            return carry

        lax.fori_loop(0, n * SLOTS, block_step, 0)

    for copy in halos:
        copy.wait_send()
    for i in range(len(PARTS)):
        def leave(j, carry, i=i):
            block_copy(i, j + 1).wait_send()
            return carry

        lax.fori_loop(0, SERVE_N - 1, leave, 0)


def route(
    groups_in, offsets_in, weights, out, scales, flag,
    groups, offsets, named, found, table, raw, eye, spread, turning, mixed_tail, lanes, turned, rest,
    hsend, hrecv, tails, extra_codes, extra_scales, fsend, frecv,
    send0, send1, send2, send3, recv0, recv1, recv2, recv3, lists,
    small_sem, table_sem, raw_sem, hs_sem, hr_sem, s_sem, r_sem, ls_sem, lr_sem, fs_sem, fr_sem,
):
    sends, recvs = (send0, send1, send2, send3), (recv0, recv1, recv2, recv3)
    t = lax.axis_index("train")
    me = lax.axis_index("serve")
    mx, my, mc = me // 8, lax.rem(me // 2, 4), lax.rem(me, 2)
    right, left = lax.rem(t + 1, TRAIN_N), lax.rem(t + TRAIN_N - 1, TRAIN_N)

    def peer(v):
        return (
            lax.rem(mx + v // 8, 2) * 8
            + lax.rem(my + lax.rem(v // 2, 4), 4) * 2
            + lax.rem(mc + lax.rem(v, 2), 2)
        )

    small = [
        pltpu.make_async_copy(groups_in, groups, small_sem.at[0]),
        pltpu.make_async_copy(offsets_in, offsets, small_sem.at[1]),
    ]
    loads = [
        [
            pltpu.make_async_copy(
                weights.at[a : a + n, :, r : r + w], raw.at[b : b + n, :, r : r + w], raw_sem.at[i, j]
            )
            for j, (a, b, n) in enumerate(((0, 16, COLS), (112, 0, 16)))
        ]
        for i, (r, w) in enumerate(((0, 128), (896, 64), (128, 768)))
    ]
    for copy in loads[0] + loads[1] + small + loads[2]:
        copy.start()

    barrier = pltpu.get_barrier_semaphore()
    for v in range(1, SERVE_N):
        pl.semaphore_signal(barrier, inc=1, device_id={"serve": peer(v)}, device_id_type=MESH)
    for step in range(1, TRAIN_N):
        pl.semaphore_signal(
            barrier, inc=1, device_id={"train": lax.rem(t + step, TRAIN_N)}, device_id_type=MESH
        )

    def index(shape, dim):
        return lax.broadcasted_iota(I32, shape, dim)

    def ones(cond):
        return jnp.where(cond, 1.0, 0.0).astype(BF)

    lane16, row16 = index((16, 128), 1), index((16, 128), 0)
    eye[...] = ones(index((256, 256), 0) == index((256, 256), 1))
    a, b = index((256, 256), 0), index((256, 256), 1)
    spread[...] = ones(((b >> 4) == (a & 15)) & ((b & 15) == (a >> 4)))
    for m in range(32):
        lanes[m] = ones((lane16 >> 2) == m)

    NT = (((1,), (1,)), ((), ()))

    def gather_columns(m, tiles):
        start = 16 * (m + 1) - 4 * lax.rem(me, 4)
        place = 16 * lax.rem(m + me // 4, 8)
        for r, w in tiles:
            x = raw[pl.ds(start, 16), :, r : r + w].reshape(256, w)
            y = jnp.dot(spread[...], x, preferred_element_type=F32).astype(BF)
            for layer in range(LAYERS):
                window = pl.ds(pl.multiple_of(128 * layer + place, 16), 16)
                turning[window, r : r + w] = y[16 * layer : 16 * layer + 16]

    ends, middle = ((0, 128), (896, 64)), ((128, 256), (384, 256), (640, 256))
    for copy in loads[0] + loads[1]:
        copy.wait()
    for m in range(8):
        gather_columns(m, ends)

    def turn_tail(tiles):
        for r, w in tiles:
            x = raw[144:148, :, r : r + w].reshape(64, w)
            y = lax.dot_general(eye[:w, :w], x, NT, preferred_element_type=F32)
            mixed_tail[r : r + w] = y.astype(BF)

    turn_tail(ends)
    hsend[0, 0:BLOCK, 0:64] = mixed_tail[BUFFER - BLOCK : BUFFER]
    hsend[1, 0:BLOCK, 0:64] = mixed_tail[0:BLOCK]
    hsend[0, 0:BLOCK, 64:128] = jnp.zeros((BLOCK, 64), BF)
    hsend[1, 0:BLOCK, 64:128] = jnp.zeros((BLOCK, 64), BF)

    def edge_step(p, carry):
        rows = pl.ds(pl.multiple_of(256 * p, 256), 256)
        low = lax.dot_general(eye[0:32, 0:128], turning[rows, 0:128], NT, preferred_element_type=F32)
        high = lax.dot_general(
            eye[32:64, 0:64], turning[rows, 896:960], NT, preferred_element_type=F32
        )
        for h in range(2):
            window = pl.ds(pl.multiple_of(BLOCK + (2 * p + h) * BLOCK, BLOCK), BLOCK)
            hsend[0, window] = high[:, 128 * h : 128 * h + 128].astype(BF)
            hsend[1, window] = low[:, 128 * h : 128 * h + 128].astype(BF)
        return carry

    lax.fori_loop(0, PAIRS, edge_step, 0, unroll=8)

    def tail_pick(p):
        k, q = index((64, 256), 0), index((64, 256), 1)
        return ones(((k & 15) == 2 * p + (q >> 7)) & ((k >> 4) == (q & 3)))

    def prepare_step(p, carry):
        rows = pl.ds(pl.multiple_of(256 * p, 256), 256)
        tail_of = tail_pick(p)
        for r, w in ((0, 128), (128, 256), (384, 256), (640, 256), (896, 64)):
            y = lax.dot_general(
                eye[:w, :w], turning[rows, r : r + w], NT, preferred_element_type=F32
            ).astype(BF)
            z = jnp.dot(mixed_tail[r : r + w], tail_of, preferred_element_type=F32).astype(BF)
            for h in range(2):
                at = pl.ds((2 * p + h) * HELD + r // BLOCK, w // BLOCK)
                turned[at] = y[:, 128 * h : 128 * h + 128].reshape(w // BLOCK, BLOCK, 128)
                rest[at] = z[:, 128 * h : 128 * h + 128].reshape(w // BLOCK, BLOCK, 128)
        return carry

    def halo(side, i):
        window = pl.ds(HALO_STARTS[i], HALO_STARTS[i + 1] - HALO_STARTS[i])
        return pltpu.make_async_remote_copy(
            src_ref=hsend.at[side, window],
            dst_ref=hrecv.at[side, window],
            send_sem=hs_sem.at[side, i],
            recv_sem=hr_sem.at[side, i],
            device_id={"train": (right, left)[side]},
            device_id_type=MESH,
        )

    block_row = index((BLOCK, 128), 0)

    def patch(p):
        tail_of = tail_pick(p)
        for side, (b, last) in enumerate(((1, False), (HELD - 2, True))):
            tail = jnp.dot(hrecv[side, 0:BLOCK, 0:64], tail_of, preferred_element_type=F32)
            for h in range(2):
                layer = 2 * p + h
                if last:
                    take = block_row >= offsets[layer, t + 1] - t * ROWS_DEV - (ROWS_DEV - BLOCK)
                else:
                    take = block_row < offsets[layer, t] - t * ROWS_DEV
                at = layer * HELD + b
                window = pl.ds(pl.multiple_of(BLOCK + layer * BLOCK, BLOCK), BLOCK)
                main = hrecv[side, window].astype(F32)
                turned[at] = jnp.where(take, main, turned[at].astype(F32)).astype(BF)
                rest[at] = jnp.where(
                    take, tail[:, 128 * h : 128 * h + 128], rest[at].astype(F32)
                ).astype(BF)

    def patch_step(p, carry):
        patch(p)
        return carry

    def message(i, v):
        return pltpu.make_async_remote_copy(
            src_ref=sends[i].at[v],
            dst_ref=recvs[i].at[me],
            send_sem=s_sem.at[i, v],
            recv_sem=r_sem.at[i, v],
            device_id={"serve": peer(v)},
            device_id_type=MESH,
        )

    def tail_of_block(total, at, slot):
        pair = rest[at]
        for h in range(2):
            total = total + pair[h * 16 : h * 16 + 16] * lanes[lax.rem(2 * slot + h + me, 32)]
        return total

    def dispatch(i):
        f, n, ends_n = MESSAGES[i]

        def fill(dest, place, group):
            total = jnp.zeros((16, 128), BF)
            for slot in range(max(n, ends_n) * BASE):
                layer, k = f + slot // BASE, slot % BASE
                at = layer * HELD + 1 + table[layer, group * SLOTS + k]
                if slot < n * BASE:
                    dest[place, slot * BLOCK : slot * BLOCK + BLOCK] = turned[at]
                if ends_n:
                    total = tail_of_block(total, at, slot)
            if ends_n:
                dest[place, LENGTHS[i] - 16 : LENGTHS[i]] = total

        def send_step(j, carry):
            v = SERVE_N - 1 - j
            fill(sends[i], v, peer(v))
            message(i, v).start()
            return carry

        lax.fori_loop(0, SERVE_N - 1, send_step, 0)
        fill(recvs[i], me, me)

    own_list, next_list = mc * 8 + mx * 4 + my, mc * 8 + (1 - mx) * 4 + my

    def list_copy(i):
        if i == 0:
            window, target = pl.ds(own_list, 1), (1 - mx) * 8 + my * 2 + mc
        elif i < 4:
            window, target = pl.ds(own_list, 1), mx * 8 + lax.rem(my + i, 4) * 2 + mc
        elif i < 7:
            window, target = pl.ds(next_list, 1), mx * 8 + lax.rem(my + i - 3, 4) * 2 + mc
        else:
            window, target = pl.ds(8 * mc, 8), mx * 8 + my * 2 + 1 - mc
        return pltpu.make_async_remote_copy(
            src_ref=lists.at[window],
            dst_ref=lists.at[window],
            send_sem=ls_sem.at[i],
            recv_sem=lr_sem.at[i],
            device_id={"serve": target},
            device_id_type=MESH,
        )

    def dispatch_list():
        total = jnp.zeros((16, 128), BF)
        for e in range(EXTRA):
            at = table[48 + e, 0]
            lists[own_list, e * BLOCK : e * BLOCK + BLOCK] = turned[at]
            total = tail_of_block(total, at, e)
        lists[own_list, LIST - 16 : LIST] = total
        for i in range(4):
            list_copy(i).start()

    lane = index((BLOCK, 128), 1)

    def take_tails(recv, rows, count, base):
        def tail_step(q, carry):
            total = jnp.zeros((16, 128), BF)
            for s in range(SERVE_N):
                total = total + recv[place_of(recv, s), rows] * lanes[lax.rem(q + s, 32)]
            tails[base + q // 2, pl.ds(pl.multiple_of(lax.rem(q, 2) * 16, 16), 16)] = pltpu.roll(
                total.astype(F32), 128 - 4 * q, axis=1
            )
            return carry

        lax.fori_loop(0, 2 * count, tail_step, 0)

    def place_of(recv, s):
        return s % 2 * 8 + s // 8 * 4 + s // 2 % 4 if recv is lists else s

    def scale_block(recv, slot, tail, at, there, codes_out, scales_out):
        before = None
        for j in range(TILES):
            if j < SERVE_N:
                window = pl.ds(pl.multiple_of(slot * BLOCK, BLOCK), BLOCK)
                now = recv[place_of(recv, j), window].astype(F32)
            else:
                now = tail
            if j == 0:
                value = now
            else:
                value = jnp.where(lane < 4 * j - 4, before, jnp.where(lane < 4 * j, tail, now))
            before = now
            top = jnp.maximum(jnp.max(jnp.abs(value), axis=0, keepdims=True), 0.25)
            codes = (value * (there / top)).astype(BF)
            width = min(128, FEAT - j * 128)
            codes_out[at, :, j * 128 : j * 128 + width] = codes[:, :width]
            scales_out[at, :, j * 128 : j * 128 + width] = (top * there)[:, :width]

    def present(layer, k):
        return jnp.minimum(jnp.maximum(table[16 + layer, me] - k, 0), 1).astype(F32)

    def finish(i):
        f, n, ends_n = MESSAGES[i]

        def arrive(j, carry):
            message(i, j + 1).wait_recv()
            return carry

        lax.fori_loop(0, SERVE_N - 1, arrive, 0)
        if ends_n:
            take_tails(recvs[i], slice(LENGTHS[i] - 16, LENGTHS[i]), ends_n * BASE, 0)
        past = 0 if ends_n else (f - MESSAGES[i - 1][0]) * BASE

        def base_step(slot, carry):
            layer, k = f + slot // BASE, lax.rem(slot, BASE)
            scale_block(
                recvs[i], slot, tails[past + slot], layer * SLOTS + k, present(layer, k), out, scales
            )
            return carry

        lax.fori_loop(0, n * BASE, base_step, 0)

    def finish_list():
        list_copy(7).wait_recv()
        take_tails(lists, slice(LIST - 16, LIST), EXTRA, 16)

        def extra_step(entry, carry):
            scale_block(lists, entry, tails[16 + entry], entry, 1.0, extra_codes, extra_scales)
            return carry

        lax.fori_loop(0, EXTRA, extra_step, 0)

        def place_step(layer, carry):
            entry, there = table[32 + layer, me], present(layer, BASE)
            at = layer * SLOTS + BASE
            out[at] = (extra_codes[entry].astype(F32) * there).astype(BF)
            scales[at] = extra_scales[entry] * there
            return carry

        lax.fori_loop(0, LAYERS, place_step, 0)

    def tell(step):
        return pltpu.make_async_remote_copy(
            src_ref=fsend,
            dst_ref=frecv.at[t],
            send_sem=fs_sem.at[step],
            recv_sem=fr_sem.at[step],
            device_id={"train": lax.rem(t + step, TRAIN_N)},
            device_id_type=MESH,
        )

    pl.semaphore_wait(barrier, SERVE_N + TRAIN_N - 2)
    for i in range(3):
        for side in range(2):
            halo(side, i).start()
    for copy in small:
        copy.wait()
    named[...] = jnp.full((16, 128), -1, I32)
    named[:, 0:BLOCKS_DEV] = groups[...]
    group = named[...]
    order = jnp.zeros((16, 128), I32)
    for d in range(1, BLOCKS_DEV):
        same = (pltpu.roll(group, d, axis=1) == group) & (lane16 >= d)
        order = order + jnp.where(same, 1, 0)
    slot_of = group * SLOTS + order
    blocks_at = jnp.zeros((16, 128), I32)
    third_at = jnp.zeros((16, 128), I32)
    counted = jnp.zeros((16, 128), I32)
    for b in range(BLOCKS_DEV):
        slot_b = slot_of[:, b : b + 1]
        blocks_at = jnp.where(slot_b == lane16, b, blocks_at)
        third_at = jnp.where(slot_b == lane16 * SLOTS + BASE, b, third_at)
        counted = counted + jnp.where(group[:, b : b + 1] == lane16, 1, 0)
    third = jnp.where(counted > BASE, 1, 0)
    rows_third = jnp.broadcast_to(jnp.sum(third, axis=1, keepdims=True), (16, 128))
    before = jnp.zeros((16, 128), I32)
    for d in range(1, LAYERS):
        before = before + jnp.where(row16 >= d, pltpu.roll(rows_third, d, axis=0), 0)
        before = before + jnp.where(lane16 >= d, pltpu.roll(third, d, axis=1), 0)
    found[0:16] = blocks_at
    found[16:32] = counted
    found[32:48] = jnp.minimum(before, EXTRA - 1)
    where_third = row16 * HELD + 1 + third_at

    def whole(x):
        return jnp.sum(jnp.sum(x, axis=0, keepdims=True), axis=1, keepdims=True)

    for e in range(EXTRA):
        mine = (third > 0) & (before == e)
        found[48 + e : 49 + e] = jnp.broadcast_to(whole(jnp.where(mine, where_third, 0)), (1, 128))
    known = pltpu.make_async_copy(found, table, table_sem)
    known.start()
    long = jnp.where(whole(third) > EXTRA, 1.0, 0.0)
    fsend[...] = jnp.broadcast_to(long, (8, 128))
    frecv[t] = fsend[...]

    for step in range(1, TRAIN_N):
        tell(step).start()
    for copy in loads[2]:
        copy.wait()
    for m in range(8):
        gather_columns(m, middle)
    turn_tail(middle)
    lax.fori_loop(0, 1, prepare_step, 0)
    known.wait()
    for side in range(2):
        halo(side, 0).wait_recv()
    patch(0)
    dispatch(0)
    lax.fori_loop(1, PAIRS, prepare_step, 0, unroll=7)
    for side in range(2):
        halo(side, 1).wait_recv()
        halo(side, 2).wait_recv()
    lax.fori_loop(1, PAIRS, patch_step, 0)
    dispatch_list()
    dispatch(1)
    finish(0)
    list_copy(0).wait_recv()
    for i in range(4, 7):
        list_copy(i).start()
    dispatch(2)
    dispatch(3)
    finish(1)
    for i in range(1, 7):
        list_copy(i).wait_recv()
    list_copy(7).start()
    finish_list()
    finish(2)
    finish(3)
    for i in range(8):
        list_copy(i).wait_send()
    for step in range(1, TRAIN_N):
        tell(step).wait()
    flag[...] = jnp.broadcast_to(jnp.max(frecv[...]).reshape(1, 1), (8, 128))

    for side in range(2):
        halo(side, 0).wait_send()
        halo(side, 1).wait_send()
        halo(side, 2).wait_send()
    for i in range(len(MESSAGES)):
        def leave(j, carry, i=i):
            message(i, j + 1).wait_send()
            return carry

        lax.fori_loop(0, SERVE_N - 1, leave, 0)


def everything(train_weights, row_offset, groups):
    position = jnp.arange(BLOCKS_DEV, dtype=I32)
    earlier = position[None, :] < position[:, None]
    same = groups[:, :, None] == groups[:, None, :]
    order = jnp.sum((same & earlier[None]).astype(I32), axis=2)
    slot_id = groups * SLOTS + order
    onehot = slot_id[:, None, :] == jnp.arange(SERVE_N * SLOTS, dtype=I32)[None, :, None]
    blocks_at = jnp.sum(jnp.where(onehot, position[None, None, :], 0), axis=2)
    group_ids = jnp.arange(SERVE_N, dtype=I32)
    counts = jnp.sum((groups[:, None, :] == group_ids[None, :, None]).astype(I32), axis=2)
    held = (counts[:, :, None] > jnp.arange(SLOTS, dtype=I32)).astype(I32)
    held = held.reshape(LAYERS, SERVE_N * SLOTS)
    weights = train_weights.reshape(LAYERS, HELD, BLOCK, COLS)
    parts = len(PARTS)
    smem = pl.BlockSpec(memory_space=pltpu.SMEM)
    vmem = pl.BlockSpec(memory_space=pltpu.VMEM)
    return pl.pallas_call(
        full_exchange,
        out_shape=(
            pltpu.VMEM((LAYERS * SLOTS, BLOCK, FEAT), BF),
            pltpu.VMEM((LAYERS * SLOTS, 1, FEAT), F32),
        ),
        in_specs=[smem, smem, smem, pl.BlockSpec(memory_space=pl.ANY)],
        out_specs=(vmem, vmem),
        scratch_shapes=[
            pltpu.VMEM((LAYERS, HELD, BLOCK, COLS), BF),
            pltpu.VMEM((2, LAYERS, BLOCK, COLS), BF),
            pltpu.VMEM((COLS, 256), BF),
            pltpu.VMEM((32, 16, 128), BF),
            pltpu.VMEM((max(PARTS) * SLOTS, BLOCK, 128), F32),
            pltpu.VMEM((max(PARTS), BLOCKS_DEV, BLOCK, 128), BF),
            pltpu.VMEM((max(PARTS), BLOCKS_DEV, BLOCK, 128), BF),
            pltpu.VMEM((2, HALO, 128), BF),
            pltpu.VMEM((2, HALO, 128), BF),
            pltpu.VMEM((SERVE_N, TOTAL, 128), BF),
            pltpu.VMEM((SERVE_N, TOTAL, 128), BF),
            pltpu.VMEM((128, 128), BF),
            pltpu.SemaphoreType.DMA((parts,)),
            pltpu.SemaphoreType.DMA((2,)),
            pltpu.SemaphoreType.DMA((2, parts)),
            pltpu.SemaphoreType.DMA((2, parts)),
            pltpu.SemaphoreType.DMA((parts, SERVE_N)),
            pltpu.SemaphoreType.DMA((parts, SERVE_N)),
        ],
        compiler_params=pltpu.CompilerParams(
            collective_id=1, has_side_effects=True, vmem_limit_bytes=44 * 2**20
        ),
    )(blocks_at, held, row_offset, weights)


def shards(train_weights, row_offset, block_group):
    groups = block_group[:, :, 0]
    smem = pl.BlockSpec(memory_space=pltpu.SMEM)
    vmem = pl.BlockSpec(memory_space=pltpu.VMEM)
    parts = len(MESSAGES)
    codes, scales, flag = pl.pallas_call(
        route,
        out_shape=(
            pltpu.VMEM((LAYERS * SLOTS, BLOCK, FEAT), BF),
            pltpu.VMEM((LAYERS * SLOTS, 1, FEAT), F32),
            jax.ShapeDtypeStruct((8, 128), F32),
        ),
        in_specs=[pl.BlockSpec(memory_space=pl.ANY)] * 3,
        out_specs=(vmem, vmem, vmem),
        scratch_shapes=[
            pltpu.VMEM((LAYERS, BLOCKS_DEV), I32),
            pltpu.SMEM((LAYERS, TRAIN_N + 1), I32),
            pltpu.VMEM((LAYERS, 128), I32),
            pltpu.VMEM((56, 128), I32),
            pltpu.SMEM((56, 128), I32),
            pltpu.VMEM((COLS + 16, LAYERS, BUFFER), BF),
            pltpu.VMEM((256, 256), BF),
            pltpu.VMEM((256, 256), BF),
            pltpu.VMEM((128 * LAYERS, BUFFER), BF),
            pltpu.VMEM((BUFFER, 64), BF),
            pltpu.VMEM((32, 16, 128), BF),
            pltpu.VMEM((LAYERS * HELD, BLOCK, 128), BF),
            pltpu.VMEM((LAYERS * HELD, BLOCK, 128), BF),
            pltpu.VMEM((2, EDGE, 128), BF),
            pltpu.VMEM((2, EDGE, 128), BF),
            pltpu.VMEM((16 + EXTRA, BLOCK, 128), F32),
            pltpu.VMEM((EXTRA, BLOCK, FEAT), BF),
            pltpu.VMEM((EXTRA, 1, FEAT), F32),
            pltpu.VMEM((8, 128), F32),
            pltpu.VMEM((TRAIN_N, 8, 128), F32),
            *[pltpu.VMEM((SERVE_N, length, 128), BF) for length in LENGTHS * 2],
            pltpu.VMEM((SERVE_N, LIST, 128), BF),
            pltpu.SemaphoreType.DMA((2,)),
            pltpu.SemaphoreType.DMA,
            pltpu.SemaphoreType.DMA((3, 3)),
            pltpu.SemaphoreType.DMA((2, 3)),
            pltpu.SemaphoreType.DMA((2, 3)),
            pltpu.SemaphoreType.DMA((parts, SERVE_N)),
            pltpu.SemaphoreType.DMA((parts, SERVE_N)),
            pltpu.SemaphoreType.DMA((8,)),
            pltpu.SemaphoreType.DMA((8,)),
            pltpu.SemaphoreType.DMA((TRAIN_N,)),
            pltpu.SemaphoreType.DMA((TRAIN_N,)),
        ],
        compiler_params=pltpu.CompilerParams(
            collective_id=2, has_side_effects=True, vmem_limit_bytes=46 * 2**20
        ),
    )(
        groups, row_offset, jnp.transpose(train_weights, (2, 0, 1)),
    )
    codes, scales = lax.cond(
        flag[0, 0] > 0.0,
        lambda: tuple(everything(train_weights, row_offset, groups)),
        lambda: (codes, scales),
    )
    return (
        codes.reshape(LAYERS, 1, 1, SLOTS, BLOCK, FEAT),
        scales.reshape(LAYERS, 1, 1, SLOTS, FEAT),
    )


def solution(mesh):
    return jax.shard_map(
        shards,
        mesh=mesh,
        in_specs=(P(None, "train", "serve"), P(), P(None, "train", None)),
        out_specs=(P(None, "serve", "train", None, None, None), P(None, "serve", "train", None, None)),
        check_vma=False,
    )
```

```python
import functools

import jax
import jax.numpy as jnp
from jax import lax
from jax.experimental import pallas as pl
from jax.experimental.pallas import tpu as pltpu
from jax.sharding import PartitionSpec as P

MESH = pl.DeviceIdType.MESH
BF = jnp.bfloat16
F32 = jnp.float32
I32 = jnp.int32
LAYERS = 16
BLOCK = 32
BLOCKS_DEV = 28
HELD = BLOCKS_DEV + 2
ROWS_DEV = 896
BUFFER = HELD * BLOCK
COLS = 132
SERVE_N = 16
TRAIN_N = 8
SLOTS = 3
FEAT = SERVE_N * COLS
TILES = -(-FEAT // 128)

PARTS = (2, 4, 4, 4, 2)
FIRST = (0, 2, 6, 10, 14)
SIZES = tuple(n * SLOTS * BLOCK + 16 for n in PARTS)
BASES = tuple(sum(SIZES[:i]) for i in range(len(PARTS)))
TOTAL = sum(SIZES)
HALO = 16 + LAYERS * BLOCK
HALO_ENDS = tuple(16 + (f + n) * BLOCK for f, n in zip(FIRST, PARTS))
HALO_BASES = (0,) + HALO_ENDS[:-1]

BASE = 2
EXTRA = 8
MESSAGES = (
    (0, 2, ()),
    (2, 3, tuple(range(2, 10))),
    (5, 5, ()),
    (10, 4, tuple(range(10, 16)) + (0, 1)),
    (14, 2, ()),
)
LENGTHS = tuple(n * BASE * BLOCK + (16 if m else 0) for _, n, m in MESSAGES)
TAIL_AT = tuple(
    next(m.index(f) * BASE for _, _, m in MESSAGES if f in m) for f, _, _ in MESSAGES
)
LIST = EXTRA * BLOCK + 16
PAIRS = LAYERS // 2
EARLY = 5
EDGE = BLOCK + LAYERS * BLOCK
HALO_STARTS = (0, 3 * BLOCK, (1 + 2 * EARLY) * BLOCK, EDGE)


def full_exchange(
    blocks_at, held, offsets, weights, out, scales,
    raw, edge, rot, lanes, tails, turned, rest, hsend, hrecv, send, recv, patch,
    raw_sem, edge_sem, hs_sem, hr_sem, s_sem, r_sem,
):
    t = lax.axis_index("train")
    me = lax.axis_index("serve")
    mx, my, mc = me // 8, lax.rem(me // 2, 4), lax.rem(me, 2)
    right, left = lax.rem(t + 1, TRAIN_N), lax.rem(t + TRAIN_N - 1, TRAIN_N)

    def peer(v):
        return (
            lax.rem(mx + v // 8, 2) * 8
            + lax.rem(my + lax.rem(v // 2, 4), 4) * 2
            + lax.rem(mc + lax.rem(v, 2), 2)
        )

    barrier = pltpu.get_barrier_semaphore()
    for v in range(1, SERVE_N):
        pl.semaphore_signal(barrier, inc=1, device_id={"serve": peer(v)}, device_id_type=MESH)
    for other in (left, right):
        pl.semaphore_signal(barrier, inc=1, device_id={"train": other}, device_id_type=MESH)

    edges = [
        pltpu.make_async_copy(weights.at[:, b], edge.at[side], edge_sem.at[side])
        for side, b in enumerate((BLOCKS_DEV + 1, 0))
    ]
    loads = [
        pltpu.make_async_copy(weights.at[pl.ds(f, n)], raw.at[pl.ds(f, n)], raw_sem.at[i])
        for i, (f, n) in enumerate(zip(FIRST, PARTS))
    ]
    for copy in edges + loads:
        copy.start()

    row = lax.broadcasted_iota(jnp.int32, (COLS, 256), 0)
    col = lax.broadcasted_iota(jnp.int32, (COLS, 256), 1)
    turn = (row < 128) & (col < 128) & (col == ((row + 4 * me) & 127))
    spread = (row >= 128) & (col >= 128) & ((col & 3) == row - 128)
    rot[...] = jnp.where(turn | spread, 1.0, 0.0).astype(BF)
    lane16 = lax.broadcasted_iota(jnp.int32, (16, 128), 1)
    for m in range(32):
        lanes[m] = jnp.where((lane16 >> 2) == m, 1.0, 0.0).astype(BF)
    rrow = lax.broadcasted_iota(jnp.int32, (128, 128), 0)
    rcol = lax.broadcasted_iota(jnp.int32, (128, 128), 1)
    patch[...] = jnp.where((rrow & 3) == (rcol & 3), 1.0, 0.0).astype(BF)

    for copy in edges:
        copy.wait()
    for side in range(2):
        def edge_step(i, total, side=side):
            x = edge[side, pl.ds(i * 4, 4)].reshape(4 * BLOCK, COLS)
            y = jnp.dot(x, rot[...], preferred_element_type=F32).astype(BF)
            hsend[side, pl.ds(pl.multiple_of(16 + i * 128, 16), 128)] = y[:, :128]
            for q in range(8):
                total = total + y[q * 16 : q * 16 + 16, 128:] * lanes[lax.rem(i * 8 + q + me, 32)]
            return total

        hsend[side, 0:16] = lax.fori_loop(0, LAYERS // 4, edge_step, jnp.zeros((16, 128), BF))

    pl.semaphore_wait(barrier, SERVE_N + 1)

    halos = []
    for i in range(len(PARTS)):
        window = pl.ds(HALO_BASES[i], HALO_ENDS[i] - HALO_BASES[i])
        for side, target in enumerate((right, left)):
            copy = pltpu.make_async_remote_copy(
                src_ref=hsend.at[side, window],
                dst_ref=hrecv.at[side, window],
                send_sem=hs_sem.at[side, i],
                recv_sem=hr_sem.at[side, i],
                device_id={"train": target},
                device_id_type=MESH,
            )
            copy.start()
            halos.append(copy)

    def block_copy(i, v):
        window = pl.ds(BASES[i], SIZES[i])
        return pltpu.make_async_remote_copy(
            src_ref=send.at[v, window],
            dst_ref=recv.at[me, window],
            send_sem=s_sem.at[i, v],
            recv_sem=r_sem.at[i, v],
            device_id={"serve": peer(v)},
            device_id_type=MESH,
        )

    block_row = lax.broadcasted_iota(jnp.int32, (BLOCK, 128), 0)

    for i, (f, n) in enumerate(zip(FIRST, PARTS)):
        loads[i].wait()

        def turn_step(j, carry, f=f):
            l, b = j // 7, lax.rem(j, 7) * 4
            x = raw[f + l, pl.ds(b + 1, 4)].reshape(4 * BLOCK, COLS)
            y = jnp.dot(x, rot[...], preferred_element_type=F32).astype(BF)
            turned[l, pl.ds(b, 4)] = y[:, :128].reshape(4, BLOCK, 128)
            rest[l, pl.ds(b, 4)] = y[:, 128:].reshape(4, BLOCK, 128)
            return carry

        lax.fori_loop(0, n * 7, turn_step, 0)
        halos[2 * i].wait_recv()
        halos[2 * i + 1].wait_recv()

        def patch_step(l, carry, f=f):
            layer = f + l
            first = offsets[layer, t] - t * ROWS_DEV
            last = offsets[layer, t + 1] - t * ROWS_DEV - (ROWS_DEV - BLOCK)
            for side, (b, take) in enumerate(
                ((0, block_row < first), (BLOCKS_DEV - 1, block_row >= last))
            ):
                main = hrecv[side, pl.ds(pl.multiple_of(16 + layer * BLOCK, 16), BLOCK)]
                packed = hrecv[side, 0:16]
                both = jnp.concatenate(
                    [packed * lanes[lax.rem(2 * layer + h + me, 32)] for h in range(2)], axis=0
                )
                tail = jnp.dot(both, patch[...], preferred_element_type=F32)
                turned[l, b] = jnp.where(take, main.astype(F32), turned[l, b].astype(F32)).astype(BF)
                rest[l, b] = jnp.where(take, tail, rest[l, b].astype(F32)).astype(BF)
            return carry

        lax.fori_loop(0, n, patch_step, 0)

        def fill(dest, index, group, i=i, f=f, n=n):
            total = jnp.zeros((16, 128), BF)
            for l in range(n):
                for k in range(SLOTS):
                    slot = l * SLOTS + k
                    b = blocks_at[f + l, group * SLOTS + k]
                    dest[index, pl.ds(BASES[i] + slot * BLOCK, BLOCK)] = turned[l, b]
                    pair = rest[l, b]
                    for h in range(2):
                        total = total + pair[h * 16 : h * 16 + 16] * lanes[
                            lax.rem(2 * slot + h + me, 32)
                        ]
            dest[index, pl.ds(BASES[i] + n * SLOTS * BLOCK, 16)] = total

        def send_step(j, carry, i=i, fill=fill):
            v = SERVE_N - 1 - j
            fill(send, v, peer(v))
            block_copy(i, v).start()
            return carry

        lax.fori_loop(0, SERVE_N - 1, send_step, 0)
        fill(recv, me, me)

    lane = lax.broadcasted_iota(jnp.int32, (BLOCK, 128), 1)
    for i, (f, n) in enumerate(zip(FIRST, PARTS)):
        def arrive(j, carry, i=i):
            block_copy(i, j + 1).wait_recv()
            return carry

        lax.fori_loop(0, SERVE_N - 1, arrive, 0)

        def tail_step(q, carry, i=i, n=n):
            total = jnp.zeros((16, 128), BF)
            for s in range(SERVE_N):
                total = total + recv[s, pl.ds(BASES[i] + n * SLOTS * BLOCK, 16)] * lanes[
                    lax.rem(q + s, 32)
                ]
            tails[q // 2, pl.ds(pl.multiple_of(lax.rem(q, 2) * 16, 16), 16)] = pltpu.roll(
                total.astype(F32), 128 - 4 * q, axis=1
            )
            return carry

        lax.fori_loop(0, 2 * n * SLOTS, tail_step, 0)

        def block_step(slot, carry, i=i, f=f):
            layer, k = f + slot // SLOTS, lax.rem(slot, SLOTS)
            there = held[layer, me * SLOTS + k].astype(F32)
            at = f * SLOTS + slot
            tail = tails[slot]
            before = None
            for j in range(TILES):
                if j < SERVE_N:
                    now = recv[j, pl.ds(pl.multiple_of(BASES[i] + slot * BLOCK, 16), BLOCK)].astype(F32)
                else:
                    now = tail
                if j == 0:
                    value = now
                else:
                    value = jnp.where(
                        lane < 4 * j - 4, before, jnp.where(lane < 4 * j, tail, now)
                    )
                before = now
                top = jnp.maximum(jnp.max(jnp.abs(value), axis=0, keepdims=True), 0.25)
                codes = (value * (there / top)).astype(BF)
                width = min(128, FEAT - j * 128)
                out[at, :, j * 128 : j * 128 + width] = codes[:, :width]
                scales[at, :, j * 128 : j * 128 + width] = (top * there)[:, :width]
            return carry

        lax.fori_loop(0, n * SLOTS, block_step, 0)

    for copy in halos:
        copy.wait_send()
    for i in range(len(PARTS)):
        def leave(j, carry, i=i):
            block_copy(i, j + 1).wait_send()
            return carry

        lax.fori_loop(0, SERVE_N - 1, leave, 0)


def route(
    groups_in, offsets_in, weights, out, scales, flag,
    groups, offsets, named, found, table, raw, eye, spread, turning, mixed_tail, lanes, turned, rest,
    hsend, hrecv, tails, extra_codes, extra_scales, fsend, frecv,
    send0, send1, send2, send3, send4, recv0, recv1, recv2, recv3, recv4, lists,
    small_sem, table_sem, raw_sem, hs_sem, hr_sem, s_sem, r_sem, ls_sem, lr_sem, fs_sem, fr_sem,
):
    sends = (send0, send1, send2, send3, send4)
    recvs = (recv0, recv1, recv2, recv3, recv4)
    t = lax.axis_index("train")
    me = lax.axis_index("serve")
    mx, my, mc = me // 8, lax.rem(me // 2, 4), lax.rem(me, 2)
    right, left = lax.rem(t + 1, TRAIN_N), lax.rem(t + TRAIN_N - 1, TRAIN_N)

    def peer(v):
        return (
            lax.rem(mx + v // 8, 2) * 8
            + lax.rem(my + lax.rem(v // 2, 4), 4) * 2
            + lax.rem(mc + lax.rem(v, 2), 2)
        )

    small = [
        pltpu.make_async_copy(groups_in, groups, small_sem.at[0]),
        pltpu.make_async_copy(offsets_in, offsets, small_sem.at[1]),
    ]
    loads = [
        [
            pltpu.make_async_copy(
                weights.at[a : a + n, :, r : r + w], raw.at[b : b + n, :, r : r + w], raw_sem.at[i, j]
            )
            for j, (a, b, n) in enumerate(((0, 16, COLS), (112, 0, 16)))
        ]
        for i, (r, w) in enumerate(((0, 128), (896, 64), (128, 768)))
    ]
    for copy in loads[0] + loads[1] + small + loads[2]:
        copy.start()

    barrier = pltpu.get_barrier_semaphore()
    for v in range(1, SERVE_N):
        pl.semaphore_signal(barrier, inc=1, device_id={"serve": peer(v)}, device_id_type=MESH)
    for step in range(1, TRAIN_N):
        pl.semaphore_signal(
            barrier, inc=1, device_id={"train": lax.rem(t + step, TRAIN_N)}, device_id_type=MESH
        )

    def index(shape, dim):
        return lax.broadcasted_iota(I32, shape, dim)

    def ones(cond):
        return jnp.where(cond, 1.0, 0.0).astype(BF)

    lane16, row16 = index((16, 128), 1), index((16, 128), 0)
    eye[...] = ones(index((256, 256), 0) == index((256, 256), 1))
    a, b = index((256, 256), 0), index((256, 256), 1)
    spread[...] = ones(((b >> 4) == (a & 15)) & ((b & 15) == (a >> 4)))
    for m in range(32):
        lanes[m] = ones((lane16 >> 2) == m)

    NT = (((1,), (1,)), ((), ()))

    def gather_columns(m, tiles):
        start = 16 * (m + 1) - 4 * lax.rem(me, 4)
        place = 16 * lax.rem(m + me // 4, 8)
        for r, w in tiles:
            x = raw[pl.ds(start, 16), :, r : r + w].reshape(256, w)
            y = jnp.dot(spread[...], x, preferred_element_type=F32).astype(BF)
            for layer in range(LAYERS):
                window = pl.ds(pl.multiple_of(128 * layer + place, 16), 16)
                turning[window, r : r + w] = y[16 * layer : 16 * layer + 16]

    ends, middle = ((0, 128), (896, 64)), ((128, 256), (384, 256), (640, 256))
    for copy in loads[0] + loads[1]:
        copy.wait()
    for m in range(8):
        gather_columns(m, ends)

    def turn_tail(tiles):
        for r, w in tiles:
            x = raw[144:148, :, r : r + w].reshape(64, w)
            y = lax.dot_general(eye[:w, :w], x, NT, preferred_element_type=F32)
            mixed_tail[r : r + w] = y.astype(BF)

    turn_tail(ends)
    hsend[0, 0:BLOCK, 0:64] = mixed_tail[BUFFER - BLOCK : BUFFER]
    hsend[1, 0:BLOCK, 0:64] = mixed_tail[0:BLOCK]
    hsend[0, 0:BLOCK, 64:128] = jnp.zeros((BLOCK, 64), BF)
    hsend[1, 0:BLOCK, 64:128] = jnp.zeros((BLOCK, 64), BF)

    def edge_step(p, carry):
        rows = pl.ds(pl.multiple_of(256 * p, 256), 256)
        low = lax.dot_general(eye[0:32, 0:128], turning[rows, 0:128], NT, preferred_element_type=F32)
        high = lax.dot_general(
            eye[32:64, 0:64], turning[rows, 896:960], NT, preferred_element_type=F32
        )
        for h in range(2):
            window = pl.ds(pl.multiple_of(BLOCK + (2 * p + h) * BLOCK, BLOCK), BLOCK)
            hsend[0, window] = high[:, 128 * h : 128 * h + 128].astype(BF)
            hsend[1, window] = low[:, 128 * h : 128 * h + 128].astype(BF)
        return carry

    lax.fori_loop(0, PAIRS, edge_step, 0, unroll=8)

    def tail_pick(p):
        k, q = index((64, 256), 0), index((64, 256), 1)
        return ones(((k & 15) == 2 * p + (q >> 7)) & ((k >> 4) == (q & 3)))

    def prepare_step(p, carry):
        rows = pl.ds(pl.multiple_of(256 * p, 256), 256)
        tail_of = tail_pick(p)
        for r, w in ((0, 128), (128, 256), (384, 256), (640, 256), (896, 64)):
            y = lax.dot_general(
                eye[:w, :w], turning[rows, r : r + w], NT, preferred_element_type=F32
            ).astype(BF)
            z = jnp.dot(mixed_tail[r : r + w], tail_of, preferred_element_type=F32).astype(BF)
            for h in range(2):
                at = pl.ds((2 * p + h) * HELD + r // BLOCK, w // BLOCK)
                turned[at] = y[:, 128 * h : 128 * h + 128].reshape(w // BLOCK, BLOCK, 128)
                rest[at] = z[:, 128 * h : 128 * h + 128].reshape(w // BLOCK, BLOCK, 128)
        return carry

    has_next = (t < TRAIN_N - 1, t > 0)

    def halo_arrived(i):
        for side in range(2):
            @pl.when(has_next[1 - side])
            def _(side=side):
                halo(side, i).wait_recv()

    def halo(side, i):
        window = pl.ds(HALO_STARTS[i], HALO_STARTS[i + 1] - HALO_STARTS[i])
        return pltpu.make_async_remote_copy(
            src_ref=hsend.at[side, window],
            dst_ref=hrecv.at[side, window],
            send_sem=hs_sem.at[side],
            recv_sem=hr_sem.at[side, i],
            device_id={"train": (right, left)[side]},
            device_id_type=MESH,
        )

    block_row = index((BLOCK, 128), 0)

    def patch(p):
        tail_of = tail_pick(p)
        for side, (b, last) in enumerate(((1, False), (HELD - 2, True))):
            tail = jnp.dot(hrecv[side, 0:BLOCK, 0:64], tail_of, preferred_element_type=F32)
            for h in range(2):
                layer = 2 * p + h
                if last:
                    take = block_row >= offsets[layer, t + 1] - t * ROWS_DEV - (ROWS_DEV - BLOCK)
                else:
                    take = block_row < offsets[layer, t] - t * ROWS_DEV
                at = layer * HELD + b
                window = pl.ds(pl.multiple_of(BLOCK + layer * BLOCK, BLOCK), BLOCK)
                main = hrecv[side, window].astype(F32)
                turned[at] = jnp.where(take, main, turned[at].astype(F32)).astype(BF)
                rest[at] = jnp.where(
                    take, tail[:, 128 * h : 128 * h + 128], rest[at].astype(F32)
                ).astype(BF)

    def patch_step(p, carry):
        patch(p)
        return carry

    def message(i, v):
        return pltpu.make_async_remote_copy(
            src_ref=sends[i].at[v],
            dst_ref=recvs[i].at[me],
            send_sem=s_sem.at[i],
            recv_sem=r_sem.at[i],
            device_id={"serve": peer(v)},
            device_id_type=MESH,
        )

    def tail_of_block(total, at, slot):
        pair = rest[at]
        for h in range(2):
            total = total + pair[h * 16 : h * 16 + 16] * lanes[lax.rem(2 * slot + h + me, 32)]
        return total

    def all_messages(i):
        most = pl.ds(0, SERVE_N - 1)
        return pltpu.make_async_remote_copy(
            src_ref=sends[i].at[most],
            dst_ref=recvs[i].at[most],
            send_sem=s_sem.at[i],
            recv_sem=r_sem.at[i],
            device_id={"serve": peer(1)},
            device_id_type=MESH,
        )

    def dispatch(i):
        f, n, ends_at = MESSAGES[i]

        def fill(dest, place, group):
            for slot in range(n * BASE):
                layer, k = f + slot // BASE, slot % BASE
                at = layer * HELD + 1 + table[layer, group * SLOTS + k]
                dest[place, slot * BLOCK : slot * BLOCK + BLOCK] = turned[at]
            if ends_at:
                total = jnp.zeros((16, 128), BF)
                for slot in range(len(ends_at) * BASE):
                    layer, k = ends_at[slot // BASE], slot % BASE
                    at = layer * HELD + 1 + table[layer, group * SLOTS + k]
                    total = tail_of_block(total, at, slot)
                dest[place, LENGTHS[i] - 16 : LENGTHS[i]] = total

        def send_step(j, carry):
            v = SERVE_N - 1 - j
            fill(sends[i], v, peer(v))
            message(i, v).start()
            return carry

        lax.fori_loop(0, SERVE_N - 1, send_step, 0)
        fill(recvs[i], me, me)

    def list_of(dx, dy):
        return mc * 8 + lax.rem(mx + dx, 2) * 4 + lax.rem(my + dy, 4)

    def list_copy(i):
        lists_at, dx, dy, dc = (
            (pl.ds(list_of(0, 0), 1), 1, 0, 0),
            (pl.ds(list_of(0, 0), 1), 0, 1, 0),
            (pl.ds(list_of(0, 0), 1), 0, 3, 0),
            (pl.ds(list_of(0, 3), 1), 0, 1, 0),
            (pl.ds(list_of(1, 0), 1), 0, 1, 0),
            (pl.ds(list_of(1, 0), 1), 0, 3, 0),
            (pl.ds(list_of(0, 2), 1), 1, 0, 0),
            (pl.ds(8 * mc, 8), 0, 0, 1),
        )[i]
        return pltpu.make_async_remote_copy(
            src_ref=lists.at[lists_at],
            dst_ref=lists.at[lists_at],
            send_sem=ls_sem,
            recv_sem=lr_sem.at[(0, 1, 4, 2, 4, 4, 4, 3)[i]],
            device_id={"serve": peer(8 * dx + 2 * dy + dc)},
            device_id_type=MESH,
        )

    def some_lists(n):
        return pltpu.make_async_remote_copy(
            src_ref=lists.at[pl.ds(0, n)],
            dst_ref=lists.at[pl.ds(0, n)],
            send_sem=ls_sem,
            recv_sem=lr_sem.at[4],
            device_id={"serve": peer(1)},
            device_id_type=MESH,
        )

    def dispatch_list():
        total = jnp.zeros((16, 128), BF)
        for e in range(EXTRA):
            at = table[48 + e, 0]
            lists[list_of(0, 0), e * BLOCK : e * BLOCK + BLOCK] = turned[at]
            total = tail_of_block(total, at, e)
        lists[list_of(0, 0), LIST - 16 : LIST] = total
        for i in range(3):
            list_copy(i).start()

    lane = index((BLOCK, 128), 1)

    def take_tails(recv, rows, count, base):
        def tail_step(q, carry):
            total = jnp.zeros((16, 128), BF)
            for s in range(SERVE_N):
                total = total + recv[place_of(recv, s), rows] * lanes[lax.rem(q + s, 32)]
            tails[base + q // 2, pl.ds(pl.multiple_of(lax.rem(q, 2) * 16, 16), 16)] = pltpu.roll(
                total.astype(F32), 128 - 4 * q, axis=1
            )
            return carry

        lax.fori_loop(0, 2 * count, tail_step, 0)

    def place_of(recv, s):
        return s % 2 * 8 + s // 8 * 4 + s // 2 % 4 if recv is lists else s

    def scale_block(recv, slot, tail, at, there, codes_out, scales_out):
        before = None
        for j in range(TILES):
            if j < SERVE_N:
                window = pl.ds(pl.multiple_of(slot * BLOCK, BLOCK), BLOCK)
                now = recv[place_of(recv, j), window].astype(F32)
            else:
                now = tail
            if j == 0:
                value = now
            else:
                value = jnp.where(lane < 4 * j - 4, before, jnp.where(lane < 4 * j, tail, now))
            before = now
            top = jnp.maximum(jnp.max(jnp.abs(value), axis=0, keepdims=True), 0.25)
            codes = (value * (there / top)).astype(BF)
            width = min(128, FEAT - j * 128)
            codes_out[at, :, j * 128 : j * 128 + width] = codes[:, :width]
            scales_out[at, :, j * 128 : j * 128 + width] = (top * there)[:, :width]

    def present(layer, k):
        return jnp.minimum(jnp.maximum(table[16 + layer, me] - k, 0), 1).astype(F32)

    def receive(i):
        f, n, ends_at = MESSAGES[i]

        all_messages(i).wait_recv()
        if ends_at:
            take_tails(recvs[i], slice(LENGTHS[i] - 16, LENGTHS[i]), len(ends_at) * BASE, 0)

    def scale_message(i):
        f, n, _ = MESSAGES[i]

        def base_step(slot, carry):
            layer, k = f + slot // BASE, lax.rem(slot, BASE)
            scale_block(
                recvs[i], slot, tails[TAIL_AT[i] + slot], layer * SLOTS + k, present(layer, k), out, scales
            )
            return carry

        lax.fori_loop(0, n * BASE, base_step, 0)

    def finish_list():
        list_copy(7).wait_recv()
        take_tails(lists, slice(LIST - 16, LIST), EXTRA, 16)

        def extra_step(entry, carry):
            scale_block(lists, entry, tails[16 + entry], entry, 1.0, extra_codes, extra_scales)
            return carry

        lax.fori_loop(0, EXTRA, extra_step, 0)

        def place_step(layer, carry):
            entry, there = table[32 + layer, me], present(layer, BASE)
            at = layer * SLOTS + BASE
            out[at] = (extra_codes[entry].astype(F32) * there).astype(BF)
            scales[at] = extra_scales[entry] * there
            return carry

        lax.fori_loop(0, LAYERS, place_step, 0)

    def left_all(i):
        all_messages(i).wait_send()

    def halo_left():
        for side in range(2):
            @pl.when(has_next[side])
            def _(side=side):
                pltpu.make_async_remote_copy(
                    src_ref=hsend.at[side],
                    dst_ref=hrecv.at[side],
                    send_sem=hs_sem.at[side],
                    recv_sem=hr_sem.at[side, 0],
                    device_id={"train": (right, left)[side]},
                    device_id_type=MESH,
                ).wait_send()

    def tell(step):
        return pltpu.make_async_remote_copy(
            src_ref=fsend,
            dst_ref=frecv.at[t],
            send_sem=fs_sem,
            recv_sem=fr_sem,
            device_id={"train": lax.rem(t + step, TRAIN_N)},
            device_id_type=MESH,
        )

    pl.semaphore_wait(barrier, SERVE_N + TRAIN_N - 2)
    for side in range(2):
        @pl.when(has_next[side])
        def _(side=side):
            halo(side, 0).start()

        @pl.when(jnp.logical_not(has_next[1 - side]))
        def _(side=side):
            hrecv[side] = jnp.zeros((EDGE, 128), BF)
    for copy in small:
        copy.wait()
    named[...] = jnp.full((16, 128), -1, I32)
    named[:, 0:BLOCKS_DEV] = groups[...]
    group = named[...]
    order = jnp.zeros((16, 128), I32)
    for d in range(1, BLOCKS_DEV):
        same = (pltpu.roll(group, d, axis=1) == group) & (lane16 >= d)
        order = order + jnp.where(same, 1, 0)
    slot_of = group * SLOTS + order
    blocks_at = jnp.zeros((16, 128), I32)
    third_at = jnp.zeros((16, 128), I32)
    counted = jnp.zeros((16, 128), I32)
    for b in range(BLOCKS_DEV):
        slot_b = slot_of[:, b : b + 1]
        blocks_at = jnp.where(slot_b == lane16, b, blocks_at)
        third_at = jnp.where(slot_b == lane16 * SLOTS + BASE, b, third_at)
        counted = counted + jnp.where(group[:, b : b + 1] == lane16, 1, 0)
    third = jnp.where(counted > BASE, 1, 0)
    rows_third = jnp.broadcast_to(jnp.sum(third, axis=1, keepdims=True), (16, 128))
    before = jnp.zeros((16, 128), I32)
    for d in range(1, LAYERS):
        before = before + jnp.where(row16 >= d, pltpu.roll(rows_third, d, axis=0), 0)
        before = before + jnp.where(lane16 >= d, pltpu.roll(third, d, axis=1), 0)
    found[0:16] = blocks_at
    found[16:32] = counted
    found[32:48] = jnp.minimum(before, EXTRA - 1)
    where_third = row16 * HELD + 1 + third_at

    def whole(x):
        return jnp.sum(jnp.sum(x, axis=0, keepdims=True), axis=1, keepdims=True)

    for e in range(EXTRA):
        mine = (third > 0) & (before == e)
        found[48 + e : 49 + e] = jnp.broadcast_to(whole(jnp.where(mine, where_third, 0)), (1, 128))
    known = pltpu.make_async_copy(found, table, table_sem)
    known.start()
    long = jnp.where(whole(third) > EXTRA, 1.0, 0.0)
    fsend[...] = jnp.broadcast_to(long, (8, 128))
    frecv[t] = fsend[...]

    for side in range(2):
        @pl.when(has_next[side])
        def _(side=side):
            halo(side, 1).start()
            halo(side, 2).start()

    for step in range(1, TRAIN_N):
        tell(step).start()
    for copy in loads[2]:
        copy.wait()
    for m in range(8):
        gather_columns(m, middle)
    turn_tail(middle)
    lax.fori_loop(0, 1, prepare_step, 0)
    known.wait()
    halo_arrived(0)
    patch(0)
    dispatch(0)
    lax.fori_loop(1, PAIRS, prepare_step, 0, unroll=7)
    halo_arrived(1)
    halo_arrived(2)
    lax.fori_loop(1, PAIRS, patch_step, 0)
    dispatch_list()
    dispatch(1)
    for i in range(2):
        list_copy(i).wait_recv()
    for i in range(3, 6):
        list_copy(i).start()
    dispatch(2)
    receive(0)
    left_all(0)
    receive(1)
    scale_message(1)
    list_copy(3).wait_recv()
    list_copy(6).start()
    dispatch(3)
    dispatch(4)
    left_all(1)
    receive(2)
    scale_message(2)
    some_lists(4).wait_recv()
    list_copy(7).start()
    left_all(2)
    told = pltpu.make_async_remote_copy(
        src_ref=frecv.at[0 : TRAIN_N - 1],
        dst_ref=frecv.at[0 : TRAIN_N - 1],
        send_sem=fs_sem,
        recv_sem=fr_sem,
        device_id={"train": right},
        device_id_type=MESH,
    )
    told.wait_send()
    told.wait_recv()
    flag[...] = jnp.broadcast_to(jnp.max(frecv[...]).reshape(1, 1), (8, 128))
    halo_left()
    finish_list()
    receive(3)
    scale_message(3)
    scale_message(0)
    some_lists(15).wait_send()
    receive(4)
    scale_message(4)
    left_all(3)
    left_all(4)


def everything(train_weights, row_offset, groups):
    position = jnp.arange(BLOCKS_DEV, dtype=I32)
    earlier = position[None, :] < position[:, None]
    same = groups[:, :, None] == groups[:, None, :]
    order = jnp.sum((same & earlier[None]).astype(I32), axis=2)
    slot_id = groups * SLOTS + order
    onehot = slot_id[:, None, :] == jnp.arange(SERVE_N * SLOTS, dtype=I32)[None, :, None]
    blocks_at = jnp.sum(jnp.where(onehot, position[None, None, :], 0), axis=2)
    group_ids = jnp.arange(SERVE_N, dtype=I32)
    counts = jnp.sum((groups[:, None, :] == group_ids[None, :, None]).astype(I32), axis=2)
    held = (counts[:, :, None] > jnp.arange(SLOTS, dtype=I32)).astype(I32)
    held = held.reshape(LAYERS, SERVE_N * SLOTS)
    weights = train_weights.reshape(LAYERS, HELD, BLOCK, COLS)
    parts = len(PARTS)
    smem = pl.BlockSpec(memory_space=pltpu.SMEM)
    vmem = pl.BlockSpec(memory_space=pltpu.VMEM)
    return pl.pallas_call(
        full_exchange,
        out_shape=(
            pltpu.VMEM((LAYERS * SLOTS, BLOCK, FEAT), BF),
            pltpu.VMEM((LAYERS * SLOTS, 1, FEAT), F32),
        ),
        in_specs=[smem, smem, smem, pl.BlockSpec(memory_space=pl.ANY)],
        out_specs=(vmem, vmem),
        scratch_shapes=[
            pltpu.VMEM((LAYERS, HELD, BLOCK, COLS), BF),
            pltpu.VMEM((2, LAYERS, BLOCK, COLS), BF),
            pltpu.VMEM((COLS, 256), BF),
            pltpu.VMEM((32, 16, 128), BF),
            pltpu.VMEM((max(PARTS) * SLOTS, BLOCK, 128), F32),
            pltpu.VMEM((max(PARTS), BLOCKS_DEV, BLOCK, 128), BF),
            pltpu.VMEM((max(PARTS), BLOCKS_DEV, BLOCK, 128), BF),
            pltpu.VMEM((2, HALO, 128), BF),
            pltpu.VMEM((2, HALO, 128), BF),
            pltpu.VMEM((SERVE_N, TOTAL, 128), BF),
            pltpu.VMEM((SERVE_N, TOTAL, 128), BF),
            pltpu.VMEM((128, 128), BF),
            pltpu.SemaphoreType.DMA((parts,)),
            pltpu.SemaphoreType.DMA((2,)),
            pltpu.SemaphoreType.DMA((2, parts)),
            pltpu.SemaphoreType.DMA((2, parts)),
            pltpu.SemaphoreType.DMA((parts, SERVE_N)),
            pltpu.SemaphoreType.DMA((parts, SERVE_N)),
        ],
        compiler_params=pltpu.CompilerParams(
            collective_id=1, has_side_effects=True, vmem_limit_bytes=44 * 2**20
        ),
    )(blocks_at, held, row_offset, weights)


def shards(train_weights, row_offset, block_group):
    groups = block_group[:, :, 0]
    smem = pl.BlockSpec(memory_space=pltpu.SMEM)
    vmem = pl.BlockSpec(memory_space=pltpu.VMEM)
    parts = len(MESSAGES)
    codes, scales, flag = pl.pallas_call(
        route,
        out_shape=(
            pltpu.VMEM((LAYERS * SLOTS, BLOCK, FEAT), BF),
            pltpu.VMEM((LAYERS * SLOTS, 1, FEAT), F32),
            jax.ShapeDtypeStruct((8, 128), F32),
        ),
        in_specs=[pl.BlockSpec(memory_space=pl.ANY)] * 3,
        out_specs=(vmem, vmem, vmem),
        scratch_shapes=[
            pltpu.VMEM((LAYERS, BLOCKS_DEV), I32),
            pltpu.SMEM((LAYERS, TRAIN_N + 1), I32),
            pltpu.VMEM((LAYERS, 128), I32),
            pltpu.VMEM((56, 128), I32),
            pltpu.SMEM((56, 128), I32),
            pltpu.VMEM((COLS + 16, LAYERS, BUFFER), BF),
            pltpu.VMEM((256, 256), BF),
            pltpu.VMEM((256, 256), BF),
            pltpu.VMEM((128 * LAYERS, BUFFER), BF),
            pltpu.VMEM((BUFFER, 64), BF),
            pltpu.VMEM((32, 16, 128), BF),
            pltpu.VMEM((LAYERS * HELD, BLOCK, 128), BF),
            pltpu.VMEM((LAYERS * HELD, BLOCK, 128), BF),
            pltpu.VMEM((2, EDGE, 128), BF),
            pltpu.VMEM((2, EDGE, 128), BF),
            pltpu.VMEM((16 + EXTRA, BLOCK, 128), F32),
            pltpu.VMEM((EXTRA, BLOCK, FEAT), BF),
            pltpu.VMEM((EXTRA, 1, FEAT), F32),
            pltpu.VMEM((8, 128), F32),
            pltpu.VMEM((TRAIN_N, 8, 128), F32),
            *[pltpu.VMEM((SERVE_N, length, 128), BF) for length in LENGTHS * 2],
            pltpu.VMEM((SERVE_N, LIST, 128), BF),
            pltpu.SemaphoreType.DMA((2,)),
            pltpu.SemaphoreType.DMA,
            pltpu.SemaphoreType.DMA((3, 2)),
            pltpu.SemaphoreType.DMA((2,)),
            pltpu.SemaphoreType.DMA((2, 3)),
            pltpu.SemaphoreType.DMA((parts,)),
            pltpu.SemaphoreType.DMA((parts,)),
            pltpu.SemaphoreType.DMA,
            pltpu.SemaphoreType.DMA((5,)),
            pltpu.SemaphoreType.DMA,
            pltpu.SemaphoreType.DMA,
        ],
        compiler_params=pltpu.CompilerParams(
            collective_id=2, has_side_effects=True, vmem_limit_bytes=46 * 2**20
        ),
    )(
        groups, row_offset, jnp.transpose(train_weights, (2, 0, 1)),
    )
    codes, scales = lax.cond(
        flag[0, 0] > 0.0,
        lambda: tuple(everything(train_weights, row_offset, groups)),
        lambda: (codes, scales),
    )
    return (
        codes.reshape(LAYERS, 1, 1, SLOTS, BLOCK, FEAT),
        scales.reshape(LAYERS, 1, 1, SLOTS, FEAT),
    )


def solution(mesh):
    return jax.shard_map(
        shards,
        mesh=mesh,
        in_specs=(P(None, "train", "serve"), P(), P(None, "train", None)),
        out_specs=(P(None, "serve", "train", None, None, None), P(None, "serve", "train", None, None)),
        check_vma=False,
    )
```

```python
import functools

import jax
import jax.numpy as jnp
from jax import lax
from jax.experimental import pallas as pl
from jax.experimental.pallas import tpu as pltpu
from jax.sharding import PartitionSpec as P

MESH = pl.DeviceIdType.MESH
BF = jnp.bfloat16
F32 = jnp.float32
I32 = jnp.int32
LAYERS = 16
BLOCK = 32
BLOCKS_DEV = 28
HELD = BLOCKS_DEV + 2
ROWS_DEV = 896
BUFFER = HELD * BLOCK
COLS = 132
SERVE_N = 16
TRAIN_N = 8
SLOTS = 3
FEAT = SERVE_N * COLS
TILES = -(-FEAT // 128)

PARTS = (2, 4, 4, 4, 2)
FIRST = (0, 2, 6, 10, 14)
SIZES = tuple(n * SLOTS * BLOCK + 16 for n in PARTS)
BASES = tuple(sum(SIZES[:i]) for i in range(len(PARTS)))
TOTAL = sum(SIZES)
HALO = 16 + LAYERS * BLOCK
HALO_ENDS = tuple(16 + (f + n) * BLOCK for f, n in zip(FIRST, PARTS))
HALO_BASES = (0,) + HALO_ENDS[:-1]

BASE = 2
EXTRA = 8
MESSAGES = (
    (0, 2, ()),
    (2, 3, tuple(range(2, 10))),
    (5, 5, ()),
    (10, 4, tuple(range(10, 16)) + (0, 1)),
    (14, 2, ()),
)
LENGTHS = tuple(n * BASE * BLOCK + (16 if m else 0) for _, n, m in MESSAGES)
TAIL_AT = tuple(
    next(m.index(f) * BASE for _, _, m in MESSAGES if f in m) for f, _, _ in MESSAGES
)
LIST = EXTRA * BLOCK + 16
PAIRS = LAYERS // 2
EARLY = 5
EDGE = BLOCK + LAYERS * BLOCK
HALO_STARTS = (0, 3 * BLOCK, (1 + 2 * EARLY) * BLOCK, EDGE)


def full_exchange(
    blocks_at, held, offsets, weights, out, scales,
    raw, edge, rot, lanes, tails, turned, rest, hsend, hrecv, send, recv, patch,
    raw_sem, edge_sem, hs_sem, hr_sem, s_sem, r_sem,
):
    t = lax.axis_index("train")
    me = lax.axis_index("serve")
    mx, my, mc = me // 8, lax.rem(me // 2, 4), lax.rem(me, 2)
    right, left = lax.rem(t + 1, TRAIN_N), lax.rem(t + TRAIN_N - 1, TRAIN_N)

    def peer(v):
        return (
            lax.rem(mx + v // 8, 2) * 8
            + lax.rem(my + lax.rem(v // 2, 4), 4) * 2
            + lax.rem(mc + lax.rem(v, 2), 2)
        )

    barrier = pltpu.get_barrier_semaphore()
    for v in range(1, SERVE_N):
        pl.semaphore_signal(barrier, inc=1, device_id={"serve": peer(v)}, device_id_type=MESH)
    for other in (left, right):
        pl.semaphore_signal(barrier, inc=1, device_id={"train": other}, device_id_type=MESH)

    edges = [
        pltpu.make_async_copy(weights.at[:, b], edge.at[side], edge_sem.at[side])
        for side, b in enumerate((BLOCKS_DEV + 1, 0))
    ]
    loads = [
        pltpu.make_async_copy(weights.at[pl.ds(f, n)], raw.at[pl.ds(f, n)], raw_sem.at[i])
        for i, (f, n) in enumerate(zip(FIRST, PARTS))
    ]
    for copy in edges + loads:
        copy.start()

    row = lax.broadcasted_iota(jnp.int32, (COLS, 256), 0)
    col = lax.broadcasted_iota(jnp.int32, (COLS, 256), 1)
    turn = (row < 128) & (col < 128) & (col == ((row + 4 * me) & 127))
    spread = (row >= 128) & (col >= 128) & ((col & 3) == row - 128)
    rot[...] = jnp.where(turn | spread, 1.0, 0.0).astype(BF)
    lane16 = lax.broadcasted_iota(jnp.int32, (16, 128), 1)
    for m in range(32):
        lanes[m] = jnp.where((lane16 >> 2) == m, 1.0, 0.0).astype(BF)
    rrow = lax.broadcasted_iota(jnp.int32, (128, 128), 0)
    rcol = lax.broadcasted_iota(jnp.int32, (128, 128), 1)
    patch[...] = jnp.where((rrow & 3) == (rcol & 3), 1.0, 0.0).astype(BF)

    for copy in edges:
        copy.wait()
    for side in range(2):
        def edge_step(i, total, side=side):
            x = edge[side, pl.ds(i * 4, 4)].reshape(4 * BLOCK, COLS)
            y = jnp.dot(x, rot[...], preferred_element_type=F32).astype(BF)
            hsend[side, pl.ds(pl.multiple_of(16 + i * 128, 16), 128)] = y[:, :128]
            for q in range(8):
                total = total + y[q * 16 : q * 16 + 16, 128:] * lanes[lax.rem(i * 8 + q + me, 32)]
            return total

        hsend[side, 0:16] = lax.fori_loop(0, LAYERS // 4, edge_step, jnp.zeros((16, 128), BF))

    pl.semaphore_wait(barrier, SERVE_N + 1)

    halos = []
    for i in range(len(PARTS)):
        window = pl.ds(HALO_BASES[i], HALO_ENDS[i] - HALO_BASES[i])
        for side, target in enumerate((right, left)):
            copy = pltpu.make_async_remote_copy(
                src_ref=hsend.at[side, window],
                dst_ref=hrecv.at[side, window],
                send_sem=hs_sem.at[side, i],
                recv_sem=hr_sem.at[side, i],
                device_id={"train": target},
                device_id_type=MESH,
            )
            copy.start()
            halos.append(copy)

    def block_copy(i, v):
        window = pl.ds(BASES[i], SIZES[i])
        return pltpu.make_async_remote_copy(
            src_ref=send.at[v, window],
            dst_ref=recv.at[me, window],
            send_sem=s_sem.at[i, v],
            recv_sem=r_sem.at[i, v],
            device_id={"serve": peer(v)},
            device_id_type=MESH,
        )

    block_row = lax.broadcasted_iota(jnp.int32, (BLOCK, 128), 0)

    for i, (f, n) in enumerate(zip(FIRST, PARTS)):
        loads[i].wait()

        def turn_step(j, carry, f=f):
            l, b = j // 7, lax.rem(j, 7) * 4
            x = raw[f + l, pl.ds(b + 1, 4)].reshape(4 * BLOCK, COLS)
            y = jnp.dot(x, rot[...], preferred_element_type=F32).astype(BF)
            turned[l, pl.ds(b, 4)] = y[:, :128].reshape(4, BLOCK, 128)
            rest[l, pl.ds(b, 4)] = y[:, 128:].reshape(4, BLOCK, 128)
            return carry

        lax.fori_loop(0, n * 7, turn_step, 0)
        halos[2 * i].wait_recv()
        halos[2 * i + 1].wait_recv()

        def patch_step(l, carry, f=f):
            layer = f + l
            first = offsets[layer, t] - t * ROWS_DEV
            last = offsets[layer, t + 1] - t * ROWS_DEV - (ROWS_DEV - BLOCK)
            for side, (b, take) in enumerate(
                ((0, block_row < first), (BLOCKS_DEV - 1, block_row >= last))
            ):
                main = hrecv[side, pl.ds(pl.multiple_of(16 + layer * BLOCK, 16), BLOCK)]
                packed = hrecv[side, 0:16]
                both = jnp.concatenate(
                    [packed * lanes[lax.rem(2 * layer + h + me, 32)] for h in range(2)], axis=0
                )
                tail = jnp.dot(both, patch[...], preferred_element_type=F32)
                turned[l, b] = jnp.where(take, main.astype(F32), turned[l, b].astype(F32)).astype(BF)
                rest[l, b] = jnp.where(take, tail, rest[l, b].astype(F32)).astype(BF)
            return carry

        lax.fori_loop(0, n, patch_step, 0)

        def fill(dest, index, group, i=i, f=f, n=n):
            total = jnp.zeros((16, 128), BF)
            for l in range(n):
                for k in range(SLOTS):
                    slot = l * SLOTS + k
                    b = blocks_at[f + l, group * SLOTS + k]
                    dest[index, pl.ds(BASES[i] + slot * BLOCK, BLOCK)] = turned[l, b]
                    pair = rest[l, b]
                    for h in range(2):
                        total = total + pair[h * 16 : h * 16 + 16] * lanes[
                            lax.rem(2 * slot + h + me, 32)
                        ]
            dest[index, pl.ds(BASES[i] + n * SLOTS * BLOCK, 16)] = total

        def send_step(j, carry, i=i, fill=fill):
            v = SERVE_N - 1 - j
            fill(send, v, peer(v))
            block_copy(i, v).start()
            return carry

        lax.fori_loop(0, SERVE_N - 1, send_step, 0)
        fill(recv, me, me)

    lane = lax.broadcasted_iota(jnp.int32, (BLOCK, 128), 1)
    for i, (f, n) in enumerate(zip(FIRST, PARTS)):
        def arrive(j, carry, i=i):
            block_copy(i, j + 1).wait_recv()
            return carry

        lax.fori_loop(0, SERVE_N - 1, arrive, 0)

        def tail_step(q, carry, i=i, n=n):
            total = jnp.zeros((16, 128), BF)
            for s in range(SERVE_N):
                total = total + recv[s, pl.ds(BASES[i] + n * SLOTS * BLOCK, 16)] * lanes[
                    lax.rem(q + s, 32)
                ]
            tails[q // 2, pl.ds(pl.multiple_of(lax.rem(q, 2) * 16, 16), 16)] = pltpu.roll(
                total.astype(F32), 128 - 4 * q, axis=1
            )
            return carry

        lax.fori_loop(0, 2 * n * SLOTS, tail_step, 0)

        def block_step(slot, carry, i=i, f=f):
            layer, k = f + slot // SLOTS, lax.rem(slot, SLOTS)
            there = held[layer, me * SLOTS + k].astype(F32)
            at = f * SLOTS + slot
            tail = tails[slot]
            before = None
            for j in range(TILES):
                if j < SERVE_N:
                    now = recv[j, pl.ds(pl.multiple_of(BASES[i] + slot * BLOCK, 16), BLOCK)].astype(F32)
                else:
                    now = tail
                if j == 0:
                    value = now
                else:
                    value = jnp.where(
                        lane < 4 * j - 4, before, jnp.where(lane < 4 * j, tail, now)
                    )
                before = now
                top = jnp.maximum(jnp.max(jnp.abs(value), axis=0, keepdims=True), 0.25)
                codes = (value * (there / top)).astype(BF)
                width = min(128, FEAT - j * 128)
                out[at, :, j * 128 : j * 128 + width] = codes[:, :width]
                scales[at, :, j * 128 : j * 128 + width] = (top * there)[:, :width]
            return carry

        lax.fori_loop(0, n * SLOTS, block_step, 0)

    for copy in halos:
        copy.wait_send()
    for i in range(len(PARTS)):
        def leave(j, carry, i=i):
            block_copy(i, j + 1).wait_send()
            return carry

        lax.fori_loop(0, SERVE_N - 1, leave, 0)


def route(
    groups_in, offsets_in, weights, out, scales, flag,
    groups, offsets, named, found, table, raw, eye, spread, turning, mixed_tail, lanes, turned, rest,
    hsend, hrecv, tails, extra_codes, extra_scales, fsend, frecv,
    send0, send1, send2, send3, send4, recv0, recv1, recv2, recv3, recv4, lists,
    small_sem, table_sem, raw_sem, hs_sem, hr_sem, s_sem, r_sem, ls_sem, lr_sem, fs_sem, fr_sem,
):
    sends = (send0, send1, send2, send3, send4)
    recvs = (recv0, recv1, recv2, recv3, recv4)
    t = lax.axis_index("train")
    me = lax.axis_index("serve")
    mx, my, mc = me // 8, lax.rem(me // 2, 4), lax.rem(me, 2)
    right, left = lax.rem(t + 1, TRAIN_N), lax.rem(t + TRAIN_N - 1, TRAIN_N)

    def peer(v):
        return (
            lax.rem(mx + v // 8, 2) * 8
            + lax.rem(my + lax.rem(v // 2, 4), 4) * 2
            + lax.rem(mc + lax.rem(v, 2), 2)
        )

    small = [
        pltpu.make_async_copy(groups_in, groups, small_sem.at[0]),
        pltpu.make_async_copy(offsets_in, offsets, small_sem.at[1]),
    ]
    loads = [
        [
            pltpu.make_async_copy(
                weights.at[a : a + n, :, r : r + w], raw.at[b : b + n, :, r : r + w], raw_sem.at[i, j]
            )
            for j, (a, b, n) in enumerate(((0, 16, COLS), (112, 0, 16)))
        ]
        for i, (r, w) in enumerate(((0, 128), (896, 64), (128, 768)))
    ]
    for copy in loads[0] + loads[1] + small + loads[2]:
        copy.start()

    barrier = pltpu.get_barrier_semaphore()
    for v in range(1, SERVE_N):
        pl.semaphore_signal(barrier, inc=1, device_id={"serve": peer(v)}, device_id_type=MESH)
    for step in range(1, TRAIN_N):
        pl.semaphore_signal(
            barrier, inc=1, device_id={"train": lax.rem(t + step, TRAIN_N)}, device_id_type=MESH
        )

    def index(shape, dim):
        return lax.broadcasted_iota(I32, shape, dim)

    def ones(cond):
        return jnp.where(cond, 1.0, 0.0).astype(BF)

    lane16, row16 = index((16, 128), 1), index((16, 128), 0)
    eye[...] = ones(index((256, 256), 0) == index((256, 256), 1))
    a, b = index((256, 256), 0), index((256, 256), 1)
    spread[...] = ones(((b >> 4) == (a & 15)) & ((b & 15) == (a >> 4)))
    for m in range(32):
        lanes[m] = ones((lane16 >> 2) == m)

    NT = (((1,), (1,)), ((), ()))

    def gather_columns(m, tiles):
        start = 16 * (m + 1) - 4 * lax.rem(me, 4)
        place = 16 * lax.rem(m + me // 4, 8)
        for r, w in tiles:
            x = raw[pl.ds(start, 16), :, r : r + w].reshape(256, w)
            y = jnp.dot(spread[...], x, preferred_element_type=F32).astype(BF)
            for layer in range(LAYERS):
                window = pl.ds(pl.multiple_of(128 * layer + place, 16), 16)
                turning[window, r : r + w] = y[16 * layer : 16 * layer + 16]

    ends, middle = ((0, 128), (896, 64)), ((128, 256), (384, 256), (640, 256))
    for copy in loads[0] + loads[1]:
        copy.wait()
    for m in range(8):
        gather_columns(m, ends)

    def turn_tail(tiles):
        for r, w in tiles:
            x = raw[144:148, :, r : r + w].reshape(64, w)
            y = lax.dot_general(eye[:w, :w], x, NT, preferred_element_type=F32)
            mixed_tail[r : r + w] = y.astype(BF)

    turn_tail(ends)
    hsend[0, 0:BLOCK, 0:64] = mixed_tail[BUFFER - BLOCK : BUFFER]
    hsend[1, 0:BLOCK, 0:64] = mixed_tail[0:BLOCK]
    hsend[0, 0:BLOCK, 64:128] = jnp.zeros((BLOCK, 64), BF)
    hsend[1, 0:BLOCK, 64:128] = jnp.zeros((BLOCK, 64), BF)

    def edge_step(p, carry):
        rows = pl.ds(pl.multiple_of(256 * p, 256), 256)
        low = lax.dot_general(eye[0:32, 0:128], turning[rows, 0:128], NT, preferred_element_type=F32)
        high = lax.dot_general(
            eye[32:64, 0:64], turning[rows, 896:960], NT, preferred_element_type=F32
        )
        for h in range(2):
            window = pl.ds(pl.multiple_of(BLOCK + (2 * p + h) * BLOCK, BLOCK), BLOCK)
            hsend[0, window] = high[:, 128 * h : 128 * h + 128].astype(BF)
            hsend[1, window] = low[:, 128 * h : 128 * h + 128].astype(BF)
        return carry

    lax.fori_loop(0, PAIRS, edge_step, 0, unroll=8)

    def tail_pick(p):
        k, q = index((64, 256), 0), index((64, 256), 1)
        return ones(((k & 15) == 2 * p + (q >> 7)) & ((k >> 4) == (q & 3)))

    def prepare_step(p, carry):
        rows = pl.ds(pl.multiple_of(256 * p, 256), 256)
        tail_of = tail_pick(p)
        for r, w in ((0, 128), (128, 256), (384, 256), (640, 256), (896, 64)):
            y = lax.dot_general(
                eye[:w, :w], turning[rows, r : r + w], NT, preferred_element_type=F32
            ).astype(BF)
            z = jnp.dot(mixed_tail[r : r + w], tail_of, preferred_element_type=F32).astype(BF)
            for h in range(2):
                at = pl.ds((2 * p + h) * HELD + r // BLOCK, w // BLOCK)
                turned[at] = y[:, 128 * h : 128 * h + 128].reshape(w // BLOCK, BLOCK, 128)
                rest[at] = z[:, 128 * h : 128 * h + 128].reshape(w // BLOCK, BLOCK, 128)
        return carry

    has_next = (t < TRAIN_N - 1, t > 0)

    def halo_arrived(i):
        for side in range(2):
            @pl.when(has_next[1 - side])
            def _(side=side):
                halo(side, i).wait_recv()

    def halo(side, i):
        window = pl.ds(HALO_STARTS[i], HALO_STARTS[i + 1] - HALO_STARTS[i])
        return pltpu.make_async_remote_copy(
            src_ref=hsend.at[side, window],
            dst_ref=hrecv.at[side, window],
            send_sem=hs_sem.at[side],
            recv_sem=hr_sem.at[side, i],
            device_id={"train": (right, left)[side]},
            device_id_type=MESH,
        )

    block_row = index((BLOCK, 128), 0)

    def patch(p):
        tail_of = tail_pick(p)
        for side, (b, last) in enumerate(((1, False), (HELD - 2, True))):
            tail = jnp.dot(hrecv[side, 0:BLOCK, 0:64], tail_of, preferred_element_type=F32)
            for h in range(2):
                layer = 2 * p + h
                if last:
                    take = block_row >= offsets[layer, t + 1] - t * ROWS_DEV - (ROWS_DEV - BLOCK)
                else:
                    take = block_row < offsets[layer, t] - t * ROWS_DEV
                at = layer * HELD + b
                window = pl.ds(pl.multiple_of(BLOCK + layer * BLOCK, BLOCK), BLOCK)
                main = hrecv[side, window].astype(F32)
                turned[at] = jnp.where(take, main, turned[at].astype(F32)).astype(BF)
                rest[at] = jnp.where(
                    take, tail[:, 128 * h : 128 * h + 128], rest[at].astype(F32)
                ).astype(BF)

    def patch_step(p, carry):
        patch(p)
        return carry

    def message(i, v):
        return pltpu.make_async_remote_copy(
            src_ref=sends[i].at[v],
            dst_ref=recvs[i].at[me],
            send_sem=s_sem.at[i],
            recv_sem=r_sem.at[i],
            device_id={"serve": peer(v)},
            device_id_type=MESH,
        )

    def tail_of_block(total, at, slot):
        pair = rest[at]
        for h in range(2):
            total = total + pair[h * 16 : h * 16 + 16] * lanes[lax.rem(2 * slot + h + me, 32)]
        return total

    def all_messages(i):
        most = pl.ds(0, SERVE_N - 1)
        return pltpu.make_async_remote_copy(
            src_ref=sends[i].at[most],
            dst_ref=recvs[i].at[most],
            send_sem=s_sem.at[i],
            recv_sem=r_sem.at[i],
            device_id={"serve": peer(1)},
            device_id_type=MESH,
        )

    def dispatch(i):
        f, n, ends_at = MESSAGES[i]

        def fill(dest, place, group):
            for slot in range(n * BASE):
                layer, k = f + slot // BASE, slot % BASE
                at = layer * HELD + 1 + table[layer, group * SLOTS + k]
                dest[place, slot * BLOCK : slot * BLOCK + BLOCK] = turned[at]
            if ends_at:
                total = jnp.zeros((16, 128), BF)
                for slot in range(len(ends_at) * BASE):
                    layer, k = ends_at[slot // BASE], slot % BASE
                    at = layer * HELD + 1 + table[layer, group * SLOTS + k]
                    total = tail_of_block(total, at, slot)
                dest[place, LENGTHS[i] - 16 : LENGTHS[i]] = total

        def send_step(j, carry):
            v = SERVE_N - 1 - j
            turn = lax.rem(lax.rem(v // 2, 4) * (1 + 2 * mc), 4)
            v = v // 8 * 8 + turn * 2 + lax.rem(v, 2)
            fill(sends[i], v, peer(v))
            message(i, v).start()
            return carry

        lax.fori_loop(0, SERVE_N - 1, send_step, 0)
        fill(recvs[i], me, me)

    def list_of(dx, dy):
        return mc * 8 + lax.rem(mx + dx, 2) * 4 + lax.rem(my + dy, 4)

    def list_copy(i):
        lists_at, dx, dy, dc = (
            (pl.ds(list_of(0, 0), 1), 1, 0, 0),
            (pl.ds(list_of(0, 0), 1), 0, 1, 0),
            (pl.ds(list_of(0, 0), 1), 0, 3, 0),
            (pl.ds(list_of(0, 3), 1), 0, 1, 0),
            (pl.ds(list_of(1, 0), 1), 0, 1, 0),
            (pl.ds(list_of(0, 1), 1), 1, 0, 0),
            (pl.ds(list_of(0, 2), 1), 1, 0, 0),
            (pl.ds(8 * mc, 8), 0, 0, 1),
        )[i]
        return pltpu.make_async_remote_copy(
            src_ref=lists.at[lists_at],
            dst_ref=lists.at[lists_at],
            send_sem=ls_sem,
            recv_sem=lr_sem.at[(0, 1, 5, 2, 4, 4, 4, 3)[i]],
            device_id={"serve": peer(8 * dx + 2 * dy + dc)},
            device_id_type=MESH,
        )

    def some_lists(n):
        return pltpu.make_async_remote_copy(
            src_ref=lists.at[pl.ds(0, n)],
            dst_ref=lists.at[pl.ds(0, n)],
            send_sem=ls_sem,
            recv_sem=lr_sem.at[4],
            device_id={"serve": peer(1)},
            device_id_type=MESH,
        )

    def dispatch_list():
        total = jnp.zeros((16, 128), BF)
        for e in range(EXTRA):
            at = table[48 + e, 0]
            lists[list_of(0, 0), e * BLOCK : e * BLOCK + BLOCK] = turned[at]
            total = tail_of_block(total, at, e)
        lists[list_of(0, 0), LIST - 16 : LIST] = total
        for i in range(3):
            list_copy(i).start()

    lane = index((BLOCK, 128), 1)

    def take_tails(recv, rows, count, base):
        def tail_step(q, carry):
            total = jnp.zeros((16, 128), BF)
            for s in range(SERVE_N):
                total = total + recv[place_of(recv, s), rows] * lanes[lax.rem(q + s, 32)]
            tails[base + q // 2, pl.ds(pl.multiple_of(lax.rem(q, 2) * 16, 16), 16)] = pltpu.roll(
                total.astype(F32), 128 - 4 * q, axis=1
            )
            return carry

        lax.fori_loop(0, 2 * count, tail_step, 0)

    def place_of(recv, s):
        return s % 2 * 8 + s // 8 * 4 + s // 2 % 4 if recv is lists else s

    def scale_block(recv, slot, tail, at, there, codes_out, scales_out):
        before = None
        for j in range(TILES):
            if j < SERVE_N:
                window = pl.ds(pl.multiple_of(slot * BLOCK, BLOCK), BLOCK)
                now = recv[place_of(recv, j), window].astype(F32)
            else:
                now = tail
            if j == 0:
                value = now
            else:
                value = jnp.where(lane < 4 * j - 4, before, jnp.where(lane < 4 * j, tail, now))
            before = now
            top = jnp.maximum(jnp.max(jnp.abs(value), axis=0, keepdims=True), 0.25)
            codes = (value * (there / top)).astype(BF)
            width = min(128, FEAT - j * 128)
            codes_out[at, :, j * 128 : j * 128 + width] = codes[:, :width]
            scales_out[at, :, j * 128 : j * 128 + width] = (top * there)[:, :width]

    def present(layer, k):
        return jnp.minimum(jnp.maximum(table[16 + layer, me] - k, 0), 1).astype(F32)

    def receive(i):
        f, n, ends_at = MESSAGES[i]

        all_messages(i).wait_recv()
        if ends_at:
            take_tails(recvs[i], slice(LENGTHS[i] - 16, LENGTHS[i]), len(ends_at) * BASE, 0)

    def scale_message(i):
        f, n, _ = MESSAGES[i]

        def base_step(slot, carry):
            layer, k = f + slot // BASE, lax.rem(slot, BASE)
            scale_block(
                recvs[i], slot, tails[TAIL_AT[i] + slot], layer * SLOTS + k, present(layer, k), out, scales
            )
            return carry

        lax.fori_loop(0, n * BASE, base_step, 0)

    def finish_list():
        list_copy(7).wait_recv()
        take_tails(lists, slice(LIST - 16, LIST), EXTRA, 16)

        def extra_step(entry, carry):
            scale_block(lists, entry, tails[16 + entry], entry, 1.0, extra_codes, extra_scales)
            return carry

        lax.fori_loop(0, EXTRA, extra_step, 0)

        def place_step(layer, carry):
            entry, there = table[32 + layer, me], present(layer, BASE)
            at = layer * SLOTS + BASE
            out[at] = (extra_codes[entry].astype(F32) * there).astype(BF)
            scales[at] = extra_scales[entry] * there
            return carry

        lax.fori_loop(0, LAYERS, place_step, 0)

    def left_all(i):
        all_messages(i).wait_send()

    def halo_left():
        for side in range(2):
            @pl.when(has_next[side])
            def _(side=side):
                pltpu.make_async_remote_copy(
                    src_ref=hsend.at[side],
                    dst_ref=hrecv.at[side],
                    send_sem=hs_sem.at[side],
                    recv_sem=hr_sem.at[side, 0],
                    device_id={"train": (right, left)[side]},
                    device_id_type=MESH,
                ).wait_send()

    def tell(step):
        return pltpu.make_async_remote_copy(
            src_ref=fsend,
            dst_ref=frecv.at[t],
            send_sem=fs_sem,
            recv_sem=fr_sem,
            device_id={"train": lax.rem(t + step, TRAIN_N)},
            device_id_type=MESH,
        )

    pl.semaphore_wait(barrier, SERVE_N + TRAIN_N - 2)
    for side in range(2):
        @pl.when(has_next[side])
        def _(side=side):
            halo(side, 0).start()

        @pl.when(jnp.logical_not(has_next[1 - side]))
        def _(side=side):
            hrecv[side] = jnp.zeros((EDGE, 128), BF)
    for copy in small:
        copy.wait()
    named[...] = jnp.full((16, 128), -1, I32)
    named[:, 0:BLOCKS_DEV] = groups[...]
    group = named[...]
    order = jnp.zeros((16, 128), I32)
    for d in range(1, BLOCKS_DEV):
        same = (pltpu.roll(group, d, axis=1) == group) & (lane16 >= d)
        order = order + jnp.where(same, 1, 0)
    slot_of = group * SLOTS + order
    blocks_at = jnp.zeros((16, 128), I32)
    third_at = jnp.zeros((16, 128), I32)
    counted = jnp.zeros((16, 128), I32)
    for b in range(BLOCKS_DEV):
        slot_b = slot_of[:, b : b + 1]
        blocks_at = jnp.where(slot_b == lane16, b, blocks_at)
        third_at = jnp.where(slot_b == lane16 * SLOTS + BASE, b, third_at)
        counted = counted + jnp.where(group[:, b : b + 1] == lane16, 1, 0)
    third = jnp.where(counted > BASE, 1, 0)
    rows_third = jnp.broadcast_to(jnp.sum(third, axis=1, keepdims=True), (16, 128))
    before = jnp.zeros((16, 128), I32)
    for d in range(1, LAYERS):
        before = before + jnp.where(row16 >= d, pltpu.roll(rows_third, d, axis=0), 0)
        before = before + jnp.where(lane16 >= d, pltpu.roll(third, d, axis=1), 0)
    found[0:16] = blocks_at
    found[16:32] = counted
    found[32:48] = jnp.minimum(before, EXTRA - 1)
    where_third = row16 * HELD + 1 + third_at

    def whole(x):
        return jnp.sum(jnp.sum(x, axis=0, keepdims=True), axis=1, keepdims=True)

    for e in range(EXTRA):
        mine = (third > 0) & (before == e)
        found[48 + e : 49 + e] = jnp.broadcast_to(whole(jnp.where(mine, where_third, 0)), (1, 128))
    known = pltpu.make_async_copy(found, table, table_sem)
    known.start()
    long = jnp.where(whole(third) > EXTRA, 1.0, 0.0)
    fsend[...] = jnp.broadcast_to(long, (8, 128))
    frecv[t] = fsend[...]

    for side in range(2):
        @pl.when(has_next[side])
        def _(side=side):
            halo(side, 1).start()
            halo(side, 2).start()

    for step in range(1, TRAIN_N):
        tell(step).start()
    for copy in loads[2]:
        copy.wait()
    for m in range(8):
        gather_columns(m, middle)
    turn_tail(middle)
    lax.fori_loop(0, 1, prepare_step, 0)
    known.wait()
    halo_arrived(0)
    patch(0)
    dispatch(0)
    lax.fori_loop(1, PAIRS, prepare_step, 0, unroll=7)
    halo_arrived(1)
    halo_arrived(2)
    lax.fori_loop(1, PAIRS, patch_step, 0)
    dispatch_list()
    dispatch(1)
    for i in range(3):
        list_copy(i).wait_recv()
    for i in range(3, 6):
        list_copy(i).start()
    dispatch(2)
    receive(0)
    left_all(0)
    receive(1)
    scale_message(1)
    list_copy(3).wait_recv()
    list_copy(6).start()
    dispatch(3)
    dispatch(4)
    left_all(1)
    receive(2)
    scale_message(2)
    some_lists(3).wait_recv()
    list_copy(7).start()
    left_all(2)
    told = pltpu.make_async_remote_copy(
        src_ref=frecv.at[0 : TRAIN_N - 1],
        dst_ref=frecv.at[0 : TRAIN_N - 1],
        send_sem=fs_sem,
        recv_sem=fr_sem,
        device_id={"train": right},
        device_id_type=MESH,
    )
    told.wait_send()
    told.wait_recv()
    flag[...] = jnp.broadcast_to(jnp.max(frecv[...]).reshape(1, 1), (8, 128))
    halo_left()
    finish_list()
    receive(3)
    scale_message(3)
    scale_message(0)
    some_lists(15).wait_send()
    receive(4)
    scale_message(4)
    left_all(3)
    left_all(4)


def everything(train_weights, row_offset, groups):
    position = jnp.arange(BLOCKS_DEV, dtype=I32)
    earlier = position[None, :] < position[:, None]
    same = groups[:, :, None] == groups[:, None, :]
    order = jnp.sum((same & earlier[None]).astype(I32), axis=2)
    slot_id = groups * SLOTS + order
    onehot = slot_id[:, None, :] == jnp.arange(SERVE_N * SLOTS, dtype=I32)[None, :, None]
    blocks_at = jnp.sum(jnp.where(onehot, position[None, None, :], 0), axis=2)
    group_ids = jnp.arange(SERVE_N, dtype=I32)
    counts = jnp.sum((groups[:, None, :] == group_ids[None, :, None]).astype(I32), axis=2)
    held = (counts[:, :, None] > jnp.arange(SLOTS, dtype=I32)).astype(I32)
    held = held.reshape(LAYERS, SERVE_N * SLOTS)
    weights = train_weights.reshape(LAYERS, HELD, BLOCK, COLS)
    parts = len(PARTS)
    smem = pl.BlockSpec(memory_space=pltpu.SMEM)
    vmem = pl.BlockSpec(memory_space=pltpu.VMEM)
    return pl.pallas_call(
        full_exchange,
        out_shape=(
            pltpu.VMEM((LAYERS * SLOTS, BLOCK, FEAT), BF),
            pltpu.VMEM((LAYERS * SLOTS, 1, FEAT), F32),
        ),
        in_specs=[smem, smem, smem, pl.BlockSpec(memory_space=pl.ANY)],
        out_specs=(vmem, vmem),
        scratch_shapes=[
            pltpu.VMEM((LAYERS, HELD, BLOCK, COLS), BF),
            pltpu.VMEM((2, LAYERS, BLOCK, COLS), BF),
            pltpu.VMEM((COLS, 256), BF),
            pltpu.VMEM((32, 16, 128), BF),
            pltpu.VMEM((max(PARTS) * SLOTS, BLOCK, 128), F32),
            pltpu.VMEM((max(PARTS), BLOCKS_DEV, BLOCK, 128), BF),
            pltpu.VMEM((max(PARTS), BLOCKS_DEV, BLOCK, 128), BF),
            pltpu.VMEM((2, HALO, 128), BF),
            pltpu.VMEM((2, HALO, 128), BF),
            pltpu.VMEM((SERVE_N, TOTAL, 128), BF),
            pltpu.VMEM((SERVE_N, TOTAL, 128), BF),
            pltpu.VMEM((128, 128), BF),
            pltpu.SemaphoreType.DMA((parts,)),
            pltpu.SemaphoreType.DMA((2,)),
            pltpu.SemaphoreType.DMA((2, parts)),
            pltpu.SemaphoreType.DMA((2, parts)),
            pltpu.SemaphoreType.DMA((parts, SERVE_N)),
            pltpu.SemaphoreType.DMA((parts, SERVE_N)),
        ],
        compiler_params=pltpu.CompilerParams(
            collective_id=1, has_side_effects=True, vmem_limit_bytes=44 * 2**20
        ),
    )(blocks_at, held, row_offset, weights)


def shards(train_weights, row_offset, block_group):
    groups = block_group[:, :, 0]
    smem = pl.BlockSpec(memory_space=pltpu.SMEM)
    vmem = pl.BlockSpec(memory_space=pltpu.VMEM)
    parts = len(MESSAGES)
    codes, scales, flag = pl.pallas_call(
        route,
        out_shape=(
            pltpu.VMEM((LAYERS * SLOTS, BLOCK, FEAT), BF),
            pltpu.VMEM((LAYERS * SLOTS, 1, FEAT), F32),
            jax.ShapeDtypeStruct((8, 128), F32),
        ),
        in_specs=[pl.BlockSpec(memory_space=pl.ANY)] * 3,
        out_specs=(vmem, vmem, vmem),
        scratch_shapes=[
            pltpu.VMEM((LAYERS, BLOCKS_DEV), I32),
            pltpu.SMEM((LAYERS, TRAIN_N + 1), I32),
            pltpu.VMEM((LAYERS, 128), I32),
            pltpu.VMEM((56, 128), I32),
            pltpu.SMEM((56, 128), I32),
            pltpu.VMEM((COLS + 16, LAYERS, BUFFER), BF),
            pltpu.VMEM((256, 256), BF),
            pltpu.VMEM((256, 256), BF),
            pltpu.VMEM((128 * LAYERS, BUFFER), BF),
            pltpu.VMEM((BUFFER, 64), BF),
            pltpu.VMEM((32, 16, 128), BF),
            pltpu.VMEM((LAYERS * HELD, BLOCK, 128), BF),
            pltpu.VMEM((LAYERS * HELD, BLOCK, 128), BF),
            pltpu.VMEM((2, EDGE, 128), BF),
            pltpu.VMEM((2, EDGE, 128), BF),
            pltpu.VMEM((16 + EXTRA, BLOCK, 128), F32),
            pltpu.VMEM((EXTRA, BLOCK, FEAT), BF),
            pltpu.VMEM((EXTRA, 1, FEAT), F32),
            pltpu.VMEM((8, 128), F32),
            pltpu.VMEM((TRAIN_N, 8, 128), F32),
            *[pltpu.VMEM((SERVE_N, length, 128), BF) for length in LENGTHS * 2],
            pltpu.VMEM((SERVE_N, LIST, 128), BF),
            pltpu.SemaphoreType.DMA((2,)),
            pltpu.SemaphoreType.DMA,
            pltpu.SemaphoreType.DMA((3, 2)),
            pltpu.SemaphoreType.DMA((2,)),
            pltpu.SemaphoreType.DMA((2, 3)),
            pltpu.SemaphoreType.DMA((parts,)),
            pltpu.SemaphoreType.DMA((parts,)),
            pltpu.SemaphoreType.DMA,
            pltpu.SemaphoreType.DMA((6,)),
            pltpu.SemaphoreType.DMA,
            pltpu.SemaphoreType.DMA,
        ],
        compiler_params=pltpu.CompilerParams(
            collective_id=2, has_side_effects=True, vmem_limit_bytes=46 * 2**20
        ),
    )(
        groups, row_offset, jnp.transpose(train_weights, (2, 0, 1)),
    )
    codes, scales = lax.cond(
        flag[0, 0] > 0.0,
        lambda: tuple(everything(train_weights, row_offset, groups)),
        lambda: (codes, scales),
    )
    return (
        codes.reshape(LAYERS, 1, 1, SLOTS, BLOCK, FEAT),
        scales.reshape(LAYERS, 1, 1, SLOTS, FEAT),
    )


def solution(mesh):
    return jax.shard_map(
        shards,
        mesh=mesh,
        in_specs=(P(None, "train", "serve"), P(), P(None, "train", None)),
        out_specs=(P(None, "serve", "train", None, None, None), P(None, "serve", "train", None, None)),
        check_vma=False,
    )
```

```python
import functools

import jax
import jax.numpy as jnp
from jax import lax
from jax.experimental import pallas as pl
from jax.experimental.pallas import tpu as pltpu
from jax.sharding import PartitionSpec as P

MESH = pl.DeviceIdType.MESH
BF = jnp.bfloat16
F32 = jnp.float32
I32 = jnp.int32
LAYERS = 16
BLOCK = 32
BLOCKS_DEV = 28
HELD = BLOCKS_DEV + 2
ROWS_DEV = 896
BUFFER = HELD * BLOCK
COLS = 132
SERVE_N = 16
TRAIN_N = 8
SLOTS = 3
FEAT = SERVE_N * COLS
TILES = -(-FEAT // 128)

PARTS = (2, 4, 4, 4, 2)
FIRST = (0, 2, 6, 10, 14)
SIZES = tuple(n * SLOTS * BLOCK + 16 for n in PARTS)
BASES = tuple(sum(SIZES[:i]) for i in range(len(PARTS)))
TOTAL = sum(SIZES)
HALO = 16 + LAYERS * BLOCK
HALO_ENDS = tuple(16 + (f + n) * BLOCK for f, n in zip(FIRST, PARTS))
HALO_BASES = (0,) + HALO_ENDS[:-1]

BASE = 2
EXTRA = 8
MESSAGES = (
    (0, 2, ()),
    (2, 3, tuple(range(2, 10))),
    (5, 5, tuple(range(10, 16)) + (0, 1)),
    (10, 4, ()),
    (14, 2, ()),
)
LENGTHS = tuple(n * BASE * BLOCK + (16 if m else 0) for _, n, m in MESSAGES)
TILE_AT = {1: 0, 2: 16 + EXTRA}
TAIL_AT = tuple(
    next(TILE_AT[i] + m.index(f) * BASE for i, (_, _, m) in enumerate(MESSAGES) if f in m)
    for f, _, _ in MESSAGES
)
LIST = EXTRA * BLOCK + 16
PAIRS = LAYERS // 2
EARLY = 5
EDGE = BLOCK + LAYERS * BLOCK
HALO_STARTS = (0, 3 * BLOCK, (1 + 2 * EARLY) * BLOCK, EDGE)


def full_exchange(
    blocks_at, held, offsets, weights, out, scales,
    raw, edge, rot, lanes, tails, turned, rest, hsend, hrecv, send, recv, patch,
    raw_sem, edge_sem, hs_sem, hr_sem, s_sem, r_sem,
):
    t = lax.axis_index("train")
    me = lax.axis_index("serve")
    mx, my, mc = me // 8, lax.rem(me // 2, 4), lax.rem(me, 2)
    right, left = lax.rem(t + 1, TRAIN_N), lax.rem(t + TRAIN_N - 1, TRAIN_N)

    def peer(v):
        return (
            lax.rem(mx + v // 8, 2) * 8
            + lax.rem(my + lax.rem(v // 2, 4), 4) * 2
            + lax.rem(mc + lax.rem(v, 2), 2)
        )

    barrier = pltpu.get_barrier_semaphore()
    for v in range(1, SERVE_N):
        pl.semaphore_signal(barrier, inc=1, device_id={"serve": peer(v)}, device_id_type=MESH)
    for other in (left, right):
        pl.semaphore_signal(barrier, inc=1, device_id={"train": other}, device_id_type=MESH)

    edges = [
        pltpu.make_async_copy(weights.at[:, b], edge.at[side], edge_sem.at[side])
        for side, b in enumerate((BLOCKS_DEV + 1, 0))
    ]
    loads = [
        pltpu.make_async_copy(weights.at[pl.ds(f, n)], raw.at[pl.ds(f, n)], raw_sem.at[i])
        for i, (f, n) in enumerate(zip(FIRST, PARTS))
    ]
    for copy in edges + loads:
        copy.start()

    row = lax.broadcasted_iota(jnp.int32, (COLS, 256), 0)
    col = lax.broadcasted_iota(jnp.int32, (COLS, 256), 1)
    turn = (row < 128) & (col < 128) & (col == ((row + 4 * me) & 127))
    spread = (row >= 128) & (col >= 128) & ((col & 3) == row - 128)
    rot[...] = jnp.where(turn | spread, 1.0, 0.0).astype(BF)
    lane16 = lax.broadcasted_iota(jnp.int32, (16, 128), 1)
    for m in range(32):
        lanes[m] = jnp.where((lane16 >> 2) == m, 1.0, 0.0).astype(BF)
    rrow = lax.broadcasted_iota(jnp.int32, (128, 128), 0)
    rcol = lax.broadcasted_iota(jnp.int32, (128, 128), 1)
    patch[...] = jnp.where((rrow & 3) == (rcol & 3), 1.0, 0.0).astype(BF)

    for copy in edges:
        copy.wait()
    for side in range(2):
        def edge_step(i, total, side=side):
            x = edge[side, pl.ds(i * 4, 4)].reshape(4 * BLOCK, COLS)
            y = jnp.dot(x, rot[...], preferred_element_type=F32).astype(BF)
            hsend[side, pl.ds(pl.multiple_of(16 + i * 128, 16), 128)] = y[:, :128]
            for q in range(8):
                total = total + y[q * 16 : q * 16 + 16, 128:] * lanes[lax.rem(i * 8 + q + me, 32)]
            return total

        hsend[side, 0:16] = lax.fori_loop(0, LAYERS // 4, edge_step, jnp.zeros((16, 128), BF))

    pl.semaphore_wait(barrier, SERVE_N + 1)

    halos = []
    for i in range(len(PARTS)):
        window = pl.ds(HALO_BASES[i], HALO_ENDS[i] - HALO_BASES[i])
        for side, target in enumerate((right, left)):
            copy = pltpu.make_async_remote_copy(
                src_ref=hsend.at[side, window],
                dst_ref=hrecv.at[side, window],
                send_sem=hs_sem.at[side, i],
                recv_sem=hr_sem.at[side, i],
                device_id={"train": target},
                device_id_type=MESH,
            )
            copy.start()
            halos.append(copy)

    def block_copy(i, v):
        window = pl.ds(BASES[i], SIZES[i])
        return pltpu.make_async_remote_copy(
            src_ref=send.at[v, window],
            dst_ref=recv.at[me, window],
            send_sem=s_sem.at[i, v],
            recv_sem=r_sem.at[i, v],
            device_id={"serve": peer(v)},
            device_id_type=MESH,
        )

    block_row = lax.broadcasted_iota(jnp.int32, (BLOCK, 128), 0)

    for i, (f, n) in enumerate(zip(FIRST, PARTS)):
        loads[i].wait()

        def turn_step(j, carry, f=f):
            l, b = j // 7, lax.rem(j, 7) * 4
            x = raw[f + l, pl.ds(b + 1, 4)].reshape(4 * BLOCK, COLS)
            y = jnp.dot(x, rot[...], preferred_element_type=F32).astype(BF)
            turned[l, pl.ds(b, 4)] = y[:, :128].reshape(4, BLOCK, 128)
            rest[l, pl.ds(b, 4)] = y[:, 128:].reshape(4, BLOCK, 128)
            return carry

        lax.fori_loop(0, n * 7, turn_step, 0)
        halos[2 * i].wait_recv()
        halos[2 * i + 1].wait_recv()

        def patch_step(l, carry, f=f):
            layer = f + l
            first = offsets[layer, t] - t * ROWS_DEV
            last = offsets[layer, t + 1] - t * ROWS_DEV - (ROWS_DEV - BLOCK)
            for side, (b, take) in enumerate(
                ((0, block_row < first), (BLOCKS_DEV - 1, block_row >= last))
            ):
                main = hrecv[side, pl.ds(pl.multiple_of(16 + layer * BLOCK, 16), BLOCK)]
                packed = hrecv[side, 0:16]
                both = jnp.concatenate(
                    [packed * lanes[lax.rem(2 * layer + h + me, 32)] for h in range(2)], axis=0
                )
                tail = jnp.dot(both, patch[...], preferred_element_type=F32)
                turned[l, b] = jnp.where(take, main.astype(F32), turned[l, b].astype(F32)).astype(BF)
                rest[l, b] = jnp.where(take, tail, rest[l, b].astype(F32)).astype(BF)
            return carry

        lax.fori_loop(0, n, patch_step, 0)

        def fill(dest, index, group, i=i, f=f, n=n):
            total = jnp.zeros((16, 128), BF)
            for l in range(n):
                for k in range(SLOTS):
                    slot = l * SLOTS + k
                    b = blocks_at[f + l, group * SLOTS + k]
                    dest[index, pl.ds(BASES[i] + slot * BLOCK, BLOCK)] = turned[l, b]
                    pair = rest[l, b]
                    for h in range(2):
                        total = total + pair[h * 16 : h * 16 + 16] * lanes[
                            lax.rem(2 * slot + h + me, 32)
                        ]
            dest[index, pl.ds(BASES[i] + n * SLOTS * BLOCK, 16)] = total

        def send_step(j, carry, i=i, fill=fill):
            v = SERVE_N - 1 - j
            fill(send, v, peer(v))
            block_copy(i, v).start()
            return carry

        lax.fori_loop(0, SERVE_N - 1, send_step, 0)
        fill(recv, me, me)

    lane = lax.broadcasted_iota(jnp.int32, (BLOCK, 128), 1)
    for i, (f, n) in enumerate(zip(FIRST, PARTS)):
        def arrive(j, carry, i=i):
            block_copy(i, j + 1).wait_recv()
            return carry

        lax.fori_loop(0, SERVE_N - 1, arrive, 0)

        def tail_step(q, carry, i=i, n=n):
            total = jnp.zeros((16, 128), BF)
            for s in range(SERVE_N):
                total = total + recv[s, pl.ds(BASES[i] + n * SLOTS * BLOCK, 16)] * lanes[
                    lax.rem(q + s, 32)
                ]
            tails[q // 2, pl.ds(pl.multiple_of(lax.rem(q, 2) * 16, 16), 16)] = pltpu.roll(
                total.astype(F32), 128 - 4 * q, axis=1
            )
            return carry

        lax.fori_loop(0, 2 * n * SLOTS, tail_step, 0)

        def block_step(slot, carry, i=i, f=f):
            layer, k = f + slot // SLOTS, lax.rem(slot, SLOTS)
            there = held[layer, me * SLOTS + k].astype(F32)
            at = f * SLOTS + slot
            tail = tails[slot]
            before = None
            for j in range(TILES):
                if j < SERVE_N:
                    now = recv[j, pl.ds(pl.multiple_of(BASES[i] + slot * BLOCK, 16), BLOCK)].astype(F32)
                else:
                    now = tail
                if j == 0:
                    value = now
                else:
                    value = jnp.where(
                        lane < 4 * j - 4, before, jnp.where(lane < 4 * j, tail, now)
                    )
                before = now
                top = jnp.maximum(jnp.max(jnp.abs(value), axis=0, keepdims=True), 0.25)
                codes = (value * (there / top)).astype(BF)
                width = min(128, FEAT - j * 128)
                out[at, :, j * 128 : j * 128 + width] = codes[:, :width]
                scales[at, :, j * 128 : j * 128 + width] = (top * there)[:, :width]
            return carry

        lax.fori_loop(0, n * SLOTS, block_step, 0)

    for copy in halos:
        copy.wait_send()
    for i in range(len(PARTS)):
        def leave(j, carry, i=i):
            block_copy(i, j + 1).wait_send()
            return carry

        lax.fori_loop(0, SERVE_N - 1, leave, 0)


def route(
    groups_in, offsets_in, weights, out, scales, flag,
    groups, offsets, named, found, table, raw, eye, spread, turning, mixed_tail, lanes, turned, rest,
    hsend, hrecv, tails, extra_codes, extra_scales, fsend, frecv,
    send0, send1, send2, send3, send4, recv0, recv1, recv2, recv3, recv4, lists,
    small_sem, table_sem, raw_sem, hs_sem, hr_sem, s_sem, r_sem, ls_sem, lr_sem, fs_sem, fr_sem,
):
    sends = (send0, send1, send2, send3, send4)
    recvs = (recv0, recv1, recv2, recv3, recv4)
    t = lax.axis_index("train")
    me = lax.axis_index("serve")
    mx, my, mc = me // 8, lax.rem(me // 2, 4), lax.rem(me, 2)
    right, left = lax.rem(t + 1, TRAIN_N), lax.rem(t + TRAIN_N - 1, TRAIN_N)

    def peer(v):
        return (
            lax.rem(mx + v // 8, 2) * 8
            + lax.rem(my + lax.rem(v // 2, 4), 4) * 2
            + lax.rem(mc + lax.rem(v, 2), 2)
        )

    small = [
        pltpu.make_async_copy(groups_in, groups, small_sem.at[0]),
        pltpu.make_async_copy(offsets_in, offsets, small_sem.at[1]),
    ]
    loads = [
        [
            pltpu.make_async_copy(
                weights.at[a : a + n, :, r : r + w], raw.at[b : b + n, :, r : r + w], raw_sem.at[i, j]
            )
            for j, (a, b, n) in enumerate(((0, 16, COLS), (112, 0, 16)))
        ]
        for i, (r, w) in enumerate(((0, 128), (896, 64), (128, 768)))
    ]
    for copy in loads[0] + loads[1] + small + loads[2]:
        copy.start()

    barrier = pltpu.get_barrier_semaphore()
    for v in range(1, SERVE_N):
        pl.semaphore_signal(barrier, inc=1, device_id={"serve": peer(v)}, device_id_type=MESH)
    for step in range(1, TRAIN_N):
        pl.semaphore_signal(
            barrier, inc=1, device_id={"train": lax.rem(t + step, TRAIN_N)}, device_id_type=MESH
        )

    def index(shape, dim):
        return lax.broadcasted_iota(I32, shape, dim)

    def ones(cond):
        return jnp.where(cond, 1.0, 0.0).astype(BF)

    lane16, row16 = index((16, 128), 1), index((16, 128), 0)
    eye[...] = ones(index((256, 256), 0) == index((256, 256), 1))
    a, b = index((256, 256), 0), index((256, 256), 1)
    spread[...] = ones(((b >> 4) == (a & 15)) & ((b & 15) == (a >> 4)))
    for m in range(32):
        lanes[m] = ones((lane16 >> 2) == m)

    NT = (((1,), (1,)), ((), ()))

    def gather_columns(m, tiles):
        start = 16 * (m + 1) - 4 * lax.rem(me, 4)
        place = 16 * lax.rem(m + me // 4, 8)
        for r, w in tiles:
            x = raw[pl.ds(start, 16), :, r : r + w].reshape(256, w)
            y = jnp.dot(spread[...], x, preferred_element_type=F32).astype(BF)
            for layer in range(LAYERS):
                window = pl.ds(pl.multiple_of(128 * layer + place, 16), 16)
                turning[window, r : r + w] = y[16 * layer : 16 * layer + 16]

    ends, middle = ((0, 128), (896, 64)), ((128, 256), (384, 256), (640, 256))
    for copy in loads[0] + loads[1]:
        copy.wait()
    for m in range(8):
        gather_columns(m, ends)

    def turn_tail(tiles):
        for r, w in tiles:
            x = raw[144:148, :, r : r + w].reshape(64, w)
            y = lax.dot_general(eye[:w, :w], x, NT, preferred_element_type=F32)
            mixed_tail[r : r + w] = y.astype(BF)

    turn_tail(ends)
    hsend[0, 0:BLOCK, 0:64] = mixed_tail[BUFFER - BLOCK : BUFFER]
    hsend[1, 0:BLOCK, 0:64] = mixed_tail[0:BLOCK]
    hsend[0, 0:BLOCK, 64:128] = jnp.zeros((BLOCK, 64), BF)
    hsend[1, 0:BLOCK, 64:128] = jnp.zeros((BLOCK, 64), BF)

    def edge_step(p, carry):
        rows = pl.ds(pl.multiple_of(256 * p, 256), 256)
        low = lax.dot_general(eye[0:32, 0:128], turning[rows, 0:128], NT, preferred_element_type=F32)
        high = lax.dot_general(
            eye[32:64, 0:64], turning[rows, 896:960], NT, preferred_element_type=F32
        )
        for h in range(2):
            window = pl.ds(pl.multiple_of(BLOCK + (2 * p + h) * BLOCK, BLOCK), BLOCK)
            hsend[0, window] = high[:, 128 * h : 128 * h + 128].astype(BF)
            hsend[1, window] = low[:, 128 * h : 128 * h + 128].astype(BF)
        return carry

    lax.fori_loop(0, PAIRS, edge_step, 0, unroll=8)

    def tail_pick(p):
        k, q = index((64, 256), 0), index((64, 256), 1)
        return ones(((k & 15) == 2 * p + (q >> 7)) & ((k >> 4) == (q & 3)))

    def prepare_step(p, carry):
        rows = pl.ds(pl.multiple_of(256 * p, 256), 256)
        tail_of = tail_pick(p)
        for r, w in ((0, 128), (128, 256), (384, 256), (640, 256), (896, 64)):
            y = lax.dot_general(
                eye[:w, :w], turning[rows, r : r + w], NT, preferred_element_type=F32
            ).astype(BF)
            z = jnp.dot(mixed_tail[r : r + w], tail_of, preferred_element_type=F32).astype(BF)
            for h in range(2):
                at = pl.ds((2 * p + h) * HELD + r // BLOCK, w // BLOCK)
                turned[at] = y[:, 128 * h : 128 * h + 128].reshape(w // BLOCK, BLOCK, 128)
                rest[at] = z[:, 128 * h : 128 * h + 128].reshape(w // BLOCK, BLOCK, 128)
        return carry

    has_next = (t < TRAIN_N - 1, t > 0)

    def halo_arrived(i):
        for side in range(2):
            @pl.when(has_next[1 - side])
            def _(side=side):
                halo(side, i).wait_recv()

    def halo(side, i):
        window = pl.ds(HALO_STARTS[i], HALO_STARTS[i + 1] - HALO_STARTS[i])
        return pltpu.make_async_remote_copy(
            src_ref=hsend.at[side, window],
            dst_ref=hrecv.at[side, window],
            send_sem=hs_sem.at[side],
            recv_sem=hr_sem.at[side, i],
            device_id={"train": (right, left)[side]},
            device_id_type=MESH,
        )

    block_row = index((BLOCK, 128), 0)

    def patch(p):
        tail_of = tail_pick(p)
        for side, (b, last) in enumerate(((1, False), (HELD - 2, True))):
            tail = jnp.dot(hrecv[side, 0:BLOCK, 0:64], tail_of, preferred_element_type=F32)
            for h in range(2):
                layer = 2 * p + h
                if last:
                    take = block_row >= offsets[layer, t + 1] - t * ROWS_DEV - (ROWS_DEV - BLOCK)
                else:
                    take = block_row < offsets[layer, t] - t * ROWS_DEV
                at = layer * HELD + b
                window = pl.ds(pl.multiple_of(BLOCK + layer * BLOCK, BLOCK), BLOCK)
                main = hrecv[side, window].astype(F32)
                turned[at] = jnp.where(take, main, turned[at].astype(F32)).astype(BF)
                rest[at] = jnp.where(
                    take, tail[:, 128 * h : 128 * h + 128], rest[at].astype(F32)
                ).astype(BF)

    def patch_step(p, carry):
        patch(p)
        return carry

    def message(i, v):
        return pltpu.make_async_remote_copy(
            src_ref=sends[i].at[v],
            dst_ref=recvs[i].at[me],
            send_sem=s_sem.at[i],
            recv_sem=r_sem.at[i],
            device_id={"serve": peer(v)},
            device_id_type=MESH,
        )

    def tail_of_block(total, at, slot):
        pair = rest[at]
        for h in range(2):
            total = total + pair[h * 16 : h * 16 + 16] * lanes[lax.rem(2 * slot + h + me, 32)]
        return total

    def all_messages(i):
        most = pl.ds(0, SERVE_N - 1)
        return pltpu.make_async_remote_copy(
            src_ref=sends[i].at[most],
            dst_ref=recvs[i].at[most],
            send_sem=s_sem.at[i],
            recv_sem=r_sem.at[i],
            device_id={"serve": peer(1)},
            device_id_type=MESH,
        )

    def dispatch(i):
        f, n, ends_at = MESSAGES[i]

        def fill(dest, place, group):
            for slot in range(n * BASE):
                layer, k = f + slot // BASE, slot % BASE
                at = layer * HELD + 1 + table[layer, group * SLOTS + k]
                dest[place, slot * BLOCK : slot * BLOCK + BLOCK] = turned[at]
            if ends_at:
                total = jnp.zeros((16, 128), BF)
                for slot in range(len(ends_at) * BASE):
                    layer, k = ends_at[slot // BASE], slot % BASE
                    at = layer * HELD + 1 + table[layer, group * SLOTS + k]
                    total = tail_of_block(total, at, slot)
                dest[place, LENGTHS[i] - 16 : LENGTHS[i]] = total

        def send_step(j, carry):
            v = SERVE_N - 1 - j
            turn = lax.rem(lax.rem(v // 2, 4) * (1 + 2 * mc), 4)
            v = v // 8 * 8 + turn * 2 + lax.rem(v, 2)
            fill(sends[i], v, peer(v))
            message(i, v).start()
            return carry

        lax.fori_loop(0, SERVE_N - 1, send_step, 0)
        fill(recvs[i], me, me)

    def list_of(dx, dy):
        return mc * 8 + lax.rem(mx + dx, 2) * 4 + lax.rem(my + dy, 4)

    def list_copy(i):
        lists_at, dx, dy, dc = (
            (pl.ds(list_of(0, 0), 1), 1, 0, 0),
            (pl.ds(list_of(0, 0), 1), 0, 1, 0),
            (pl.ds(list_of(0, 0), 1), 0, 3, 0),
            (pl.ds(list_of(0, 3), 1), 0, 1, 0),
            (pl.ds(list_of(1, 0), 1), 0, 1, 0),
            (pl.ds(list_of(0, 1), 1), 1, 0, 0),
            (pl.ds(list_of(0, 2), 1), 1, 0, 0),
            (pl.ds(8 * mc, 8), 0, 0, 1),
        )[i]
        return pltpu.make_async_remote_copy(
            src_ref=lists.at[lists_at],
            dst_ref=lists.at[lists_at],
            send_sem=ls_sem,
            recv_sem=lr_sem.at[(0, 1, 5, 2, 4, 4, 4, 3)[i]],
            device_id={"serve": peer(8 * dx + 2 * dy + dc)},
            device_id_type=MESH,
        )

    def some_lists(n):
        return pltpu.make_async_remote_copy(
            src_ref=lists.at[pl.ds(0, n)],
            dst_ref=lists.at[pl.ds(0, n)],
            send_sem=ls_sem,
            recv_sem=lr_sem.at[4],
            device_id={"serve": peer(1)},
            device_id_type=MESH,
        )

    def dispatch_list():
        total = jnp.zeros((16, 128), BF)
        for e in range(EXTRA):
            at = table[48 + e, 0]
            lists[list_of(0, 0), e * BLOCK : e * BLOCK + BLOCK] = turned[at]
            total = tail_of_block(total, at, e)
        lists[list_of(0, 0), LIST - 16 : LIST] = total
        for i in range(3):
            list_copy(i).start()

    lane = index((BLOCK, 128), 1)

    def take_tails(recv, rows, count, base):
        def tail_step(q, carry):
            total = jnp.zeros((16, 128), BF)
            for s in range(SERVE_N):
                total = total + recv[place_of(recv, s), rows] * lanes[lax.rem(q + s, 32)]
            tails[base + q // 2, pl.ds(pl.multiple_of(lax.rem(q, 2) * 16, 16), 16)] = pltpu.roll(
                total.astype(F32), 128 - 4 * q, axis=1
            )
            return carry

        lax.fori_loop(0, 2 * count, tail_step, 0)

    def place_of(recv, s):
        return s % 2 * 8 + s // 8 * 4 + s // 2 % 4 if recv is lists else s

    def scale_block(recv, slot, tail, at, there, codes_out, scales_out):
        before = None
        for j in range(TILES):
            if j < SERVE_N:
                window = pl.ds(pl.multiple_of(slot * BLOCK, BLOCK), BLOCK)
                now = recv[place_of(recv, j), window].astype(F32)
            else:
                now = tail
            if j == 0:
                value = now
            else:
                value = jnp.where(lane < 4 * j - 4, before, jnp.where(lane < 4 * j, tail, now))
            before = now
            top = jnp.maximum(jnp.max(jnp.abs(value), axis=0, keepdims=True), 0.25)
            codes = (value * (there / top)).astype(BF)
            width = min(128, FEAT - j * 128)
            codes_out[at, :, j * 128 : j * 128 + width] = codes[:, :width]
            scales_out[at, :, j * 128 : j * 128 + width] = (top * there)[:, :width]

    def present(layer, k):
        return jnp.minimum(jnp.maximum(table[16 + layer, me] - k, 0), 1).astype(F32)

    def receive(i):
        f, n, ends_at = MESSAGES[i]

        all_messages(i).wait_recv()
        if ends_at:
            take_tails(recvs[i], slice(LENGTHS[i] - 16, LENGTHS[i]), len(ends_at) * BASE, TILE_AT[i])

    def scale_message(i):
        f, n, _ = MESSAGES[i]

        def base_step(slot, carry):
            layer, k = f + slot // BASE, lax.rem(slot, BASE)
            scale_block(
                recvs[i], slot, tails[TAIL_AT[i] + slot], layer * SLOTS + k, present(layer, k), out, scales
            )
            return carry

        lax.fori_loop(0, n * BASE, base_step, 0)

    def finish_list():
        list_copy(7).wait_recv()
        take_tails(lists, slice(LIST - 16, LIST), EXTRA, 16)

        def extra_step(entry, carry):
            scale_block(lists, entry, tails[16 + entry], entry, 1.0, extra_codes, extra_scales)
            return carry

        lax.fori_loop(0, EXTRA, extra_step, 0)

        def place_step(layer, carry):
            entry, there = table[32 + layer, me], present(layer, BASE)
            at = layer * SLOTS + BASE
            out[at] = (extra_codes[entry].astype(F32) * there).astype(BF)
            scales[at] = extra_scales[entry] * there
            return carry

        lax.fori_loop(0, LAYERS, place_step, 0)

    def left_all(i):
        all_messages(i).wait_send()

    def halo_left():
        for side in range(2):
            @pl.when(has_next[side])
            def _(side=side):
                pltpu.make_async_remote_copy(
                    src_ref=hsend.at[side],
                    dst_ref=hrecv.at[side],
                    send_sem=hs_sem.at[side],
                    recv_sem=hr_sem.at[side, 0],
                    device_id={"train": (right, left)[side]},
                    device_id_type=MESH,
                ).wait_send()

    def tell(step):
        return pltpu.make_async_remote_copy(
            src_ref=fsend,
            dst_ref=frecv.at[t],
            send_sem=fs_sem,
            recv_sem=fr_sem,
            device_id={"train": lax.rem(t + step, TRAIN_N)},
            device_id_type=MESH,
        )

    pl.semaphore_wait(barrier, SERVE_N + TRAIN_N - 2)
    for side in range(2):
        @pl.when(has_next[side])
        def _(side=side):
            halo(side, 0).start()

        @pl.when(jnp.logical_not(has_next[1 - side]))
        def _(side=side):
            hrecv[side] = jnp.zeros((EDGE, 128), BF)
    for copy in small:
        copy.wait()
    named[...] = jnp.full((16, 128), -1, I32)
    named[:, 0:BLOCKS_DEV] = groups[...]
    group = named[...]
    order = jnp.zeros((16, 128), I32)
    for d in range(1, BLOCKS_DEV):
        same = (pltpu.roll(group, d, axis=1) == group) & (lane16 >= d)
        order = order + jnp.where(same, 1, 0)
    slot_of = group * SLOTS + order
    blocks_at = jnp.zeros((16, 128), I32)
    third_at = jnp.zeros((16, 128), I32)
    counted = jnp.zeros((16, 128), I32)
    for b in range(BLOCKS_DEV):
        slot_b = slot_of[:, b : b + 1]
        blocks_at = jnp.where(slot_b == lane16, b, blocks_at)
        third_at = jnp.where(slot_b == lane16 * SLOTS + BASE, b, third_at)
        counted = counted + jnp.where(group[:, b : b + 1] == lane16, 1, 0)
    third = jnp.where(counted > BASE, 1, 0)
    rows_third = jnp.broadcast_to(jnp.sum(third, axis=1, keepdims=True), (16, 128))
    before = jnp.zeros((16, 128), I32)
    for d in range(1, LAYERS):
        before = before + jnp.where(row16 >= d, pltpu.roll(rows_third, d, axis=0), 0)
        before = before + jnp.where(lane16 >= d, pltpu.roll(third, d, axis=1), 0)
    found[0:16] = blocks_at
    found[16:32] = counted
    found[32:48] = jnp.minimum(before, EXTRA - 1)
    where_third = row16 * HELD + 1 + third_at

    def whole(x):
        return jnp.sum(jnp.sum(x, axis=0, keepdims=True), axis=1, keepdims=True)

    for e in range(EXTRA):
        mine = (third > 0) & (before == e)
        found[48 + e : 49 + e] = jnp.broadcast_to(whole(jnp.where(mine, where_third, 0)), (1, 128))
    known = pltpu.make_async_copy(found, table, table_sem)
    known.start()
    long = jnp.where(whole(third) > EXTRA, 1.0, 0.0)
    fsend[...] = jnp.broadcast_to(long, (8, 128))
    frecv[t] = fsend[...]

    for side in range(2):
        @pl.when(has_next[side])
        def _(side=side):
            halo(side, 1).start()
            halo(side, 2).start()

    for step in range(1, TRAIN_N):
        tell(step).start()
    for copy in loads[2]:
        copy.wait()
    for m in range(8):
        gather_columns(m, middle)
    turn_tail(middle)
    lax.fori_loop(0, 1, prepare_step, 0)
    known.wait()
    halo_arrived(0)
    patch(0)
    dispatch(0)
    lax.fori_loop(1, PAIRS, prepare_step, 0, unroll=7)
    halo_arrived(1)
    halo_arrived(2)
    lax.fori_loop(1, PAIRS, patch_step, 0)
    dispatch_list()
    dispatch(1)
    for i in range(3):
        list_copy(i).wait_recv()
    for i in range(3, 6):
        list_copy(i).start()
    dispatch(2)
    receive(0)
    left_all(0)
    receive(1)
    scale_message(1)
    list_copy(3).wait_recv()
    list_copy(6).start()
    dispatch(3)
    dispatch(4)
    left_all(1)
    receive(2)
    scale_message(2)
    scale_message(0)
    some_lists(3).wait_recv()
    list_copy(7).start()
    left_all(2)
    told = pltpu.make_async_remote_copy(
        src_ref=frecv.at[0 : TRAIN_N - 1],
        dst_ref=frecv.at[0 : TRAIN_N - 1],
        send_sem=fs_sem,
        recv_sem=fr_sem,
        device_id={"train": right},
        device_id_type=MESH,
    )
    told.wait_send()
    told.wait_recv()
    flag[...] = jnp.broadcast_to(jnp.max(frecv[...]).reshape(1, 1), (8, 128))
    halo_left()
    finish_list()
    receive(3)
    scale_message(3)
    some_lists(15).wait_send()
    receive(4)
    scale_message(4)
    left_all(3)
    left_all(4)


def everything(train_weights, row_offset, groups):
    position = jnp.arange(BLOCKS_DEV, dtype=I32)
    earlier = position[None, :] < position[:, None]
    same = groups[:, :, None] == groups[:, None, :]
    order = jnp.sum((same & earlier[None]).astype(I32), axis=2)
    slot_id = groups * SLOTS + order
    onehot = slot_id[:, None, :] == jnp.arange(SERVE_N * SLOTS, dtype=I32)[None, :, None]
    blocks_at = jnp.sum(jnp.where(onehot, position[None, None, :], 0), axis=2)
    group_ids = jnp.arange(SERVE_N, dtype=I32)
    counts = jnp.sum((groups[:, None, :] == group_ids[None, :, None]).astype(I32), axis=2)
    held = (counts[:, :, None] > jnp.arange(SLOTS, dtype=I32)).astype(I32)
    held = held.reshape(LAYERS, SERVE_N * SLOTS)
    weights = train_weights.reshape(LAYERS, HELD, BLOCK, COLS)
    parts = len(PARTS)
    smem = pl.BlockSpec(memory_space=pltpu.SMEM)
    vmem = pl.BlockSpec(memory_space=pltpu.VMEM)
    return pl.pallas_call(
        full_exchange,
        out_shape=(
            pltpu.VMEM((LAYERS * SLOTS, BLOCK, FEAT), BF),
            pltpu.VMEM((LAYERS * SLOTS, 1, FEAT), F32),
        ),
        in_specs=[smem, smem, smem, pl.BlockSpec(memory_space=pl.ANY)],
        out_specs=(vmem, vmem),
        scratch_shapes=[
            pltpu.VMEM((LAYERS, HELD, BLOCK, COLS), BF),
            pltpu.VMEM((2, LAYERS, BLOCK, COLS), BF),
            pltpu.VMEM((COLS, 256), BF),
            pltpu.VMEM((32, 16, 128), BF),
            pltpu.VMEM((max(PARTS) * SLOTS, BLOCK, 128), F32),
            pltpu.VMEM((max(PARTS), BLOCKS_DEV, BLOCK, 128), BF),
            pltpu.VMEM((max(PARTS), BLOCKS_DEV, BLOCK, 128), BF),
            pltpu.VMEM((2, HALO, 128), BF),
            pltpu.VMEM((2, HALO, 128), BF),
            pltpu.VMEM((SERVE_N, TOTAL, 128), BF),
            pltpu.VMEM((SERVE_N, TOTAL, 128), BF),
            pltpu.VMEM((128, 128), BF),
            pltpu.SemaphoreType.DMA((parts,)),
            pltpu.SemaphoreType.DMA((2,)),
            pltpu.SemaphoreType.DMA((2, parts)),
            pltpu.SemaphoreType.DMA((2, parts)),
            pltpu.SemaphoreType.DMA((parts, SERVE_N)),
            pltpu.SemaphoreType.DMA((parts, SERVE_N)),
        ],
        compiler_params=pltpu.CompilerParams(
            collective_id=1, has_side_effects=True, vmem_limit_bytes=44 * 2**20
        ),
    )(blocks_at, held, row_offset, weights)


def shards(train_weights, row_offset, block_group):
    groups = block_group[:, :, 0]
    smem = pl.BlockSpec(memory_space=pltpu.SMEM)
    vmem = pl.BlockSpec(memory_space=pltpu.VMEM)
    parts = len(MESSAGES)
    codes, scales, flag = pl.pallas_call(
        route,
        out_shape=(
            pltpu.VMEM((LAYERS * SLOTS, BLOCK, FEAT), BF),
            pltpu.VMEM((LAYERS * SLOTS, 1, FEAT), F32),
            jax.ShapeDtypeStruct((8, 128), F32),
        ),
        in_specs=[pl.BlockSpec(memory_space=pl.ANY)] * 3,
        out_specs=(vmem, vmem, vmem),
        scratch_shapes=[
            pltpu.VMEM((LAYERS, BLOCKS_DEV), I32),
            pltpu.SMEM((LAYERS, TRAIN_N + 1), I32),
            pltpu.VMEM((LAYERS, 128), I32),
            pltpu.VMEM((56, 128), I32),
            pltpu.SMEM((56, 128), I32),
            pltpu.VMEM((COLS + 16, LAYERS, BUFFER), BF),
            pltpu.VMEM((256, 256), BF),
            pltpu.VMEM((256, 256), BF),
            pltpu.VMEM((128 * LAYERS, BUFFER), BF),
            pltpu.VMEM((BUFFER, 64), BF),
            pltpu.VMEM((32, 16, 128), BF),
            pltpu.VMEM((LAYERS * HELD, BLOCK, 128), BF),
            pltpu.VMEM((LAYERS * HELD, BLOCK, 128), BF),
            pltpu.VMEM((2, EDGE, 128), BF),
            pltpu.VMEM((2, EDGE, 128), BF),
            pltpu.VMEM((32 + EXTRA, BLOCK, 128), F32),
            pltpu.VMEM((EXTRA, BLOCK, FEAT), BF),
            pltpu.VMEM((EXTRA, 1, FEAT), F32),
            pltpu.VMEM((8, 128), F32),
            pltpu.VMEM((TRAIN_N, 8, 128), F32),
            *[pltpu.VMEM((SERVE_N, length, 128), BF) for length in LENGTHS * 2],
            pltpu.VMEM((SERVE_N, LIST, 128), BF),
            pltpu.SemaphoreType.DMA((2,)),
            pltpu.SemaphoreType.DMA,
            pltpu.SemaphoreType.DMA((3, 2)),
            pltpu.SemaphoreType.DMA((2,)),
            pltpu.SemaphoreType.DMA((2, 3)),
            pltpu.SemaphoreType.DMA((parts,)),
            pltpu.SemaphoreType.DMA((parts,)),
            pltpu.SemaphoreType.DMA,
            pltpu.SemaphoreType.DMA((6,)),
            pltpu.SemaphoreType.DMA,
            pltpu.SemaphoreType.DMA,
        ],
        compiler_params=pltpu.CompilerParams(
            collective_id=2, has_side_effects=True, vmem_limit_bytes=46 * 2**20
        ),
    )(
        groups, row_offset, jnp.transpose(train_weights, (2, 0, 1)),
    )
    codes, scales = lax.cond(
        flag[0, 0] > 0.0,
        lambda: tuple(everything(train_weights, row_offset, groups)),
        lambda: (codes, scales),
    )
    return (
        codes.reshape(LAYERS, 1, 1, SLOTS, BLOCK, FEAT),
        scales.reshape(LAYERS, 1, 1, SLOTS, FEAT),
    )


def solution(mesh):
    return jax.shard_map(
        shards,
        mesh=mesh,
        in_specs=(P(None, "train", "serve"), P(), P(None, "train", None)),
        out_specs=(P(None, "serve", "train", None, None, None), P(None, "serve", "train", None, None)),
        check_vma=False,
    )
```
